32 devices in a mesh: bs: 4 (over y, z), tp: 8 (over x, core).
Axes of the slice: x: 4, y: 2, z: 2, core: 2. Of those that a mesh axis runs over, the one named last changes fastest.
The devices are a block of a 4x4x8 slice.
Arguments:
- new_hidden: bfloat16 [512, 3072], P('bs'), parts along dimension 0
- cache_k: bfloat16 [512, 64, 8, 128], P('bs', None, 'tp'), parts along dimension 0
- cache_v: bfloat16 [512, 64, 8, 128], P('bs', None, 'tp'), parts along dimension 0
- lengths: int32 [512], P('bs'), parts along dimension 0
- ln1_gain: float32 [3072], replicated
- ln1_bias: float32 [3072], replicated
- w_q: bfloat16 [3072, 3072], P(None, 'tp')
- w_k: bfloat16 [3072, 1024], P(None, 'tp')
- w_v: bfloat16 [3072, 1024], P(None, 'tp')
- w_o: bfloat16 [3072, 3072], P('tp')
- ln2_gain: float32 [3072], replicated
- ln2_bias: float32 [3072], replicated
- w_up: bfloat16 [3072, 8192], P(None, 'tp')
- w_down: bfloat16 [8192, 3072], P('tp')
- lnf_gain: float32 [3072], replicated
- lnf_bias: float32 [3072], replicated
- w_out: bfloat16 [3072, 128256], P(None, 'tp')
Outputs:
- output 1: float32 [512, 128256], P('bs', 'tp'), parts along dimension 0
- output 2: bfloat16 [512, 64, 8, 128], P('bs', None, 'tp'), parts along dimension 0
- output 3: bfloat16 [512, 64, 8, 128], P('bs', None, 'tp'), parts along dimension 0
- output 4: bfloat16 [512, 3072], P('bs'), parts along dimension 0
There are 4 independent parts. The reference program is written for one: setup_inputs(seed, part) draws one part's arguments, and reference() takes and returns one part's arrays. A program takes and returns all parts, laid end to end along the dimension named above; an argument that names none is the same for every part.
All inputs are finite; a program needn't handle non-finite values.
Results may differ from the reference program's by a relative error of at most 0.0124614.
Values are sent between devices in bfloat16 or wider.
A program may use at most 768 MiB of HBM per device.

```python
import math
import jax
import jax.numpy as jnp
from jax import lax

BATCH = 128
CACHE_LEN = 64
D_MODEL = 3072
HEADS = 24
KV_HEADS = 8
HEAD_DIM = 128
FF_DIM = 8192
VOCAB_SIZE = 128256
TP_SIZE = 8

EPSILON = 1e-5
ROPE_BASE = 10000.0
KV_GROUP = HEADS // KV_HEADS
SCORE_SCALE = HEAD_DIM ** -0.5
KEY_SCALE = math.sqrt(math.log(CACHE_LEN / 16.0) + 1.0)
LEN_BITS = int(math.log2(CACHE_LEN))


def layer_norm1p(values, gain, bias):
    mean = jnp.mean(values, axis=-1, keepdims=True)
    centered = values - mean
    variance = jnp.mean(jnp.square(centered), axis=-1, keepdims=True)
    return centered * lax.rsqrt(variance + EPSILON) * (1.0 + gain) + bias


def apply_rotary(vecs, positions):
    rot_dim = HEAD_DIM // 2
    half_rot = rot_dim // 2
    exponent = -2.0 * jnp.arange(half_rot, dtype=jnp.float32) / rot_dim
    inv_freq = ROPE_BASE ** exponent
    angles = positions.astype(jnp.float32)[:, None] * inv_freq[None, :]
    cosine = jnp.cos(angles)[:, None, :]
    sine = jnp.sin(angles)[:, None, :]
    first = vecs[..., :half_rot]
    second = vecs[..., half_rot:rot_dim]
    return jnp.concatenate([first * cosine - second * sine, second * cosine + first * sine, vecs[..., rot_dim:]], axis=-1)


def split_sum(activations, weight):
    act_blocks = jnp.transpose(activations.reshape(BATCH, TP_SIZE, -1), (1, 0, 2))
    weight_blocks = weight.reshape(TP_SIZE, -1, D_MODEL)

    def block_product(pair):
        return jnp.dot(pair[0], pair[1], preferred_element_type=jnp.float32).astype(jnp.bfloat16)

    partials = lax.map(block_product, (act_blocks, weight_blocks))
    return jnp.sum(partials.astype(jnp.float32), axis=0)


def draw_lengths(key):
    exp_key, off_key, long_key, short_key = jax.random.split(key, 4)
    exponent = jax.random.randint(exp_key, (BATCH,), 0, LEN_BITS)
    low_end = jnp.left_shift(jnp.ones((BATCH,), jnp.int32), exponent)
    offset = jax.random.randint(off_key, (BATCH,), 0, 1 << 30) % low_end
    raw_len = low_end + offset
    long_row = jax.random.randint(long_key, (), 0, BATCH)
    short_row = (long_row + jax.random.randint(short_key, (), 1, BATCH)) % BATCH
    rows = jnp.arange(BATCH)
    picked = jnp.where(rows == long_row, CACHE_LEN - 1, jnp.where(rows == short_row, 1, raw_len))
    return picked.astype(jnp.int32)


def setup_inputs(seed: int = 0, part: int = 0) -> dict:
    root_key = jax.random.key(seed)
    shared_root, group_root = jax.random.split(root_key)
    group_keys = jax.random.split(jax.random.fold_in(group_root, part), 4)
    shared_keys = jax.random.split(shared_root, 13)
    cache_shape = (BATCH, CACHE_LEN, KV_HEADS, HEAD_DIM)

    def gaussian(key, shape, scale):
        return scale * jax.random.normal(key, shape, jnp.float32)

    d_scale = 1.0 / math.sqrt(D_MODEL)
    o_scale = 1.0 / math.sqrt(HEADS * HEAD_DIM)
    ff_scale = 1.0 / math.sqrt(FF_DIM)
    return {
        'new_hidden': gaussian(group_keys[0], (BATCH, D_MODEL), 1.0).astype(jnp.bfloat16),
        'cache_k': gaussian(group_keys[1], cache_shape, KEY_SCALE).astype(jnp.bfloat16),
        'cache_v': gaussian(group_keys[2], cache_shape, 2.0).astype(jnp.bfloat16),
        'lengths': draw_lengths(group_keys[3]),
        'ln1_gain': gaussian(shared_keys[0], (D_MODEL,), 0.4),
        'ln1_bias': gaussian(shared_keys[1], (D_MODEL,), 0.4),
        'w_q': gaussian(shared_keys[2], (D_MODEL, HEADS * HEAD_DIM), d_scale).astype(jnp.bfloat16),
        'w_k': gaussian(shared_keys[3], (D_MODEL, KV_HEADS * HEAD_DIM), KEY_SCALE * d_scale).astype(jnp.bfloat16),
        'w_v': gaussian(shared_keys[4], (D_MODEL, KV_HEADS * HEAD_DIM), 2.0 * d_scale).astype(jnp.bfloat16),
        'w_o': gaussian(shared_keys[5], (HEADS * HEAD_DIM, D_MODEL), o_scale).astype(jnp.bfloat16),
        'ln2_gain': gaussian(shared_keys[6], (D_MODEL,), 0.4),
        'ln2_bias': gaussian(shared_keys[7], (D_MODEL,), 0.4),
        'w_up': gaussian(shared_keys[8], (D_MODEL, FF_DIM), d_scale).astype(jnp.bfloat16),
        'w_down': gaussian(shared_keys[9], (FF_DIM, D_MODEL), ff_scale).astype(jnp.bfloat16),
        'lnf_gain': gaussian(shared_keys[10], (D_MODEL,), 0.4),
        'lnf_bias': gaussian(shared_keys[11], (D_MODEL,), 0.4),
        'w_out': gaussian(shared_keys[12], (D_MODEL, VOCAB_SIZE), 2.0 * d_scale).astype(jnp.bfloat16),
    }


def reference(new_hidden, cache_k, cache_v, lengths, ln1_gain, ln1_bias, w_q, w_k, w_v, w_o, ln2_gain, ln2_bias, w_up, w_down, lnf_gain, lnf_bias, w_out):
    hidden_f = new_hidden.astype(jnp.float32)
    normed = layer_norm1p(hidden_f, ln1_gain, ln1_bias).astype(jnp.bfloat16)
    query = jnp.dot(normed, w_q, preferred_element_type=jnp.float32).reshape(BATCH, HEADS, HEAD_DIM)
    key_new = jnp.dot(normed, w_k, preferred_element_type=jnp.float32).reshape(BATCH, KV_HEADS, HEAD_DIM)
    val_new = jnp.dot(normed, w_v, preferred_element_type=jnp.float32).reshape(BATCH, KV_HEADS, HEAD_DIM)
    query = apply_rotary(query, lengths).astype(jnp.bfloat16)
    key_new = apply_rotary(key_new, lengths).astype(jnp.bfloat16)
    val_new = val_new.astype(jnp.bfloat16)
    write_slot = (jnp.arange(CACHE_LEN)[None, :] == lengths[:, None])[:, :, None, None]
    new_cache_k = jnp.where(write_slot, key_new[:, None], cache_k)
    new_cache_v = jnp.where(write_slot, val_new[:, None], cache_v)

    def one_sequence(seq_parts):
        q_row, k_rows, v_rows, length = seq_parts
        q_groups = q_row.reshape(KV_HEADS, KV_GROUP, HEAD_DIM).astype(jnp.float32)
        scores = jnp.einsum('grk,lgk->grl', q_groups, k_rows.astype(jnp.float32)) * SCORE_SCALE
        valid = jnp.arange(CACHE_LEN) <= length
        scores = jnp.where(valid[None, None, :], scores, -1e30)
        attn_prob = jax.nn.softmax(scores, axis=-1).astype(jnp.bfloat16)
        mixed = jnp.einsum('grl,lgk->grk', attn_prob.astype(jnp.float32), v_rows.astype(jnp.float32))
        return mixed.astype(jnp.bfloat16).reshape(HEADS * HEAD_DIM)

    attended = lax.map(one_sequence, (query, new_cache_k, new_cache_v, lengths))
    mid_hidden = (hidden_f + split_sum(attended, w_o)).astype(jnp.bfloat16)
    normed_mid = layer_norm1p(mid_hidden.astype(jnp.float32), ln2_gain, ln2_bias).astype(jnp.bfloat16)
    up_proj = jnp.dot(normed_mid, w_up, preferred_element_type=jnp.float32)
    activated = jnp.square(jnp.maximum(up_proj, 0.0)).astype(jnp.bfloat16)
    out_hidden = (mid_hidden.astype(jnp.float32) + split_sum(activated, w_down)).astype(jnp.bfloat16)
    normed_out = layer_norm1p(out_hidden.astype(jnp.float32), lnf_gain, lnf_bias).astype(jnp.bfloat16)
    logits = jnp.dot(normed_out, w_out, preferred_element_type=jnp.float32)
    peak = jnp.max(logits, axis=-1, keepdims=True)
    total = jnp.sum(jnp.exp(logits - peak), axis=-1, keepdims=True)
    log_probs = logits - (peak + jnp.log(total))
    return (log_probs, new_cache_k, new_cache_v, out_hidden)
```

```python
import functools

import jax
import jax.numpy as jnp
from jax import lax
from jax.experimental import pallas as pl
from jax.experimental.pallas import tpu as pltpu
from jax.sharding import PartitionSpec as P

EPSILON = 1e-5
ROPE_BASE = 10000.0
BF16 = jnp.bfloat16
F32 = jnp.float32
MESH = pl.DeviceIdType.MESH
RING = 14
ROWS = 512
NSEM = 26


def layer_norm1p(values, gain, bias):
    mean = jnp.mean(values, axis=-1, keepdims=True)
    centered = values - mean
    variance = jnp.mean(jnp.square(centered), axis=-1, keepdims=True)
    return centered * lax.rsqrt(variance + EPSILON) * (1.0 + gain) + bias


def apply_rotary(vecs, positions):
    rot_dim = vecs.shape[-1] // 2
    half_rot = rot_dim // 2
    exponent = -2.0 * jnp.arange(half_rot, dtype=jnp.float32) / rot_dim
    inv_freq = ROPE_BASE ** exponent
    angles = positions.astype(jnp.float32)[:, None] * inv_freq[None, :]
    cosine = jnp.cos(angles)[:, None, :]
    sine = jnp.sin(angles)[:, None, :]
    first = vecs[..., :half_rot]
    second = vecs[..., half_rot:rot_dim]
    return jnp.concatenate([first * cosine - second * sine, second * cosine + first * sine, vecs[..., rot_dim:]], axis=-1)


def project_and_attend(new_hidden, cache_k, cache_v, lengths, ln1_gain, ln1_bias, w_q, w_k, w_v):
    batch, cache_len, kv_heads, head_dim = cache_k.shape
    normed = layer_norm1p(new_hidden.astype(jnp.float32), ln1_gain, ln1_bias).astype(jnp.bfloat16)
    query = jnp.dot(normed, w_q, preferred_element_type=jnp.float32).reshape(batch, -1, head_dim)
    key_new = jnp.dot(normed, w_k, preferred_element_type=jnp.float32).reshape(batch, kv_heads, head_dim)
    val_new = jnp.dot(normed, w_v, preferred_element_type=jnp.float32).reshape(batch, kv_heads, head_dim)
    query = apply_rotary(query, lengths).astype(jnp.bfloat16)
    key_new = apply_rotary(key_new, lengths).astype(jnp.bfloat16)
    val_new = val_new.astype(jnp.bfloat16)
    positions = jnp.arange(cache_len)
    write_slot = (positions[None, :] == lengths[:, None])[:, :, None, None]
    new_cache_k = jnp.where(write_slot, key_new[:, None], cache_k)
    new_cache_v = jnp.where(write_slot, val_new[:, None], cache_v)
    group = query.shape[1] // kv_heads
    q_groups = query.reshape(batch, kv_heads, group, head_dim)
    score_scale = head_dim ** -0.5
    scores = jnp.einsum('bgrk,blgk->bgrl', q_groups, new_cache_k, preferred_element_type=jnp.float32) * score_scale
    valid = (positions[None, :] <= lengths[:, None])[:, None, None, :]
    scores = jnp.where(valid, scores, -1e30)
    attn_prob = jax.nn.softmax(scores, axis=-1).astype(jnp.bfloat16)
    mixed = jnp.einsum('bgrl,blgk->bgrk', attn_prob, new_cache_v, preferred_element_type=jnp.float32)
    return mixed.astype(jnp.bfloat16).reshape(batch, -1), new_cache_k, new_cache_v


def dotf(lhs, rhs):
    return jnp.dot(lhs, rhs, preferred_element_type=F32)


def fold(values):
    out = values[:, 0:128]
    for lane in range(128, values.shape[1], 128):
        out = out + values[:, lane:lane + 128]
    return out


def norm_chunks(chunks, gain, bias, out):
    count, rows, piece = chunks.shape
    width = count * piece
    total = jnp.zeros((rows, 128), F32)
    for j in range(count):
        total = total + fold(chunks[j].astype(F32))
    mean = jnp.sum(total, axis=-1, keepdims=True) / width
    total = jnp.zeros((rows, 128), F32)
    for j in range(count):
        total = total + fold(jnp.square(chunks[j].astype(F32) - mean))
    scale = lax.rsqrt(jnp.sum(total, axis=-1, keepdims=True) / width + EPSILON)
    for j in range(count):
        cols = slice(j * piece, (j + 1) * piece)
        normed = (chunks[j].astype(F32) - mean) * scale * (1.0 + gain[:, cols]) + bias[:, cols]
        out[:, cols] = normed.astype(BF16)


def tail_kernel(ways, attended, hidden, w_o, w_up, w_down, w_out, gain2, bias2, gainf, biasf,
                logits, norm_out, y_out,
                ring, last, resid, act, normed, normed_t, parts, raw1, raw2, sib, sibh, send3, recv3, own, gath, stats,
                w_sem, small_sem, send_sem, recv_sem, stat_send, stat_recv):
    me = lax.axis_index('tp')
    core = lax.rem(me, 2)
    chip = me // 2
    chips = ways // 2
    right = lax.rem(chip + 1, chips)
    left = lax.rem(chip + chips - 1, chips)
    far = lax.rem(chip + 2, chips)
    other = 1 - core
    rows, piece = resid.shape
    half = rows // 2
    top, bot = pl.ds(0, half), pl.ds(half, half)
    vocab, width = w_out.shape
    n_full = vocab // ROWS
    rest = vocab - n_full * ROWS
    s_o, s_up, s_down = RING - 5, RING - 4, RING - 2

    def dev(c, k):
        return {'tp': 2 * c + k}

    ld_res = pltpu.make_async_copy(hidden.at[:, pl.ds(pl.multiple_of(me * piece, piece), piece)], resid, small_sem.at[0])
    ld_o = pltpu.make_async_copy(w_o, ring.at[s_o, pl.ds(0, w_o.shape[0])], w_sem.at[s_o])
    ld_up = []
    for i in range(width // ROWS):
        ld_up.append(pltpu.make_async_copy(w_up.at[pl.ds(i * ROWS, ROWS)], ring.at[s_up + i // 3, :, pl.ds((i % 3) * w_up.shape[1], w_up.shape[1])], small_sem.at[4 + i]))
    ld_down = [pltpu.make_async_copy(w_down.at[pl.ds(i * ROWS, ROWS)], ring.at[s_down + i], small_sem.at[1 + i]) for i in range(2)]
    ld_last = pltpu.make_async_copy(w_out.at[pl.ds(n_full * ROWS, rest)], last, small_sem.at[3])

    def ld_tile(tile):
        slot = lax.rem(tile, RING)
        return pltpu.make_async_copy(w_out.at[pl.ds(pl.multiple_of(tile * ROWS, ROWS), ROWS)], ring.at[slot], w_sem.at[slot])

    ld_o.start()
    ld_res.start()
    for c in ld_up:
        c.start()
    for c in ld_down:
        c.start()
    for tile in range(s_o):
        ld_tile(tile).start()
    ld_last.start()

    barrier = pltpu.get_barrier_semaphore()
    for d in range(1, ways):
        pl.semaphore_signal(barrier, inc=1, device_id={'tp': lax.rem(me + d, ways)}, device_id_type=MESH)

    def copy(phase, idx, src, dst, to, ridx=None):
        ridx = idx if ridx is None else ridx
        return pltpu.make_async_remote_copy(src_ref=src, dst_ref=dst, send_sem=send_sem.at[phase, idx], recv_sem=recv_sem.at[phase, ridx],
                                            device_id=to, device_id_type=MESH)

    def arrive(phase, idx, dst):
        copy(phase, idx, dst, dst, dev(chip, core)).wait_recv()

    def all_sum(phase, product, residual, out_cols):
        pb = parts.at[phase]
        sent = []

        def go(c):
            c.start()
            sent.append(c)

        def term(c):
            value = product(c).astype(BF16)
            pb[2 * c] = value[:, :piece]
            pb[2 * c + 1] = value[:, piece:]

        g = gath.at[phase]
        term(far)
        if phase == 0:
            pl.semaphore_wait(barrier, ways - 1)
        for k in range(2):
            go(copy(phase, k, pb.at[2 * far + k, top], raw1.at[phase, 0, core], dev(right, k), core))
            go(copy(phase, 2 + k, pb.at[2 * far + k, bot], raw1.at[phase, 1, core], dev(left, k), 2 + core))
        term(right)
        for k in range(2):
            go(copy(phase, 6 + k, pb.at[2 * right + k, bot], raw2.at[phase, 1, core], dev(right, k), 6 + core))
        go(copy(phase, 9, pb.at[2 * right + other, top], sibh.at[phase, 0], dev(chip, other)))
        term(left)
        for k in range(2):
            go(copy(phase, 4 + k, pb.at[2 * left + k, top], raw2.at[phase, 0, core], dev(left, k), 4 + core))
        go(copy(phase, 10, pb.at[2 * left + other, bot], sibh.at[phase, 1], dev(chip, other)))
        term(chip)
        go(copy(phase, 8, pb.at[2 * chip + other], sib.at[phase], dev(chip, other)))
        for side, (to, rws) in enumerate(((right, top), (left, bot))):
            for k in range(2):
                arrive(phase, 2 * side + k, raw1.at[phase, side, k])
            arrive(phase, 9 + side, sibh.at[phase, side])
            send3[phase, side] = (raw1[phase, side, 0].astype(F32) + raw1[phase, side, 1].astype(F32)
                                  + pb[2 * to + core, rws].astype(F32) + sibh[phase, side].astype(F32))
            go(copy(phase, 11 + side, send3.at[phase, side], recv3.at[phase, side], dev(to, core)))
        arrive(phase, 8, sib.at[phase])
        for side, rws in enumerate((top, bot)):
            for k in range(2):
                arrive(phase, 4 + 2 * side + k, raw2.at[phase, side, k])
            base = (residual[rws].astype(F32) + pb[me, rws].astype(F32) + sib[phase, rws].astype(F32)
                    + raw2[phase, side, 0].astype(F32) + raw2[phase, side, 1].astype(F32))
            arrive(phase, 11 + side, recv3.at[phase, side])
            value = (base + recv3[phase, side]).astype(BF16)
            own[phase, rws] = value
            g[me, rws] = value
        ob = own.at[phase]
        go(copy(phase, 13, ob.at[top], g.at[me, top], dev(right, core)))
        go(copy(phase, 16, ob.at[bot], g.at[me, bot], dev(left, core)))
        go(copy(phase, 19, ob, g.at[me], dev(chip, other)))
        go(copy(phase, 14, ob.at[bot], g.at[me, bot], dev(right, core)))
        go(copy(phase, 15, ob.at[top], g.at[me, top], dev(left, core)))
        ml, mr, mf = 2 * left + core, 2 * right + core, 2 * far + core
        arrive(phase, 13, g.at[ml, top])
        go(copy(phase, 17, g.at[ml, top], g.at[ml, top], dev(right, core)))
        arrive(phase, 16, g.at[mr, bot])
        go(copy(phase, 18, g.at[mr, bot], g.at[mr, bot], dev(left, core)))
        go(copy(phase, 20, g.at[ml, top], g.at[ml, top], dev(chip, other)))
        go(copy(phase, 21, g.at[mr, bot], g.at[mr, bot], dev(chip, other)))
        arrive(phase, 14, g.at[ml, bot])
        go(copy(phase, 22, g.at[ml, bot], g.at[ml, bot], dev(chip, other)))
        arrive(phase, 15, g.at[mr, top])
        go(copy(phase, 23, g.at[mr, top], g.at[mr, top], dev(chip, other)))
        arrive(phase, 17, g.at[mf, top])
        go(copy(phase, 24, g.at[mf, top], g.at[mf, top], dev(chip, other)))
        arrive(phase, 18, g.at[mf, bot])
        go(copy(phase, 25, g.at[mf, bot], g.at[mf, bot], dev(chip, other)))
        ol, orr, of = 2 * left + other, 2 * right + other, 2 * far + other
        arrive(phase, 19, g.at[2 * chip + other])
        arrive(phase, 20, g.at[ol, top])
        arrive(phase, 21, g.at[orr, bot])
        arrive(phase, 22, g.at[ol, bot])
        arrive(phase, 23, g.at[orr, top])
        arrive(phase, 24, g.at[of, top])
        arrive(phase, 25, g.at[of, bot])
        return sent

    ld_o.wait()
    ld_res.wait()
    depth_o = w_o.shape[0]

    def product_o(c):
        return dotf(attended[...], ring[s_o, 0:depth_o, pl.ds(pl.multiple_of(2 * piece * c, 2 * piece), 2 * piece)])

    sent = all_sum(0, product_o, resid, None)
    ld_tile(s_o).start()
    norm_chunks(gath.at[0], gain2, bias2, normed)

    for c in ld_up:
        c.wait()
    ff = w_up.shape[1]
    for n in range(0, ff, 256):
        total = jnp.zeros((rows, 256), F32)
        for i in range(width // ROWS):
            total = total + dotf(normed[:, i * ROWS:(i + 1) * ROWS], ring[s_up + i // 3, :, (i % 3) * ff + n:(i % 3) * ff + n + 256])
        act[:, n:n + 256] = jnp.square(jnp.maximum(total, 0.0)).astype(BF16)
    ld_tile(s_up).start()
    ld_tile(s_up + 1).start()
    for c in ld_down:
        c.wait()

    def product_down(c):
        cols = pl.ds(pl.multiple_of(2 * piece * c, 2 * piece), 2 * piece)
        return dotf(act[:, :ROWS], ring[s_down, :, cols]) + dotf(act[:, ROWS:], ring[s_down + 1, :, cols])

    sent += all_sum(1, product_down, gath.at[0, me], None)
    ld_tile(s_down).start()
    ld_tile(s_down + 1).start()
    norm_chunks(gath.at[1], gainf, biasf, normed)
    for j in range(ways):
        y_out[:, j * piece:(j + 1) * piece] = gath[1, j]
        normed_t[j * piece:(j + 1) * piece] = normed[:, j * piece:(j + 1) * piece].T

    def reduce_tile(z, carry):
        peak, total = carry
        z3 = z.reshape(z.shape[0] // 8, 8, z.shape[1])
        new_peak = jnp.maximum(peak, jnp.max(z3, axis=0))
        total = total * jnp.exp(peak - new_peak) + jnp.sum(jnp.exp(z3 - new_peak[None]), axis=0)
        return new_peak, total

    def step(tile, carry):
        slot = lax.rem(tile, RING)
        ld_tile(tile).wait()
        z = dotf(ring[slot], normed_t[...])
        logits[pl.ds(pl.multiple_of(tile * ROWS, ROWS), ROWS)] = z

        @pl.when(tile + RING < n_full)
        def _():
            ld_tile(tile + RING).start()
        return reduce_tile(z, carry)

    carry = (jnp.full((8, rows), -1e30, F32), jnp.zeros((8, rows), F32))
    carry = lax.fori_loop(0, n_full, step, carry)
    ld_last.wait()
    z = dotf(last[...], normed_t[...])
    logits[pl.ds(n_full * ROWS, rest)] = z
    peak8, total8 = reduce_tile(z, carry)
    peak = jnp.max(peak8, axis=0, keepdims=True)
    total = jnp.sum(total8 * jnp.exp(peak8 - peak), axis=0, keepdims=True)
    row = lax.broadcasted_iota(jnp.int32, (8, rows), 0)
    stats[me] = jnp.where(row == 0, peak, total)
    stat_out = []
    for d in range(1, ways):
        c = pltpu.make_async_remote_copy(src_ref=stats.at[me], dst_ref=stats.at[me], send_sem=stat_send.at[d], recv_sem=stat_recv.at[d],
                                         device_id={'tp': lax.rem(me + d, ways)}, device_id_type=MESH)
        c.start()
        stat_out.append(c)
    for d in range(1, ways):
        src = lax.rem(me + ways - d, ways)
        pltpu.make_async_remote_copy(src_ref=stats.at[src], dst_ref=stats.at[src], send_sem=stat_send.at[d], recv_sem=stat_recv.at[d],
                                     device_id={'tp': me}, device_id_type=MESH).wait_recv()
    all_stats = stats[...]
    peaks = all_stats[:, 0, :]
    totals = all_stats[:, 1, :]
    top_peak = jnp.max(peaks, axis=0, keepdims=True)
    whole = jnp.sum(totals * jnp.exp(peaks - top_peak), axis=0, keepdims=True)
    norm_out[...] = jnp.broadcast_to(top_peak + jnp.log(whole), norm_out.shape)
    for c in sent + stat_out:
        c.wait_send()


def run_tail(ways, attended, hidden, w_o, w_up, w_down, w_out_t, gain2, bias2, gainf, biasf):
    rows, width = hidden.shape
    piece = width // ways
    half = rows // 2
    vocab = w_out_t.shape[0]
    rest = vocab % ROWS
    ff = w_up.shape[1]
    any_ = pl.BlockSpec(memory_space=pl.ANY)
    vmem = pl.BlockSpec(memory_space=pltpu.VMEM)
    hbm = pl.BlockSpec(memory_space=pltpu.HBM)
    return pl.pallas_call(
        functools.partial(tail_kernel, ways),
        out_shape=(pltpu.VMEM((vocab, rows), F32), pltpu.VMEM((8, rows), F32), pltpu.VMEM((rows, width), BF16)),
        in_specs=[vmem, hbm, hbm, hbm, hbm, hbm, vmem, vmem, vmem, vmem],
        out_specs=(vmem, vmem, vmem),
        scratch_shapes=[
            pltpu.VMEM((RING, ROWS, width), BF16),
            pltpu.VMEM((rest, width), BF16),
            pltpu.VMEM((rows, piece), BF16),
            pltpu.VMEM((rows, ff), BF16),
            pltpu.VMEM((rows, width), BF16),
            pltpu.VMEM((width, rows), BF16),
            pltpu.VMEM((2, ways, rows, piece), BF16),
            pltpu.VMEM((2, 2, 2, half, piece), BF16),
            pltpu.VMEM((2, 2, 2, half, piece), BF16),
            pltpu.VMEM((2, rows, piece), BF16),
            pltpu.VMEM((2, 2, half, piece), BF16),
            pltpu.VMEM((2, 2, half, piece), F32),
            pltpu.VMEM((2, 2, half, piece), F32),
            pltpu.VMEM((2, rows, piece), BF16),
            pltpu.VMEM((2, ways, rows, piece), BF16),
            pltpu.VMEM((ways, 8, rows), F32),
            pltpu.SemaphoreType.DMA((RING,)),
            pltpu.SemaphoreType.DMA((10,)),
            pltpu.SemaphoreType.DMA((2, NSEM)),
            pltpu.SemaphoreType.DMA((2, NSEM)),
            pltpu.SemaphoreType.DMA((ways,)),
            pltpu.SemaphoreType.DMA((ways,)),
        ],
        compiler_params=pltpu.CompilerParams(collective_id=0, has_side_effects=True, vmem_limit_bytes=LIMIT),
        name='tail',
    )(attended, hidden, w_o, w_up, w_down, w_out_t, gain2, bias2, gainf, biasf)


LIMIT = 54 * 1024 * 1024


def finish_kernel(logits, norm, y, out, y_out, sem):
    copy = pltpu.make_async_copy(y, y_out, sem)

    @pl.when(pl.program_id(0) == 0)
    def _():
        copy.start()

    block = out.shape[0]
    start = pl.multiple_of(pl.program_id(0) * block, 8)
    out[...] = logits[pl.ds(start, block)] - norm[0:1]

    @pl.when(pl.program_id(0) == pl.num_programs(0) - 1)
    def _():
        copy.wait()


def run_finish(logits, norm, y):
    vocab, rows = logits.shape
    block = vocab // 12
    vmem = pl.BlockSpec(memory_space=pltpu.VMEM)
    return pl.pallas_call(
        finish_kernel,
        grid=(12,),
        out_shape=(jax.ShapeDtypeStruct((vocab, rows), F32), jax.ShapeDtypeStruct(y.shape, BF16)),
        in_specs=[vmem, vmem, vmem],
        out_specs=(pl.BlockSpec((block, rows), lambda i: (i, 0)), pl.BlockSpec(memory_space=pltpu.HBM)),
        scratch_shapes=[pltpu.SemaphoreType.DMA],
        compiler_params=pltpu.CompilerParams(vmem_limit_bytes=8 * 1024 * 1024),
        name='finish',
    )(logits, norm, y)


def solution(mesh):
    ways = mesh.shape['tp']
    row_spec = P('bs', None)
    cache_spec = P('bs', None, 'tp', None)
    col_split = P(None, 'tp')
    row_split = P('tp', None)
    in_specs = (row_spec, cache_spec, cache_spec, P('bs'), P(), P(), col_split, col_split, col_split, row_split, P(), P(), col_split, row_split, P(), P(), col_split)
    out_specs = (P('bs', 'tp'), cache_spec, cache_spec, row_spec)

    def local_step(new_hidden, cache_k, cache_v, lengths, ln1_gain, ln1_bias, w_q, w_k, w_v, w_o, ln2_gain, ln2_bias, w_up, w_down, lnf_gain, lnf_bias, w_out):
        attended, new_cache_k, new_cache_v = project_and_attend(new_hidden, cache_k, cache_v, lengths, ln1_gain, ln1_bias, w_q, w_k, w_v)
        logits, norm, y = run_tail(ways, attended, new_hidden, w_o, w_up, w_down, w_out.T,
                                   ln2_gain[None], ln2_bias[None], lnf_gain[None], lnf_bias[None])
        log_probs_t, out_hidden = run_finish(logits, norm, y)
        return log_probs_t.T, new_cache_k, new_cache_v, out_hidden

    return jax.shard_map(local_step, mesh=mesh, in_specs=in_specs, out_specs=out_specs, check_vma=False)
```

```python
import functools
import math

import jax
import jax.numpy as jnp
from jax import lax
from jax.experimental import pallas as pl
from jax.experimental.pallas import tpu as pltpu
from jax.sharding import PartitionSpec as P

EPSILON = 1e-5
ROPE_BASE = 10000.0
BF16 = jnp.bfloat16
F32 = jnp.float32
MESH = pl.DeviceIdType.MESH
RING = 14
ROWS = 512
NSEM = 26


def dotf(lhs, rhs):
    return jnp.dot(lhs, rhs, preferred_element_type=F32)


def fold(values):
    out = values[:, 0:128]
    for lane in range(128, values.shape[1], 128):
        out = out + values[:, lane:lane + 128]
    return out


def norm_chunks(chunks, gain, bias, out):
    count, rows, piece = chunks.shape
    width = count * piece
    total = jnp.zeros((rows, 128), F32)
    for j in range(count):
        total = total + fold(chunks[j].astype(F32))
    mean = jnp.sum(total, axis=-1, keepdims=True) / width
    total = jnp.zeros((rows, 128), F32)
    for j in range(count):
        total = total + fold(jnp.square(chunks[j].astype(F32) - mean))
    scale = lax.rsqrt(jnp.sum(total, axis=-1, keepdims=True) / width + EPSILON)
    for j in range(count):
        cols = slice(j * piece, (j + 1) * piece)
        normed = (chunks[j].astype(F32) - mean) * scale * (1.0 + gain[:, cols]) + bias[:, cols]
        out[:, cols] = normed.astype(BF16)


def tail_kernel(ways, attended, hidden, w_o, w_up, w_down, w_out, gain2, bias2, gainf, biasf,
                logits, norm_out, y_out,
                ring, last, resid, act, normed, normed_t, parts, raw1, raw2, sib, sibh, send3, recv3, own, gath, stats,
                w_sem, small_sem, send_sem, recv_sem, stat_send, stat_recv):
    me = lax.axis_index('tp')
    core = lax.rem(me, 2)
    chip = me // 2
    chips = ways // 2
    right = lax.rem(chip + 1, chips)
    left = lax.rem(chip + chips - 1, chips)
    far = lax.rem(chip + 2, chips)
    other = 1 - core
    rows, piece = resid.shape
    half = rows // 2
    top, bot = pl.ds(0, half), pl.ds(half, half)
    vocab, width = w_out.shape
    n_full = vocab // ROWS
    rest = vocab - n_full * ROWS
    s_o, s_up, s_down = RING - 5, RING - 4, RING - 2

    def dev(c, k):
        return {'tp': 2 * c + k}

    ld_res = pltpu.make_async_copy(hidden.at[:, pl.ds(pl.multiple_of(me * piece, piece), piece)], resid, small_sem.at[0])
    ld_o = pltpu.make_async_copy(w_o, ring.at[s_o, pl.ds(0, w_o.shape[0])], w_sem.at[s_o])
    ld_up = []
    for i in range(width // ROWS):
        ld_up.append(pltpu.make_async_copy(w_up.at[pl.ds(i * ROWS, ROWS)], ring.at[s_up + i // 3, :, pl.ds((i % 3) * w_up.shape[1], w_up.shape[1])], small_sem.at[4 + i]))
    ld_down = [pltpu.make_async_copy(w_down.at[pl.ds(i * ROWS, ROWS)], ring.at[s_down + i], small_sem.at[1 + i]) for i in range(2)]
    ld_last = pltpu.make_async_copy(w_out.at[pl.ds(n_full * ROWS, rest)], last, small_sem.at[3])

    def ld_tile(tile):
        slot = lax.rem(tile, RING)
        return pltpu.make_async_copy(w_out.at[pl.ds(pl.multiple_of(tile * ROWS, ROWS), ROWS)], ring.at[slot], w_sem.at[slot])

    ld_o.start()
    ld_res.start()
    for c in ld_up:
        c.start()
    for c in ld_down:
        c.start()
    for tile in range(s_o):
        ld_tile(tile).start()
    ld_last.start()

    barrier = pltpu.get_barrier_semaphore()
    for d in range(1, ways):
        pl.semaphore_signal(barrier, inc=1, device_id={'tp': lax.rem(me + d, ways)}, device_id_type=MESH)

    def copy(phase, idx, src, dst, to, ridx=None):
        ridx = idx if ridx is None else ridx
        return pltpu.make_async_remote_copy(src_ref=src, dst_ref=dst, send_sem=send_sem.at[phase, idx], recv_sem=recv_sem.at[phase, ridx],
                                            device_id=to, device_id_type=MESH)

    def arrive(phase, idx, dst):
        copy(phase, idx, dst, dst, dev(chip, core)).wait_recv()

    def all_sum(phase, product, residual, out_cols):
        pb = parts.at[phase]
        sent = []

        def go(c):
            c.start()
            sent.append(c)

        def term(c):
            value = product(c).astype(BF16)
            pb[2 * c] = value[:, :piece]
            pb[2 * c + 1] = value[:, piece:]

        g = gath.at[phase]
        term(far)
        if phase == 0:
            pl.semaphore_wait(barrier, ways - 1)
        for k in range(2):
            go(copy(phase, k, pb.at[2 * far + k, top], raw1.at[phase, 0, core], dev(right, k), core))
            go(copy(phase, 2 + k, pb.at[2 * far + k, bot], raw1.at[phase, 1, core], dev(left, k), 2 + core))
        term(right)
        for k in range(2):
            go(copy(phase, 6 + k, pb.at[2 * right + k, bot], raw2.at[phase, 1, core], dev(right, k), 6 + core))
        go(copy(phase, 9, pb.at[2 * right + other, top], sibh.at[phase, 0], dev(chip, other)))
        term(left)
        for k in range(2):
            go(copy(phase, 4 + k, pb.at[2 * left + k, top], raw2.at[phase, 0, core], dev(left, k), 4 + core))
        go(copy(phase, 10, pb.at[2 * left + other, bot], sibh.at[phase, 1], dev(chip, other)))
        term(chip)
        go(copy(phase, 8, pb.at[2 * chip + other], sib.at[phase], dev(chip, other)))
        for side, (to, rws) in enumerate(((right, top), (left, bot))):
            for k in range(2):
                arrive(phase, 2 * side + k, raw1.at[phase, side, k])
            arrive(phase, 9 + side, sibh.at[phase, side])
            send3[phase, side] = (raw1[phase, side, 0].astype(F32) + raw1[phase, side, 1].astype(F32)
                                  + pb[2 * to + core, rws].astype(F32) + sibh[phase, side].astype(F32))
            go(copy(phase, 11 + side, send3.at[phase, side], recv3.at[phase, side], dev(to, core)))
        arrive(phase, 8, sib.at[phase])
        for side, rws in enumerate((top, bot)):
            for k in range(2):
                arrive(phase, 4 + 2 * side + k, raw2.at[phase, side, k])
            base = (residual[rws].astype(F32) + pb[me, rws].astype(F32) + sib[phase, rws].astype(F32)
                    + raw2[phase, side, 0].astype(F32) + raw2[phase, side, 1].astype(F32))
            arrive(phase, 11 + side, recv3.at[phase, side])
            value = (base + recv3[phase, side]).astype(BF16)
            own[phase, rws] = value
            g[me, rws] = value
        ob = own.at[phase]
        go(copy(phase, 13, ob.at[top], g.at[me, top], dev(right, core)))
        go(copy(phase, 16, ob.at[bot], g.at[me, bot], dev(left, core)))
        go(copy(phase, 19, ob, g.at[me], dev(chip, other)))
        go(copy(phase, 14, ob.at[bot], g.at[me, bot], dev(right, core)))
        go(copy(phase, 15, ob.at[top], g.at[me, top], dev(left, core)))
        ml, mr, mf = 2 * left + core, 2 * right + core, 2 * far + core
        arrive(phase, 13, g.at[ml, top])
        go(copy(phase, 17, g.at[ml, top], g.at[ml, top], dev(right, core)))
        arrive(phase, 16, g.at[mr, bot])
        go(copy(phase, 18, g.at[mr, bot], g.at[mr, bot], dev(left, core)))
        go(copy(phase, 20, g.at[ml, top], g.at[ml, top], dev(chip, other)))
        go(copy(phase, 21, g.at[mr, bot], g.at[mr, bot], dev(chip, other)))
        arrive(phase, 14, g.at[ml, bot])
        go(copy(phase, 22, g.at[ml, bot], g.at[ml, bot], dev(chip, other)))
        arrive(phase, 15, g.at[mr, top])
        go(copy(phase, 23, g.at[mr, top], g.at[mr, top], dev(chip, other)))
        arrive(phase, 17, g.at[mf, top])
        go(copy(phase, 24, g.at[mf, top], g.at[mf, top], dev(chip, other)))
        arrive(phase, 18, g.at[mf, bot])
        go(copy(phase, 25, g.at[mf, bot], g.at[mf, bot], dev(chip, other)))
        ol, orr, of = 2 * left + other, 2 * right + other, 2 * far + other
        arrive(phase, 19, g.at[2 * chip + other])
        arrive(phase, 20, g.at[ol, top])
        arrive(phase, 21, g.at[orr, bot])
        arrive(phase, 22, g.at[ol, bot])
        arrive(phase, 23, g.at[orr, top])
        arrive(phase, 24, g.at[of, top])
        arrive(phase, 25, g.at[of, bot])
        return sent

    ld_o.wait()
    ld_res.wait()
    depth_o = w_o.shape[0]

    def product_o(c):
        return dotf(attended[...], ring[s_o, 0:depth_o, pl.ds(pl.multiple_of(2 * piece * c, 2 * piece), 2 * piece)])

    sent = all_sum(0, product_o, resid, None)
    ld_tile(s_o).start()
    norm_chunks(gath.at[0], gain2, bias2, normed)

    for c in ld_up:
        c.wait()
    ff = w_up.shape[1]
    for n in range(0, ff, 256):
        total = jnp.zeros((rows, 256), F32)
        for i in range(width // ROWS):
            total = total + dotf(normed[:, i * ROWS:(i + 1) * ROWS], ring[s_up + i // 3, :, (i % 3) * ff + n:(i % 3) * ff + n + 256])
        act[:, n:n + 256] = jnp.square(jnp.maximum(total, 0.0)).astype(BF16)
    ld_tile(s_up).start()
    ld_tile(s_up + 1).start()
    for c in ld_down:
        c.wait()

    def product_down(c):
        cols = pl.ds(pl.multiple_of(2 * piece * c, 2 * piece), 2 * piece)
        return dotf(act[:, :ROWS], ring[s_down, :, cols]) + dotf(act[:, ROWS:], ring[s_down + 1, :, cols])

    sent += all_sum(1, product_down, gath.at[0, me], None)
    ld_tile(s_down).start()
    ld_tile(s_down + 1).start()
    norm_chunks(gath.at[1], gainf, biasf, normed)
    for j in range(ways):
        y_out[:, j * piece:(j + 1) * piece] = gath[1, j]
        normed_t[j * piece:(j + 1) * piece] = normed[:, j * piece:(j + 1) * piece].T

    def reduce_tile(z, carry):
        peak, total = carry
        z3 = z.reshape(z.shape[0] // 8, 8, z.shape[1])
        new_peak = jnp.maximum(peak, jnp.max(z3, axis=0))
        total = total * jnp.exp(peak - new_peak) + jnp.sum(jnp.exp(z3 - new_peak[None]), axis=0)
        return new_peak, total

    def step(tile, carry):
        slot = lax.rem(tile, RING)
        ld_tile(tile).wait()
        z = dotf(ring[slot], normed_t[...])
        logits[pl.ds(pl.multiple_of(tile * ROWS, ROWS), ROWS)] = z

        @pl.when(tile + RING < n_full)
        def _():
            ld_tile(tile + RING).start()
        return reduce_tile(z, carry)

    carry = (jnp.full((8, rows), -1e30, F32), jnp.zeros((8, rows), F32))
    carry = lax.fori_loop(0, n_full, step, carry)
    ld_last.wait()
    z = dotf(last[...], normed_t[...])
    logits[pl.ds(n_full * ROWS, rest)] = z
    peak8, total8 = reduce_tile(z, carry)
    peak = jnp.max(peak8, axis=0, keepdims=True)
    total = jnp.sum(total8 * jnp.exp(peak8 - peak), axis=0, keepdims=True)
    row = lax.broadcasted_iota(jnp.int32, (8, rows), 0)
    stats[me] = jnp.where(row == 0, peak, total)
    stat_out = []
    for d in range(1, ways):
        c = pltpu.make_async_remote_copy(src_ref=stats.at[me], dst_ref=stats.at[me], send_sem=stat_send.at[d], recv_sem=stat_recv.at[d],
                                         device_id={'tp': lax.rem(me + d, ways)}, device_id_type=MESH)
        c.start()
        stat_out.append(c)
    for d in range(1, ways):
        src = lax.rem(me + ways - d, ways)
        pltpu.make_async_remote_copy(src_ref=stats.at[src], dst_ref=stats.at[src], send_sem=stat_send.at[d], recv_sem=stat_recv.at[d],
                                     device_id={'tp': me}, device_id_type=MESH).wait_recv()
    all_stats = stats[...]
    peaks = all_stats[:, 0, :]
    totals = all_stats[:, 1, :]
    top_peak = jnp.max(peaks, axis=0, keepdims=True)
    whole = jnp.sum(totals * jnp.exp(peaks - top_peak), axis=0, keepdims=True)
    norm_out[...] = jnp.broadcast_to(top_peak + jnp.log(whole), norm_out.shape)
    for c in sent + stat_out:
        c.wait_send()


def run_tail(ways, attended, hidden, w_o, w_up, w_down, w_out_t, gain2, bias2, gainf, biasf):
    rows, width = hidden.shape
    piece = width // ways
    half = rows // 2
    vocab = w_out_t.shape[0]
    rest = vocab % ROWS
    ff = w_up.shape[1]
    any_ = pl.BlockSpec(memory_space=pl.ANY)
    vmem = pl.BlockSpec(memory_space=pltpu.VMEM)
    hbm = pl.BlockSpec(memory_space=pltpu.HBM)
    return pl.pallas_call(
        functools.partial(tail_kernel, ways),
        out_shape=(pltpu.VMEM((vocab, rows), F32), pltpu.VMEM((8, rows), F32), pltpu.VMEM((rows, width), BF16)),
        in_specs=[vmem, hbm, hbm, hbm, hbm, hbm, vmem, vmem, vmem, vmem],
        out_specs=(vmem, vmem, vmem),
        scratch_shapes=[
            pltpu.VMEM((RING, ROWS, width), BF16),
            pltpu.VMEM((rest, width), BF16),
            pltpu.VMEM((rows, piece), BF16),
            pltpu.VMEM((rows, ff), BF16),
            pltpu.VMEM((rows, width), BF16),
            pltpu.VMEM((width, rows), BF16),
            pltpu.VMEM((2, ways, rows, piece), BF16),
            pltpu.VMEM((2, 2, 2, half, piece), BF16),
            pltpu.VMEM((2, 2, 2, half, piece), BF16),
            pltpu.VMEM((2, rows, piece), BF16),
            pltpu.VMEM((2, 2, half, piece), BF16),
            pltpu.VMEM((2, 2, half, piece), F32),
            pltpu.VMEM((2, 2, half, piece), F32),
            pltpu.VMEM((2, rows, piece), BF16),
            pltpu.VMEM((2, ways, rows, piece), BF16),
            pltpu.VMEM((ways, 8, rows), F32),
            pltpu.SemaphoreType.DMA((RING,)),
            pltpu.SemaphoreType.DMA((10,)),
            pltpu.SemaphoreType.DMA((2, NSEM)),
            pltpu.SemaphoreType.DMA((2, NSEM)),
            pltpu.SemaphoreType.DMA((ways,)),
            pltpu.SemaphoreType.DMA((ways,)),
        ],
        compiler_params=pltpu.CompilerParams(collective_id=0, has_side_effects=True, vmem_limit_bytes=LIMIT),
        name='tail',
    )(pltpu.with_memory_space_constraint(attended, pltpu.VMEM), hidden, w_o, w_up, w_down, w_out_t, gain2, bias2, gainf, biasf)


LIMIT = 53 * 1024 * 1024


CHUNKS = 4


def attend_kernel(hidden, lengths, gain, bias, w_q, w_k, w_v, cache_k, cache_v,
                  attended, out_k, out_v,
                  x, gb, len_row, normed, w_qkv, qkv, len_col, k_buf, v_buf, misc_sem, w_sem, in_sem, out_sem):
    rows, width = hidden.shape
    seqs, slots, dim = cache_k.shape
    q_cols = w_q.shape[1]
    heads = q_cols // dim
    step_w = width // CHUNKS
    step_s = seqs // CHUNKS

    small = [pltpu.make_async_copy(hidden, x, misc_sem.at[0]),
             pltpu.make_async_copy(gain, gb.at[pl.ds(0, 1)], misc_sem.at[1]),
             pltpu.make_async_copy(bias, gb.at[pl.ds(1, 1)], misc_sem.at[2]),
             pltpu.make_async_copy(lengths, len_row, misc_sem.at[3])]
    for c in small:
        c.start()
    w_in = []
    for i in range(CHUNKS):
        part = pl.ds(i * step_w, step_w)
        w_in.append([pltpu.make_async_copy(w_q.at[part], w_qkv.at[part, pl.ds(0, q_cols)], w_sem.at[0, i]),
                     pltpu.make_async_copy(w_k.at[part], w_qkv.at[part, pl.ds(q_cols, dim)], w_sem.at[1, i]),
                     pltpu.make_async_copy(w_v.at[part], w_qkv.at[part, pl.ds(q_cols + dim, dim)], w_sem.at[2, i])])
        for c in w_in[-1]:
            c.start()
    kv_in, kv_out = [], []
    for i in range(CHUNKS):
        part = pl.ds(i * step_s, step_s)
        kv_in.append([pltpu.make_async_copy(cache_k.at[part], k_buf.at[part], in_sem.at[0, i]),
                      pltpu.make_async_copy(cache_v.at[part], v_buf.at[part], in_sem.at[1, i])])
        kv_out.append([pltpu.make_async_copy(k_buf.at[part], out_k.at[part], out_sem.at[0, i]),
                       pltpu.make_async_copy(v_buf.at[part], out_v.at[part], out_sem.at[1, i])])
        for c in kv_in[-1]:
            c.start()

    small[3].wait()
    lens = jnp.broadcast_to(len_row[...].astype(F32), (rows, rows)).T
    len_col[...] = lens
    lane = lax.broadcasted_iota(jnp.int32, (1, dim), 1)
    half_rot = dim // 4
    freq_lane = jnp.where(lane < half_rot, lane, lane - half_rot).astype(F32)
    inv_freq = jnp.where(lane < 2 * half_rot, jnp.exp(freq_lane * (-2.0 / (2 * half_rot) * math.log(ROPE_BASE))), 0.0)
    angle = lens * inv_freq
    cosine = jnp.cos(angle)
    sine = jnp.where(lane < half_rot, -1.0, 1.0) * jnp.sin(angle)
    for c in small[:3]:
        c.wait()
    total = jnp.zeros((rows, 128), F32)
    piece = width // 8
    for j in range(8):
        total = total + fold(x[:, j * piece:(j + 1) * piece].astype(F32))
    mean = jnp.sum(total, axis=-1, keepdims=True) / width
    total = jnp.zeros((rows, 128), F32)
    for j in range(8):
        total = total + fold(jnp.square(x[:, j * piece:(j + 1) * piece].astype(F32) - mean))
    scale = lax.rsqrt(jnp.sum(total, axis=-1, keepdims=True) / width + EPSILON)
    for j in range(8):
        cols = slice(j * piece, (j + 1) * piece)
        normed[:, cols] = ((x[:, cols].astype(F32) - mean) * scale * (1.0 + gb[0:1, cols]) + gb[1:2, cols]).astype(BF16)

    for i in range(CHUNKS):
        for c in w_in[i]:
            c.wait()
        part = slice(i * step_w, (i + 1) * step_w)
        product = dotf(normed[:, part], w_qkv[part])
        if i == 0:
            qkv[...] = product
        else:
            qkv[...] += product
    for h in range(heads + 1):
        cols = slice(h * dim, (h + 1) * dim)
        vec = qkv[:, cols]
        partner = jnp.where(lane < half_rot, pltpu.roll(vec, dim - half_rot, 1), pltpu.roll(vec, half_rot, 1))
        qkv[:, cols] = vec * cosine + partner * sine

    row_id = lax.broadcasted_iota(jnp.int32, (slots, dim), 0).astype(F32)
    group = 8
    span = group * slots
    offset = (lax.broadcasted_iota(jnp.int32, (group, span), 1) - slots * lax.broadcasted_iota(jnp.int32, (group, span), 0)).astype(F32)
    k_cols, v_cols = slice(q_cols, q_cols + dim), slice(q_cols + dim, q_cols + 2 * dim)
    for i in range(CHUNKS):
        for c in kv_in[i]:
            c.wait()

        def put(s, carry):
            base = pl.multiple_of(i * step_s + s * 8, 8)
            lens8 = len_col[pl.ds(base, 8), :]
            new_k = qkv[pl.ds(base, 8), k_cols]
            new_v = qkv[pl.ds(base, 8), v_cols]
            for t in range(8):
                here = row_id == lens8[t:t + 1]
                k_buf[base + t] = jnp.where(here, new_k[t:t + 1], k_buf[base + t].astype(F32)).astype(BF16)
                v_buf[base + t] = jnp.where(here, new_v[t:t + 1], v_buf[base + t].astype(F32)).astype(BF16)
            return carry

        lax.fori_loop(0, step_s // 8, put, 0)
        for c in kv_out[i]:
            c.start()
        for g in range(step_s // group):
            b = i * step_s + g * group
            q = jnp.concatenate([qkv[b:b + group, h * dim:(h + 1) * dim] for h in range(heads)], axis=0).astype(BF16)
            keys = k_buf[b:b + group].reshape(span, dim)
            vals = v_buf[b:b + group].reshape(span, dim)
            scores = lax.dot_general(q, keys, (((1,), (1,)), ((), ())), preferred_element_type=F32) * (dim ** -0.5)
            lens8 = len_col[b:b + group, 0:1]
            valid = (offset >= 0.0) & (offset <= lens8)
            scores = jnp.where(valid[None], scores.reshape(heads, group, span), -1e30)
            peak = jnp.max(scores, axis=-1, keepdims=True)
            weight = jnp.where(valid[None], jnp.exp(scores - peak), 0.0)
            prob = (weight / jnp.sum(weight, axis=-1, keepdims=True)).astype(BF16)
            mixed = dotf(prob.reshape(heads * group, span), vals).astype(BF16)
            for h in range(heads):
                attended[b:b + group, h * dim:(h + 1) * dim] = mixed[h * group:(h + 1) * group]
    for pair in kv_out:
        for c in pair:
            c.wait()


def run_attend(hidden, cache_k, cache_v, lengths, gain, bias, w_q, w_k, w_v):
    rows, width = hidden.shape
    seqs, slots, dim = cache_k.shape
    q_cols = w_q.shape[1]
    hbm = pl.BlockSpec(memory_space=pltpu.HBM)
    vmem = pl.BlockSpec(memory_space=pltpu.VMEM)
    return pl.pallas_call(
        attend_kernel,
        out_shape=(pltpu.VMEM((rows, q_cols), BF16), jax.ShapeDtypeStruct(cache_k.shape, BF16), jax.ShapeDtypeStruct(cache_v.shape, BF16)),
        in_specs=[hbm] * 9,
        out_specs=(vmem, hbm, hbm),
        scratch_shapes=[
            pltpu.VMEM((rows, width), BF16),
            pltpu.VMEM((8, width), F32),
            pltpu.VMEM((1, rows), jnp.int32),
            pltpu.VMEM((rows, width), BF16),
            pltpu.VMEM((width, q_cols + 2 * dim), BF16),
            pltpu.VMEM((rows, q_cols + 2 * dim), F32),
            pltpu.VMEM((rows, rows), F32),
            pltpu.VMEM((seqs, slots, dim), BF16),
            pltpu.VMEM((seqs, slots, dim), BF16),
            pltpu.SemaphoreType.DMA((4,)),
            pltpu.SemaphoreType.DMA((3, CHUNKS)),
            pltpu.SemaphoreType.DMA((2, CHUNKS)),
            pltpu.SemaphoreType.DMA((2, CHUNKS)),
        ],
        compiler_params=pltpu.CompilerParams(vmem_limit_bytes=62 * 1024 * 1024),
        name='attend',
    )(hidden, lengths, gain, bias, w_q, w_k, w_v, cache_k, cache_v)


PARTS = 8


def finish_kernel(logits, norm, y, out, y_out, buf, sem, y_sem):
    copy = pltpu.make_async_copy(y, y_out, y_sem)
    copy.start()
    block = logits.shape[0] // PARTS // 8 * 8
    outs = []
    for i in range(PARTS):
        size = block if i < PARTS - 1 else logits.shape[0] - block * (PARTS - 1)
        part = pl.ds(i * block, size)
        buf[part] = logits[part] - norm[0:1]
        outs.append(pltpu.make_async_copy(buf.at[part], out.at[part], sem.at[i]))
        outs[-1].start()
    for c in outs:
        c.wait()
    copy.wait()


def run_finish(logits, norm, y):
    vocab, rows = logits.shape
    vmem = pl.BlockSpec(memory_space=pltpu.VMEM)
    hbm = pl.BlockSpec(memory_space=pltpu.HBM)
    return pl.pallas_call(
        finish_kernel,
        out_shape=(jax.ShapeDtypeStruct((vocab, rows), F32), jax.ShapeDtypeStruct(y.shape, BF16)),
        in_specs=[vmem, vmem, vmem],
        out_specs=(hbm, hbm),
        scratch_shapes=[pltpu.VMEM((vocab, rows), F32), pltpu.SemaphoreType.DMA((PARTS,)), pltpu.SemaphoreType.DMA],
        compiler_params=pltpu.CompilerParams(vmem_limit_bytes=16 * 1024 * 1024),
        name='finish',
    )(logits, norm, y)


def solution(mesh):
    ways = mesh.shape['tp']
    row_spec = P('bs', None)
    cache_spec = P('bs', None, 'tp', None)
    col_split = P(None, 'tp')
    row_split = P('tp', None)
    in_specs = (row_spec, cache_spec, cache_spec, P('bs'), P(), P(), col_split, col_split, col_split, row_split, P(), P(), col_split, row_split, P(), P(), col_split)
    out_specs = (P('bs', 'tp'), cache_spec, cache_spec, row_spec)

    def local_step(new_hidden, cache_k, cache_v, lengths, ln1_gain, ln1_bias, w_q, w_k, w_v, w_o, ln2_gain, ln2_bias, w_up, w_down, lnf_gain, lnf_bias, w_out):
        shape = cache_k.shape
        flat = (shape[0], shape[1], shape[3])
        attended, new_cache_k, new_cache_v = run_attend(new_hidden, cache_k.reshape(flat), cache_v.reshape(flat), lengths[None], ln1_gain[None], ln1_bias[None], w_q, w_k, w_v)
        logits, norm, y = run_tail(ways, attended, new_hidden, w_o, w_up, w_down, w_out.T,
                                   ln2_gain[None], ln2_bias[None], lnf_gain[None], lnf_bias[None])
        log_probs_t, out_hidden = run_finish(logits, norm, y)
        return log_probs_t.T, new_cache_k.reshape(shape), new_cache_v.reshape(shape), out_hidden

    return jax.shard_map(local_step, mesh=mesh, in_specs=in_specs, out_specs=out_specs, check_vma=False)
```

```python
import functools
import math

import jax
import jax.numpy as jnp
from jax import lax
from jax.experimental import pallas as pl
from jax.experimental.pallas import tpu as pltpu
from jax.sharding import PartitionSpec as P

EPSILON = 1e-5
ROPE_BASE = 10000.0
BF16 = jnp.bfloat16
F32 = jnp.float32
MESH = pl.DeviceIdType.MESH
RING = 14
FLIPS = 12
BLOCK = 256
ROWS = 512
NSEM = 26


def dotf(lhs, rhs):
    return jnp.dot(lhs, rhs, preferred_element_type=F32)


def fold(values):
    out = values[:, 0:128]
    for lane in range(128, values.shape[1], 128):
        out = out + values[:, lane:lane + 128]
    return out


def norm_chunks(chunks, gain, bias, out):
    count, rows, piece = chunks.shape
    width = count * piece
    total = jnp.zeros((rows, 128), F32)
    for j in range(count):
        total = total + fold(chunks[j].astype(F32))
    mean = jnp.sum(total, axis=-1, keepdims=True) / width
    total = jnp.zeros((rows, 128), F32)
    for j in range(count):
        total = total + fold(jnp.square(chunks[j].astype(F32) - mean))
    scale = lax.rsqrt(jnp.sum(total, axis=-1, keepdims=True) / width + EPSILON)
    for j in range(count):
        cols = slice(j * piece, (j + 1) * piece)
        normed = (chunks[j].astype(F32) - mean) * scale * (1.0 + gain[:, cols]) + bias[:, cols]
        out[:, cols] = normed.astype(BF16)


def tail_kernel(ways, attended, hidden, w_o, w_up, w_down, w_out, gain2, bias2, gainf, biasf,
                logits, norm_out, y_out,
                ring, last, resid, act, normed, normed_t, parts, raw1, raw2, sib, sibh, send3, recv3, own, gath, stats,
                w_sem, small_sem, send_sem, recv_sem, stat_send, stat_recv):
    me = lax.axis_index('tp')
    core = lax.rem(me, 2)
    chip = me // 2
    chips = ways // 2
    right = lax.rem(chip + 1, chips)
    left = lax.rem(chip + chips - 1, chips)
    far = lax.rem(chip + 2, chips)
    other = 1 - core
    rows, piece = resid.shape
    half = rows // 2
    top, bot = pl.ds(0, half), pl.ds(half, half)
    vocab, width = w_out.shape
    n_full = vocab // ROWS
    rest = vocab - n_full * ROWS
    s_o, s_up, s_down = RING - 5, RING - 4, RING - 2

    def dev(c, k):
        return {'tp': 2 * c + k}

    ld_res = pltpu.make_async_copy(hidden.at[:, pl.ds(pl.multiple_of(me * piece, piece), piece)], resid, small_sem.at[0])
    ld_o = pltpu.make_async_copy(w_o, ring.at[s_o, pl.ds(0, w_o.shape[0])], w_sem.at[s_o])
    ld_up = []
    for i in range(width // ROWS):
        ld_up.append(pltpu.make_async_copy(w_up.at[pl.ds(i * ROWS, ROWS)], ring.at[s_up + i // 3, :, pl.ds((i % 3) * w_up.shape[1], w_up.shape[1])], small_sem.at[4 + i]))
    ld_down = [pltpu.make_async_copy(w_down.at[pl.ds(i * ROWS, ROWS)], ring.at[s_down + i], small_sem.at[1 + i]) for i in range(2)]
    ld_last = pltpu.make_async_copy(w_out.at[pl.ds(n_full * ROWS, rest)], last, small_sem.at[3])

    def ld_tile(tile):
        slot = lax.rem(tile, RING)
        return pltpu.make_async_copy(w_out.at[pl.ds(pl.multiple_of(tile * ROWS, ROWS), ROWS)], ring.at[slot], w_sem.at[slot])

    ld_o.start()
    ld_res.start()
    for tile in range(4):
        ld_tile(tile).start()
    for c in ld_up:
        c.start()
    for c in ld_down:
        c.start()
    for tile in range(4, s_o):
        ld_tile(tile).start()
    ld_last.start()

    def flip(tile):
        ld_tile(tile).wait()

        def turn(b, carry):
            for part in range(2):
                cols = pl.ds(pl.multiple_of((2 * b + part) * BLOCK, BLOCK), BLOCK)
                for a in range(0, ROWS, BLOCK):
                    ring[tile, a:a + BLOCK, cols] = ring[tile, a:a + BLOCK, cols].T
            return carry

        lax.fori_loop(0, width // BLOCK // 2, turn, 0)

    barrier = pltpu.get_barrier_semaphore()
    for d in range(1, ways):
        pl.semaphore_signal(barrier, inc=1, device_id={'tp': lax.rem(me + d, ways)}, device_id_type=MESH)

    def copy(phase, idx, src, dst, to, ridx=None):
        ridx = idx if ridx is None else ridx
        return pltpu.make_async_remote_copy(src_ref=src, dst_ref=dst, send_sem=send_sem.at[phase, idx], recv_sem=recv_sem.at[phase, ridx],
                                            device_id=to, device_id_type=MESH)

    def arrive(phase, idx, dst):
        copy(phase, idx, dst, dst, dev(chip, core)).wait_recv()

    def all_sum(phase, product, residual, fill):
        pb = parts.at[phase]
        sent = []

        def go(c):
            c.start()
            sent.append(c)

        def term(c):
            value = product(c).astype(BF16)
            pb[2 * c] = value[:, :piece]
            pb[2 * c + 1] = value[:, piece:]

        g = gath.at[phase]
        term(far)
        if phase == 0:
            pl.semaphore_wait(barrier, ways - 1)
        for k in range(2):
            go(copy(phase, k, pb.at[2 * far + k, top], raw1.at[phase, 0, core], dev(right, k), core))
            go(copy(phase, 2 + k, pb.at[2 * far + k, bot], raw1.at[phase, 1, core], dev(left, k), 2 + core))
        term(right)
        for k in range(2):
            go(copy(phase, 6 + k, pb.at[2 * right + k, bot], raw2.at[phase, 1, core], dev(right, k), 6 + core))
        go(copy(phase, 9, pb.at[2 * right + other, top], sibh.at[phase, 0], dev(chip, other)))
        term(left)
        for k in range(2):
            go(copy(phase, 4 + k, pb.at[2 * left + k, top], raw2.at[phase, 0, core], dev(left, k), 4 + core))
        go(copy(phase, 10, pb.at[2 * left + other, bot], sibh.at[phase, 1], dev(chip, other)))
        term(chip)
        go(copy(phase, 8, pb.at[2 * chip + other], sib.at[phase], dev(chip, other)))
        for tile in fill[0]:
            flip(tile)
        for side, (to, rws) in enumerate(((right, top), (left, bot))):
            for k in range(2):
                arrive(phase, 2 * side + k, raw1.at[phase, side, k])
            arrive(phase, 9 + side, sibh.at[phase, side])
            send3[phase, side] = (raw1[phase, side, 0].astype(F32) + raw1[phase, side, 1].astype(F32)
                                  + pb[2 * to + core, rws].astype(F32) + sibh[phase, side].astype(F32))
            go(copy(phase, 11 + side, send3.at[phase, side], recv3.at[phase, side], dev(to, core)))
        for tile in fill[1]:
            flip(tile)
        arrive(phase, 8, sib.at[phase])
        for side, rws in enumerate((top, bot)):
            for k in range(2):
                arrive(phase, 4 + 2 * side + k, raw2.at[phase, side, k])
            base = (residual[rws].astype(F32) + pb[me, rws].astype(F32) + sib[phase, rws].astype(F32)
                    + raw2[phase, side, 0].astype(F32) + raw2[phase, side, 1].astype(F32))
            arrive(phase, 11 + side, recv3.at[phase, side])
            value = (base + recv3[phase, side]).astype(BF16)
            own[phase, rws] = value
            g[me, rws] = value
        ob = own.at[phase]
        go(copy(phase, 13, ob.at[top], g.at[me, top], dev(right, core)))
        go(copy(phase, 16, ob.at[bot], g.at[me, bot], dev(left, core)))
        go(copy(phase, 19, ob, g.at[me], dev(chip, other)))
        go(copy(phase, 14, ob.at[bot], g.at[me, bot], dev(right, core)))
        go(copy(phase, 15, ob.at[top], g.at[me, top], dev(left, core)))
        for tile in fill[2]:
            flip(tile)
        ml, mr, mf = 2 * left + core, 2 * right + core, 2 * far + core
        arrive(phase, 13, g.at[ml, top])
        go(copy(phase, 17, g.at[ml, top], g.at[ml, top], dev(right, core)))
        arrive(phase, 16, g.at[mr, bot])
        go(copy(phase, 18, g.at[mr, bot], g.at[mr, bot], dev(left, core)))
        go(copy(phase, 20, g.at[ml, top], g.at[ml, top], dev(chip, other)))
        go(copy(phase, 21, g.at[mr, bot], g.at[mr, bot], dev(chip, other)))
        for tile in fill[3]:
            flip(tile)
        arrive(phase, 14, g.at[ml, bot])
        go(copy(phase, 22, g.at[ml, bot], g.at[ml, bot], dev(chip, other)))
        arrive(phase, 15, g.at[mr, top])
        go(copy(phase, 23, g.at[mr, top], g.at[mr, top], dev(chip, other)))
        arrive(phase, 17, g.at[mf, top])
        go(copy(phase, 24, g.at[mf, top], g.at[mf, top], dev(chip, other)))
        arrive(phase, 18, g.at[mf, bot])
        go(copy(phase, 25, g.at[mf, bot], g.at[mf, bot], dev(chip, other)))
        ol, orr, of = 2 * left + other, 2 * right + other, 2 * far + other
        arrive(phase, 19, g.at[2 * chip + other])
        arrive(phase, 20, g.at[ol, top])
        arrive(phase, 21, g.at[orr, bot])
        arrive(phase, 22, g.at[ol, bot])
        arrive(phase, 23, g.at[orr, top])
        arrive(phase, 24, g.at[of, top])
        arrive(phase, 25, g.at[of, bot])
        return sent

    ld_o.wait()
    ld_res.wait()
    depth_o = w_o.shape[0]

    def product_o(c):
        return dotf(attended[...], ring[s_o, 0:depth_o, pl.ds(pl.multiple_of(2 * piece * c, 2 * piece), 2 * piece)])

    sent = all_sum(0, product_o, resid, ((0,), (1, 2), (3,), (4,)))
    ld_tile(s_o).start()
    norm_chunks(gath.at[0], gain2, bias2, normed)

    for c in ld_up:
        c.wait()
    ff = w_up.shape[1]
    for n in range(0, ff, 256):
        total = jnp.zeros((rows, 256), F32)
        for i in range(width // ROWS):
            total = total + dotf(normed[:, i * ROWS:(i + 1) * ROWS], ring[s_up + i // 3, :, (i % 3) * ff + n:(i % 3) * ff + n + 256])
        act[:, n:n + 256] = jnp.square(jnp.maximum(total, 0.0)).astype(BF16)
    ld_tile(s_up).start()
    ld_tile(s_up + 1).start()
    for c in ld_down:
        c.wait()

    def product_down(c):
        cols = pl.ds(pl.multiple_of(2 * piece * c, 2 * piece), 2 * piece)
        return dotf(act[:, :ROWS], ring[s_down, :, cols]) + dotf(act[:, ROWS:], ring[s_down + 1, :, cols])

    sent += all_sum(1, product_down, gath.at[0, me], ((5,), (6, 7, 8), (9, 10), (11,)))
    ld_tile(s_down).start()
    ld_tile(s_down + 1).start()
    norm_chunks(gath.at[1], gainf, biasf, normed)
    for j in range(ways):
        y_out[:, j * piece:(j + 1) * piece] = gath[1, j]
        normed_t[j * piece:(j + 1) * piece] = normed[:, j * piece:(j + 1) * piece].T

    def reduce_tile(z, carry):
        peak, total = carry
        z3 = z.reshape(z.shape[0] // 8, 8, z.shape[1])
        new_peak = jnp.maximum(peak, jnp.max(z3, axis=0))
        total = total * jnp.exp(peak - new_peak) + jnp.sum(jnp.exp(z3 - new_peak[None]), axis=0)
        return new_peak, total

    def rows_of(tile):
        return pl.ds(pl.multiple_of(tile * ROWS, ROWS), ROWS)

    def refill(tile):
        @pl.when(tile + RING < n_full)
        def _():
            ld_tile(tile + RING).start()

    def step_turned(pair, carry):
        for t in range(2):
            before = jnp.maximum(2 * pair - 2 + t, 0)
            carry = reduce_tile(logits[rows_of(before)], carry)
        for t in range(2):
            tile = 2 * pair + t
            for a in range(0, ROWS, BLOCK):
                z = jnp.zeros((rows, BLOCK), F32)
                for b in range(0, width, BLOCK):
                    z = z + dotf(normed[:, b:b + BLOCK], ring[tile, a:a + BLOCK, b:b + BLOCK])
                logits[pl.ds(pl.multiple_of(tile * ROWS + a, BLOCK), BLOCK)] = z.T
        for t in range(2):
            refill(2 * pair + t)
        return carry

    def step(tile, carry):
        slot = lax.rem(tile, RING)
        ld_tile(tile).wait()
        carry = reduce_tile(logits[rows_of(tile - 1)], carry)
        logits[rows_of(tile)] = dotf(ring[slot], normed_t[...])
        refill(tile)
        return carry

    logits[pl.ds(0, 2 * ROWS)] = jnp.full((2 * ROWS, rows), -1e30, F32)
    carry = (jnp.full((8, rows), -1e30, F32), jnp.zeros((8, rows), F32))
    carry = lax.fori_loop(0, FLIPS // 2, step_turned, carry)
    last_turned = FLIPS // 2 * 2
    carry = reduce_tile(logits[rows_of(last_turned - 2)], carry)
    carry = lax.fori_loop(last_turned, n_full, step, carry)
    ld_last.wait()
    carry = reduce_tile(logits[rows_of(n_full - 1)], carry)
    z = dotf(last[...], normed_t[...])
    logits[pl.ds(n_full * ROWS, rest)] = z
    peak8, total8 = reduce_tile(z, carry)
    peak = jnp.max(peak8, axis=0, keepdims=True)
    total = jnp.sum(total8 * jnp.exp(peak8 - peak), axis=0, keepdims=True)
    row = lax.broadcasted_iota(jnp.int32, (8, rows), 0)
    stats[me] = jnp.where(row == 0, peak, total)
    stat_out = []
    for d in range(1, ways):
        c = pltpu.make_async_remote_copy(src_ref=stats.at[me], dst_ref=stats.at[me], send_sem=stat_send.at[d], recv_sem=stat_recv.at[d],
                                         device_id={'tp': lax.rem(me + d, ways)}, device_id_type=MESH)
        c.start()
        stat_out.append(c)
    for d in range(1, ways):
        src = lax.rem(me + ways - d, ways)
        pltpu.make_async_remote_copy(src_ref=stats.at[src], dst_ref=stats.at[src], send_sem=stat_send.at[d], recv_sem=stat_recv.at[d],
                                     device_id={'tp': me}, device_id_type=MESH).wait_recv()
    all_stats = stats[...]
    peaks = all_stats[:, 0, :]
    totals = all_stats[:, 1, :]
    top_peak = jnp.max(peaks, axis=0, keepdims=True)
    whole = jnp.sum(totals * jnp.exp(peaks - top_peak), axis=0, keepdims=True)
    norm_out[...] = jnp.broadcast_to(top_peak + jnp.log(whole), norm_out.shape)
    for c in sent + stat_out:
        c.wait_send()


def run_tail(ways, attended, hidden, w_o, w_up, w_down, w_out_t, gain2, bias2, gainf, biasf):
    rows, width = hidden.shape
    piece = width // ways
    half = rows // 2
    vocab = w_out_t.shape[0]
    rest = vocab % ROWS
    ff = w_up.shape[1]
    any_ = pl.BlockSpec(memory_space=pl.ANY)
    vmem = pl.BlockSpec(memory_space=pltpu.VMEM)
    hbm = pl.BlockSpec(memory_space=pltpu.HBM)
    return pl.pallas_call(
        functools.partial(tail_kernel, ways),
        out_shape=(pltpu.VMEM((vocab, rows), F32), pltpu.VMEM((8, rows), F32), pltpu.VMEM((rows, width), BF16)),
        in_specs=[vmem, hbm, hbm, hbm, hbm, hbm, vmem, vmem, vmem, vmem],
        out_specs=(vmem, vmem, vmem),
        scratch_shapes=[
            pltpu.VMEM((RING, ROWS, width), BF16),
            pltpu.VMEM((rest, width), BF16),
            pltpu.VMEM((rows, piece), BF16),
            pltpu.VMEM((rows, ff), BF16),
            pltpu.VMEM((rows, width), BF16),
            pltpu.VMEM((width, rows), BF16),
            pltpu.VMEM((2, ways, rows, piece), BF16),
            pltpu.VMEM((2, 2, 2, half, piece), BF16),
            pltpu.VMEM((2, 2, 2, half, piece), BF16),
            pltpu.VMEM((2, rows, piece), BF16),
            pltpu.VMEM((2, 2, half, piece), BF16),
            pltpu.VMEM((2, 2, half, piece), F32),
            pltpu.VMEM((2, 2, half, piece), F32),
            pltpu.VMEM((2, rows, piece), BF16),
            pltpu.VMEM((2, ways, rows, piece), BF16),
            pltpu.VMEM((ways, 8, rows), F32),
            pltpu.SemaphoreType.DMA((RING,)),
            pltpu.SemaphoreType.DMA((10,)),
            pltpu.SemaphoreType.DMA((2, NSEM)),
            pltpu.SemaphoreType.DMA((2, NSEM)),
            pltpu.SemaphoreType.DMA((ways,)),
            pltpu.SemaphoreType.DMA((ways,)),
        ],
        compiler_params=pltpu.CompilerParams(collective_id=0, has_side_effects=True, vmem_limit_bytes=LIMIT),
        name='tail',
    )(pltpu.with_memory_space_constraint(attended, pltpu.VMEM), hidden, w_o, w_up, w_down, w_out_t, gain2, bias2, gainf, biasf)


LIMIT = 53 * 1024 * 1024


CHUNKS = 4
PROJ = 2


def attend_kernel(hidden, lengths, gain, bias, w_q, w_k, w_v, cache_k, cache_v,
                  attended, out_k, out_v,
                  x, gb, len_row, normed, w_qkv, qkv, len_col, k_buf, v_buf, misc_sem, w_sem, in_sem, out_sem):
    rows, width = hidden.shape
    seqs, slots, dim = cache_k.shape
    q_cols = w_q.shape[1]
    heads = q_cols // dim
    step_w = width // PROJ
    step_s = seqs // CHUNKS

    small = [pltpu.make_async_copy(hidden, x, misc_sem.at[0]),
             pltpu.make_async_copy(gain, gb.at[pl.ds(0, 1)], misc_sem.at[1]),
             pltpu.make_async_copy(bias, gb.at[pl.ds(1, 1)], misc_sem.at[2]),
             pltpu.make_async_copy(lengths, len_row, misc_sem.at[3])]
    for c in small:
        c.start()
    w_in = []
    for i in range(PROJ):
        part = pl.ds(i * step_w, step_w)
        w_in.append([pltpu.make_async_copy(w_q.at[part], w_qkv.at[part, pl.ds(0, q_cols)], w_sem.at[0, i]),
                     pltpu.make_async_copy(w_k.at[part], w_qkv.at[part, pl.ds(q_cols, dim)], w_sem.at[1, i]),
                     pltpu.make_async_copy(w_v.at[part], w_qkv.at[part, pl.ds(q_cols + dim, dim)], w_sem.at[2, i])])
        for c in w_in[-1]:
            c.start()
    kv_in, kv_out = [], []
    for i in range(CHUNKS):
        part = pl.ds(i * step_s, step_s)
        kv_in.append([pltpu.make_async_copy(cache_k.at[part], k_buf.at[part], in_sem.at[0, i]),
                      pltpu.make_async_copy(cache_v.at[part], v_buf.at[part], in_sem.at[1, i])])
        kv_out.append([pltpu.make_async_copy(k_buf.at[part], out_k.at[part], out_sem.at[0, i]),
                       pltpu.make_async_copy(v_buf.at[part], out_v.at[part], out_sem.at[1, i])])
        for c in kv_in[-1]:
            c.start()

    small[3].wait()
    lens = jnp.broadcast_to(len_row[...].astype(F32), (rows, rows)).T
    len_col[...] = lens
    lane = lax.broadcasted_iota(jnp.int32, (1, dim), 1)
    half_rot = dim // 4
    freq_lane = jnp.where(lane < half_rot, lane, lane - half_rot).astype(F32)
    inv_freq = jnp.where(lane < 2 * half_rot, jnp.exp(freq_lane * (-2.0 / (2 * half_rot) * math.log(ROPE_BASE))), 0.0)
    angle = lens * inv_freq
    cosine = jnp.cos(angle)
    sine = jnp.where(lane < half_rot, -1.0, 1.0) * jnp.sin(angle)
    for c in small[:3]:
        c.wait()
    total = jnp.zeros((rows, 128), F32)
    piece = width // 8
    for j in range(8):
        total = total + fold(x[:, j * piece:(j + 1) * piece].astype(F32))
    mean = jnp.sum(total, axis=-1, keepdims=True) / width
    total = jnp.zeros((rows, 128), F32)
    for j in range(8):
        total = total + fold(jnp.square(x[:, j * piece:(j + 1) * piece].astype(F32) - mean))
    scale = lax.rsqrt(jnp.sum(total, axis=-1, keepdims=True) / width + EPSILON)
    for j in range(8):
        cols = slice(j * piece, (j + 1) * piece)
        normed[:, cols] = ((x[:, cols].astype(F32) - mean) * scale * (1.0 + gb[0:1, cols]) + gb[1:2, cols]).astype(BF16)

    for i in range(PROJ):
        for c in w_in[i]:
            c.wait()
        part = slice(i * step_w, (i + 1) * step_w)
        product = dotf(normed[:, part], w_qkv[part])
        if i == 0:
            qkv[...] = product
        else:
            qkv[...] += product
    for h in range(heads + 1):
        cols = slice(h * dim, (h + 1) * dim)
        vec = qkv[:, cols]
        partner = jnp.where(lane < half_rot, pltpu.roll(vec, dim - half_rot, 1), pltpu.roll(vec, half_rot, 1))
        qkv[:, cols] = vec * cosine + partner * sine

    row_id = lax.broadcasted_iota(jnp.int32, (slots, dim), 0).astype(F32)
    group = 8
    span = group * slots
    offset = (lax.broadcasted_iota(jnp.int32, (group, span), 1) - slots * lax.broadcasted_iota(jnp.int32, (group, span), 0)).astype(F32)
    k_cols, v_cols = slice(q_cols, q_cols + dim), slice(q_cols + dim, q_cols + 2 * dim)
    for i in range(CHUNKS):
        for c in kv_in[i]:
            c.wait()

        def put(s, carry):
            base = pl.multiple_of(i * step_s + s * 8, 8)
            lens8 = len_col[pl.ds(base, 8), :]
            new_k = qkv[pl.ds(base, 8), k_cols]
            new_v = qkv[pl.ds(base, 8), v_cols]
            for t in range(8):
                here = row_id == lens8[t:t + 1]
                k_buf[base + t] = jnp.where(here, new_k[t:t + 1], k_buf[base + t].astype(F32)).astype(BF16)
                v_buf[base + t] = jnp.where(here, new_v[t:t + 1], v_buf[base + t].astype(F32)).astype(BF16)
            return carry

        lax.fori_loop(0, step_s // 8, put, 0)
        for c in kv_out[i]:
            c.start()
        groups = [i * step_s + g * group for g in range(step_s // group)]
        all_scores = []
        for b in groups:
            q = jnp.concatenate([qkv[b:b + group, h * dim:(h + 1) * dim] for h in range(heads)], axis=0).astype(BF16)
            keys = k_buf[b:b + group].reshape(span, dim)
            all_scores.append(lax.dot_general(q, keys, (((1,), (1,)), ((), ())), preferred_element_type=F32))
        probs = []
        for b, scores in zip(groups, all_scores):
            valid = (offset >= 0.0) & (offset <= len_col[b:b + group, 0:1])
            scores = jnp.where(valid[None], scores.reshape(heads, group, span) * (dim ** -0.5), -1e30)
            peak = jnp.max(scores, axis=-1, keepdims=True)
            weight = jnp.where(valid[None], jnp.exp(scores - peak), 0.0)
            prob = (weight / jnp.sum(weight, axis=-1, keepdims=True)).astype(BF16)
            probs.append(prob.reshape(heads * group, span))
        for b, prob in zip(groups, probs):
            mixed = dotf(prob, v_buf[b:b + group].reshape(span, dim)).astype(BF16)
            for h in range(heads):
                attended[b:b + group, h * dim:(h + 1) * dim] = mixed[h * group:(h + 1) * group]
    for pair in kv_out:
        for c in pair:
            c.wait()


def run_attend(hidden, cache_k, cache_v, lengths, gain, bias, w_q, w_k, w_v):
    rows, width = hidden.shape
    seqs, slots, dim = cache_k.shape
    q_cols = w_q.shape[1]
    hbm = pl.BlockSpec(memory_space=pltpu.HBM)
    vmem = pl.BlockSpec(memory_space=pltpu.VMEM)
    return pl.pallas_call(
        attend_kernel,
        out_shape=(pltpu.VMEM((rows, q_cols), BF16), jax.ShapeDtypeStruct(cache_k.shape, BF16), jax.ShapeDtypeStruct(cache_v.shape, BF16)),
        in_specs=[hbm] * 9,
        out_specs=(vmem, hbm, hbm),
        scratch_shapes=[
            pltpu.VMEM((rows, width), BF16),
            pltpu.VMEM((8, width), F32),
            pltpu.VMEM((1, rows), jnp.int32),
            pltpu.VMEM((rows, width), BF16),
            pltpu.VMEM((width, q_cols + 2 * dim), BF16),
            pltpu.VMEM((rows, q_cols + 2 * dim), F32),
            pltpu.VMEM((rows, rows), F32),
            pltpu.VMEM((seqs, slots, dim), BF16),
            pltpu.VMEM((seqs, slots, dim), BF16),
            pltpu.SemaphoreType.DMA((4,)),
            pltpu.SemaphoreType.DMA((3, PROJ)),
            pltpu.SemaphoreType.DMA((2, CHUNKS)),
            pltpu.SemaphoreType.DMA((2, CHUNKS)),
        ],
        compiler_params=pltpu.CompilerParams(vmem_limit_bytes=62 * 1024 * 1024),
        name='attend',
    )(hidden, lengths, gain, bias, w_q, w_k, w_v, cache_k, cache_v)


PARTS = 8


def finish_kernel(logits, norm, y, out, y_out, buf, sem, y_sem):
    copy = pltpu.make_async_copy(y, y_out, y_sem)
    copy.start()
    block = logits.shape[0] // PARTS // 8 * 8
    outs = []
    for i in range(PARTS):
        size = block if i < PARTS - 1 else logits.shape[0] - block * (PARTS - 1)
        part = pl.ds(i * block, size)
        buf[part] = logits[part] - norm[0:1]
        outs.append(pltpu.make_async_copy(buf.at[part], out.at[part], sem.at[i]))
        outs[-1].start()
    for c in outs:
        c.wait()
    copy.wait()


def run_finish(logits, norm, y):
    vocab, rows = logits.shape
    vmem = pl.BlockSpec(memory_space=pltpu.VMEM)
    hbm = pl.BlockSpec(memory_space=pltpu.HBM)
    return pl.pallas_call(
        finish_kernel,
        out_shape=(jax.ShapeDtypeStruct((vocab, rows), F32), jax.ShapeDtypeStruct(y.shape, BF16)),
        in_specs=[vmem, vmem, vmem],
        out_specs=(hbm, hbm),
        scratch_shapes=[pltpu.VMEM((vocab, rows), F32), pltpu.SemaphoreType.DMA((PARTS,)), pltpu.SemaphoreType.DMA],
        compiler_params=pltpu.CompilerParams(vmem_limit_bytes=16 * 1024 * 1024),
        name='finish',
    )(logits, norm, y)


def solution(mesh):
    ways = mesh.shape['tp']
    row_spec = P('bs', None)
    cache_spec = P('bs', None, 'tp', None)
    col_split = P(None, 'tp')
    row_split = P('tp', None)
    in_specs = (row_spec, cache_spec, cache_spec, P('bs'), P(), P(), col_split, col_split, col_split, row_split, P(), P(), col_split, row_split, P(), P(), col_split)
    out_specs = (P('bs', 'tp'), cache_spec, cache_spec, row_spec)

    def local_step(new_hidden, cache_k, cache_v, lengths, ln1_gain, ln1_bias, w_q, w_k, w_v, w_o, ln2_gain, ln2_bias, w_up, w_down, lnf_gain, lnf_bias, w_out):
        shape = cache_k.shape
        flat = (shape[0], shape[1], shape[3])
        attended, new_cache_k, new_cache_v = run_attend(new_hidden, cache_k.reshape(flat), cache_v.reshape(flat), lengths[None], ln1_gain[None], ln1_bias[None], w_q, w_k, w_v)
        logits, norm, y = run_tail(ways, attended, new_hidden, w_o, w_up, w_down, w_out.T,
                                   ln2_gain[None], ln2_bias[None], lnf_gain[None], lnf_bias[None])
        log_probs_t, out_hidden = run_finish(logits, norm, y)
        return log_probs_t.T, new_cache_k.reshape(shape), new_cache_v.reshape(shape), out_hidden

    return jax.shard_map(local_step, mesh=mesh, in_specs=in_specs, out_specs=out_specs, check_vma=False)
```

```python
import functools
import math

import jax
import jax.numpy as jnp
from jax import lax
from jax.experimental import pallas as pl
from jax.experimental.pallas import tpu as pltpu
from jax.sharding import PartitionSpec as P

EPSILON = 1e-5
ROPE_BASE = 10000.0
BF16 = jnp.bfloat16
F32 = jnp.float32
MESH = pl.DeviceIdType.MESH
RING = 13
FLIPS = 12
BLOCK = 256
ROWS = 512
NSEM = 26


def dotf(lhs, rhs):
    return jnp.dot(lhs, rhs, preferred_element_type=F32)


def fold(values):
    out = values[:, 0:128]
    for lane in range(128, values.shape[1], 128):
        out = out + values[:, lane:lane + 128]
    return out


def norm_chunks(chunks, gain, bias, out):
    count, rows, piece = chunks.shape
    width = count * piece
    total = jnp.zeros((rows, 128), F32)
    for j in range(count):
        total = total + fold(chunks[j].astype(F32))
    mean = jnp.sum(total, axis=-1, keepdims=True) / width
    total = jnp.zeros((rows, 128), F32)
    for j in range(count):
        total = total + fold(jnp.square(chunks[j].astype(F32) - mean))
    scale = lax.rsqrt(jnp.sum(total, axis=-1, keepdims=True) / width + EPSILON)
    for j in range(count):
        cols = slice(j * piece, (j + 1) * piece)
        normed = (chunks[j].astype(F32) - mean) * scale * (1.0 + gain[:, cols]) + bias[:, cols]
        out[:, cols] = normed.astype(BF16)


def tail_kernel(ways, attended, hidden, w_o, w_up, w_down, w_out, gain2, bias2, gainf, biasf,
                logits, norm_out, y_out,
                ring, turned, last, resid, act, normed, normed_t, parts, raw1, raw2, sib, sibh, send3, recv3, own, gath, stats,
                w_sem, small_sem, send_sem, recv_sem, stat_send, stat_recv):
    me = lax.axis_index('tp')
    core = lax.rem(me, 2)
    chip = me // 2
    chips = ways // 2
    right = lax.rem(chip + 1, chips)
    left = lax.rem(chip + chips - 1, chips)
    far = lax.rem(chip + 2, chips)
    other = 1 - core
    rows, piece = resid.shape
    half = rows // 2
    top, bot = pl.ds(0, half), pl.ds(half, half)
    vocab, width = w_out.shape
    n_full = vocab // ROWS
    rest = vocab - n_full * ROWS
    s_o, s_up, s_down = RING - 5, RING - 4, RING - 2

    def dev(c, k):
        return {'tp': 2 * c + k}

    ld_res = pltpu.make_async_copy(hidden.at[:, pl.ds(pl.multiple_of(me * piece, piece), piece)], resid, small_sem.at[0])
    ld_o = pltpu.make_async_copy(w_o, ring.at[s_o, pl.ds(0, w_o.shape[0])], w_sem.at[s_o])
    ld_up = []
    for i in range(width // ROWS):
        ld_up.append(pltpu.make_async_copy(w_up.at[pl.ds(i * ROWS, ROWS)], ring.at[s_up + i // 3, :, pl.ds((i % 3) * w_up.shape[1], w_up.shape[1])], small_sem.at[4 + i]))
    ld_down = [pltpu.make_async_copy(w_down.at[pl.ds(i * ROWS, ROWS)], ring.at[s_down + i], small_sem.at[1 + i]) for i in range(2)]
    ld_last = pltpu.make_async_copy(w_out.at[pl.ds(n_full * ROWS, rest)], last, small_sem.at[3])

    def ld_tile(tile):
        slot = lax.rem(tile, RING)
        return pltpu.make_async_copy(w_out.at[pl.ds(pl.multiple_of(tile * ROWS, ROWS), ROWS)], ring.at[slot], w_sem.at[slot])

    ld_o.start()
    ld_res.start()
    for tile in range(4):
        ld_tile(tile).start()
    for c in ld_up:
        c.start()
    for c in ld_down:
        c.start()
    for tile in range(4, s_o):
        ld_tile(tile).start()
    ld_last.start()

    def flip(tile):
        ld_tile(tile).wait()
        target = ring.at[tile] if tile < FLIPS else turned

        def turn(b, carry):
            for part in range(2):
                cols = pl.ds(pl.multiple_of((2 * b + part) * BLOCK, BLOCK), BLOCK)
                for a in range(0, ROWS, BLOCK):
                    target[a:a + BLOCK, cols] = ring[tile, a:a + BLOCK, cols].T
            return carry

        lax.fori_loop(0, width // BLOCK // 2, turn, 0)
        if tile == FLIPS:
            ld_tile(tile + RING).start()

    barrier = pltpu.get_barrier_semaphore()
    for d in range(1, ways):
        pl.semaphore_signal(barrier, inc=1, device_id={'tp': lax.rem(me + d, ways)}, device_id_type=MESH)

    def copy(phase, idx, src, dst, to, ridx=None):
        ridx = idx if ridx is None else ridx
        return pltpu.make_async_remote_copy(src_ref=src, dst_ref=dst, send_sem=send_sem.at[phase, idx], recv_sem=recv_sem.at[phase, ridx],
                                            device_id=to, device_id_type=MESH)

    def arrive(phase, idx, dst):
        copy(phase, idx, dst, dst, dev(chip, core)).wait_recv()

    def all_sum(phase, product, residual, fill, freed):
        pb = parts.at[phase]
        sent = []

        def go(c):
            c.start()
            sent.append(c)

        def term(c):
            value = product(c).astype(BF16)
            pb[2 * c] = value[:, :piece]
            pb[2 * c + 1] = value[:, piece:]

        g = gath.at[phase]
        term(far)
        if phase == 0:
            pl.semaphore_wait(barrier, ways - 1)
        for k in range(2):
            go(copy(phase, k, pb.at[2 * far + k, top], raw1.at[phase, 0, core], dev(right, k), core))
            go(copy(phase, 2 + k, pb.at[2 * far + k, bot], raw1.at[phase, 1, core], dev(left, k), 2 + core))
        term(right)
        for k in range(2):
            go(copy(phase, 6 + k, pb.at[2 * right + k, bot], raw2.at[phase, 1, core], dev(right, k), 6 + core))
        go(copy(phase, 9, pb.at[2 * right + other, top], sibh.at[phase, 0], dev(chip, other)))
        term(left)
        for k in range(2):
            go(copy(phase, 4 + k, pb.at[2 * left + k, top], raw2.at[phase, 0, core], dev(left, k), 4 + core))
        go(copy(phase, 10, pb.at[2 * left + other, bot], sibh.at[phase, 1], dev(chip, other)))
        term(chip)
        go(copy(phase, 8, pb.at[2 * chip + other], sib.at[phase], dev(chip, other)))
        for tile in freed:
            ld_tile(tile).start()
        for tile in fill[0]:
            flip(tile)
        for side, (to, rws) in enumerate(((right, top), (left, bot))):
            for k in range(2):
                arrive(phase, 2 * side + k, raw1.at[phase, side, k])
            arrive(phase, 9 + side, sibh.at[phase, side])
            send3[phase, side] = (raw1[phase, side, 0].astype(F32) + raw1[phase, side, 1].astype(F32)
                                  + pb[2 * to + core, rws].astype(F32) + sibh[phase, side].astype(F32))
            go(copy(phase, 11 + side, send3.at[phase, side], recv3.at[phase, side], dev(to, core)))
        for tile in fill[1]:
            flip(tile)
        arrive(phase, 8, sib.at[phase])
        for side, rws in enumerate((top, bot)):
            for k in range(2):
                arrive(phase, 4 + 2 * side + k, raw2.at[phase, side, k])
            base = (residual[rws].astype(F32) + pb[me, rws].astype(F32) + sib[phase, rws].astype(F32)
                    + raw2[phase, side, 0].astype(F32) + raw2[phase, side, 1].astype(F32))
            arrive(phase, 11 + side, recv3.at[phase, side])
            value = (base + recv3[phase, side]).astype(BF16)
            own[phase, rws] = value
            g[me, rws] = value
        ob = own.at[phase]
        go(copy(phase, 13, ob.at[top], g.at[me, top], dev(right, core)))
        go(copy(phase, 16, ob.at[bot], g.at[me, bot], dev(left, core)))
        go(copy(phase, 19, ob, g.at[me], dev(chip, other)))
        go(copy(phase, 14, ob.at[bot], g.at[me, bot], dev(right, core)))
        go(copy(phase, 15, ob.at[top], g.at[me, top], dev(left, core)))
        for tile in fill[2]:
            flip(tile)
        ml, mr, mf = 2 * left + core, 2 * right + core, 2 * far + core
        arrive(phase, 13, g.at[ml, top])
        go(copy(phase, 17, g.at[ml, top], g.at[ml, top], dev(right, core)))
        arrive(phase, 16, g.at[mr, bot])
        go(copy(phase, 18, g.at[mr, bot], g.at[mr, bot], dev(left, core)))
        go(copy(phase, 20, g.at[ml, top], g.at[ml, top], dev(chip, other)))
        go(copy(phase, 21, g.at[mr, bot], g.at[mr, bot], dev(chip, other)))
        for tile in fill[3]:
            flip(tile)
        arrive(phase, 14, g.at[ml, bot])
        go(copy(phase, 22, g.at[ml, bot], g.at[ml, bot], dev(chip, other)))
        arrive(phase, 15, g.at[mr, top])
        go(copy(phase, 23, g.at[mr, top], g.at[mr, top], dev(chip, other)))
        arrive(phase, 17, g.at[mf, top])
        go(copy(phase, 24, g.at[mf, top], g.at[mf, top], dev(chip, other)))
        arrive(phase, 18, g.at[mf, bot])
        go(copy(phase, 25, g.at[mf, bot], g.at[mf, bot], dev(chip, other)))
        ol, orr, of = 2 * left + other, 2 * right + other, 2 * far + other
        arrive(phase, 19, g.at[2 * chip + other])
        arrive(phase, 20, g.at[ol, top])
        arrive(phase, 21, g.at[orr, bot])
        arrive(phase, 22, g.at[ol, bot])
        arrive(phase, 23, g.at[orr, top])
        arrive(phase, 24, g.at[of, top])
        arrive(phase, 25, g.at[of, bot])
        return sent

    ld_o.wait()
    ld_res.wait()
    depth_o = w_o.shape[0]

    def product_o(c):
        return dotf(attended[...], ring[s_o, 0:depth_o, pl.ds(pl.multiple_of(2 * piece * c, 2 * piece), 2 * piece)])

    sent = all_sum(0, product_o, resid, ((0,), (1, 2), (3,), (4,)), (s_o,))
    norm_chunks(gath.at[0], gain2, bias2, normed)

    for c in ld_up:
        c.wait()
    ff = w_up.shape[1]
    for n in range(0, ff, 256):
        total = jnp.zeros((rows, 256), F32)
        for i in range(width // ROWS):
            total = total + dotf(normed[:, i * ROWS:(i + 1) * ROWS], ring[s_up + i // 3, :, (i % 3) * ff + n:(i % 3) * ff + n + 256])
        act[:, n:n + 256] = jnp.square(jnp.maximum(total, 0.0)).astype(BF16)
    ld_tile(s_up).start()
    ld_tile(s_up + 1).start()
    for c in ld_down:
        c.wait()

    def product_down(c):
        cols = pl.ds(pl.multiple_of(2 * piece * c, 2 * piece), 2 * piece)
        return dotf(act[:, :ROWS], ring[s_down, :, cols]) + dotf(act[:, ROWS:], ring[s_down + 1, :, cols])

    sent += all_sum(1, product_down, gath.at[0, me], ((5,), (6, 7, 8), (9, 10), (11, 12)), (s_down, s_down + 1))
    norm_chunks(gath.at[1], gainf, biasf, normed)
    for j in range(ways):
        y_out[:, j * piece:(j + 1) * piece] = gath[1, j]
        normed_t[j * piece:(j + 1) * piece] = normed[:, j * piece:(j + 1) * piece].T

    def reduce_tile(z, carry):
        peak, total = carry
        z3 = z.reshape(z.shape[0] // 8, 8, z.shape[1])
        new_peak = jnp.maximum(peak, jnp.max(z3, axis=0))
        total = total * jnp.exp(peak - new_peak) + jnp.sum(jnp.exp(z3 - new_peak[None]), axis=0)
        return new_peak, total

    def rows_of(tile):
        return pl.ds(pl.multiple_of(tile * ROWS, ROWS), ROWS)

    def refill(tile):
        @pl.when(tile + RING < n_full)
        def _():
            ld_tile(tile + RING).start()

    def step_turned(pair, carry):
        for t in range(2):
            before = jnp.maximum(2 * pair - 2 + t, 0)
            carry = reduce_tile(logits[rows_of(before)], carry)
        for t in range(2):
            tile = 2 * pair + t
            for a in range(0, ROWS, BLOCK):
                z = jnp.zeros((rows, BLOCK), F32)
                for b in range(0, width, BLOCK):
                    z = z + dotf(normed[:, b:b + BLOCK], ring[tile, a:a + BLOCK, b:b + BLOCK])
                logits[pl.ds(pl.multiple_of(tile * ROWS + a, BLOCK), BLOCK)] = z.T
        for t in range(2):
            refill(2 * pair + t)
        return carry

    def turned_product(tile):
        for a in range(0, ROWS, BLOCK):
            z = jnp.zeros((rows, BLOCK), F32)
            for b in range(0, width, BLOCK):
                z = z + dotf(normed[:, b:b + BLOCK], turned[a:a + BLOCK, b:b + BLOCK])
            logits[pl.ds(pl.multiple_of(tile * ROWS + a, BLOCK), BLOCK)] = z.T

    def step_pair(pair, carry):
        tile = FLIPS + 2 * pair
        plain, coming = lax.rem(tile + 1, RING), lax.rem(tile + 2, RING)
        ld_tile(tile + 1).wait()
        ld_tile(tile + 2).wait()
        for t in range(2):
            carry = reduce_tile(logits[rows_of(tile - 2 + t)], carry)
        turned_product(tile)
        for a in range(0, ROWS, BLOCK):
            logits[pl.ds(pl.multiple_of((tile + 1) * ROWS + a, BLOCK), BLOCK)] = dotf(ring[plain, a:a + BLOCK], normed_t[...])
            for b in range(width // ROWS * a, width // ROWS * (a + BLOCK), BLOCK):
                for r in range(0, ROWS, BLOCK):
                    turned[r:r + BLOCK, b:b + BLOCK] = ring[coming, r:r + BLOCK, b:b + BLOCK].T
        refill(tile + 1)
        refill(tile + 2)
        return carry

    logits[pl.ds(0, 2 * ROWS)] = jnp.full((2 * ROWS, rows), -1e30, F32)
    carry = (jnp.full((8, rows), -1e30, F32), jnp.zeros((8, rows), F32))
    carry = lax.fori_loop(0, FLIPS // 2, step_turned, carry)
    carry = lax.fori_loop(0, (n_full - FLIPS - 1) // 2, step_pair, carry)
    for t in range(n_full - 3, n_full - 1):
        carry = reduce_tile(logits[rows_of(t)], carry)
    ld_last.wait()
    turned_product(n_full - 1)
    logits[pl.ds(n_full * ROWS, rest)] = dotf(last[...], normed_t[...])
    peak8, total8 = reduce_tile(logits[pl.ds((n_full - 1) * ROWS, ROWS + rest)], carry)
    peak = jnp.max(peak8, axis=0, keepdims=True)
    total = jnp.sum(total8 * jnp.exp(peak8 - peak), axis=0, keepdims=True)
    row = lax.broadcasted_iota(jnp.int32, (8, rows), 0)
    stats[me] = jnp.where(row == 0, peak, total)
    stat_out = []
    for d in range(1, ways):
        c = pltpu.make_async_remote_copy(src_ref=stats.at[me], dst_ref=stats.at[me], send_sem=stat_send.at[d], recv_sem=stat_recv.at[d],
                                         device_id={'tp': lax.rem(me + d, ways)}, device_id_type=MESH)
        c.start()
        stat_out.append(c)
    for d in range(1, ways):
        src = lax.rem(me + ways - d, ways)
        pltpu.make_async_remote_copy(src_ref=stats.at[src], dst_ref=stats.at[src], send_sem=stat_send.at[d], recv_sem=stat_recv.at[d],
                                     device_id={'tp': me}, device_id_type=MESH).wait_recv()
    all_stats = stats[...]
    peaks = all_stats[:, 0, :]
    totals = all_stats[:, 1, :]
    top_peak = jnp.max(peaks, axis=0, keepdims=True)
    whole = jnp.sum(totals * jnp.exp(peaks - top_peak), axis=0, keepdims=True)
    norm_out[...] = jnp.broadcast_to(top_peak + jnp.log(whole), norm_out.shape)
    for c in sent + stat_out:
        c.wait_send()


def run_tail(ways, attended, hidden, w_o, w_up, w_down, w_out_t, gain2, bias2, gainf, biasf):
    rows, width = hidden.shape
    piece = width // ways
    half = rows // 2
    vocab = w_out_t.shape[0]
    rest = vocab % ROWS
    ff = w_up.shape[1]
    any_ = pl.BlockSpec(memory_space=pl.ANY)
    vmem = pl.BlockSpec(memory_space=pltpu.VMEM)
    hbm = pl.BlockSpec(memory_space=pltpu.HBM)
    return pl.pallas_call(
        functools.partial(tail_kernel, ways),
        out_shape=(pltpu.VMEM((vocab, rows), F32), pltpu.VMEM((8, rows), F32), pltpu.VMEM((rows, width), BF16)),
        in_specs=[vmem, hbm, hbm, hbm, hbm, hbm, vmem, vmem, vmem, vmem],
        out_specs=(vmem, vmem, vmem),
        scratch_shapes=[
            pltpu.VMEM((RING, ROWS, width), BF16),
            pltpu.VMEM((ROWS, width), BF16),
            pltpu.VMEM((rest, width), BF16),
            pltpu.VMEM((rows, piece), BF16),
            pltpu.VMEM((rows, ff), BF16),
            pltpu.VMEM((rows, width), BF16),
            pltpu.VMEM((width, rows), BF16),
            pltpu.VMEM((2, ways, rows, piece), BF16),
            pltpu.VMEM((2, 2, 2, half, piece), BF16),
            pltpu.VMEM((2, 2, 2, half, piece), BF16),
            pltpu.VMEM((2, rows, piece), BF16),
            pltpu.VMEM((2, 2, half, piece), BF16),
            pltpu.VMEM((2, 2, half, piece), F32),
            pltpu.VMEM((2, 2, half, piece), F32),
            pltpu.VMEM((2, rows, piece), BF16),
            pltpu.VMEM((2, ways, rows, piece), BF16),
            pltpu.VMEM((ways, 8, rows), F32),
            pltpu.SemaphoreType.DMA((RING,)),
            pltpu.SemaphoreType.DMA((10,)),
            pltpu.SemaphoreType.DMA((2, NSEM)),
            pltpu.SemaphoreType.DMA((2, NSEM)),
            pltpu.SemaphoreType.DMA((ways,)),
            pltpu.SemaphoreType.DMA((ways,)),
        ],
        compiler_params=pltpu.CompilerParams(collective_id=0, has_side_effects=True, vmem_limit_bytes=LIMIT),
        name='tail',
    )(pltpu.with_memory_space_constraint(attended, pltpu.VMEM), hidden, w_o, w_up, w_down, w_out_t, gain2, bias2, gainf, biasf)


LIMIT = 53 * 1024 * 1024


CHUNKS = 4
PROJ = 2


def attend_kernel(hidden, lengths, gain, bias, w_q, w_k, w_v, cache_k, cache_v,
                  attended, out_k, out_v,
                  x, gb, len_row, normed, w_qkv, qkv, len_col, k_buf, v_buf, misc_sem, w_sem, in_sem, out_sem):
    rows, width = hidden.shape
    seqs, slots, dim = cache_k.shape
    q_cols = w_q.shape[1]
    heads = q_cols // dim
    step_w = width // PROJ
    step_s = seqs // CHUNKS

    small = [pltpu.make_async_copy(hidden, x, misc_sem.at[0]),
             pltpu.make_async_copy(gain, gb.at[pl.ds(0, 1)], misc_sem.at[1]),
             pltpu.make_async_copy(bias, gb.at[pl.ds(1, 1)], misc_sem.at[2]),
             pltpu.make_async_copy(lengths, len_row, misc_sem.at[3])]
    for c in small:
        c.start()
    w_in = []
    for i in range(PROJ):
        part = pl.ds(i * step_w, step_w)
        w_in.append([pltpu.make_async_copy(w_q.at[part], w_qkv.at[part, pl.ds(0, q_cols)], w_sem.at[0, i]),
                     pltpu.make_async_copy(w_k.at[part], w_qkv.at[part, pl.ds(q_cols, dim)], w_sem.at[1, i]),
                     pltpu.make_async_copy(w_v.at[part], w_qkv.at[part, pl.ds(q_cols + dim, dim)], w_sem.at[2, i])])
        for c in w_in[-1]:
            c.start()
    kv_in, kv_out = [], []
    for i in range(CHUNKS):
        part = pl.ds(i * step_s, step_s)
        kv_in.append([pltpu.make_async_copy(cache_k.at[part], k_buf.at[part], in_sem.at[0, i]),
                      pltpu.make_async_copy(cache_v.at[part], v_buf.at[part], in_sem.at[1, i])])
        kv_out.append([pltpu.make_async_copy(k_buf.at[part], out_k.at[part], out_sem.at[0, i]),
                       pltpu.make_async_copy(v_buf.at[part], out_v.at[part], out_sem.at[1, i])])
        for c in kv_in[-1]:
            c.start()

    small[3].wait()
    lens = jnp.broadcast_to(len_row[...].astype(F32), (rows, rows)).T
    len_col[...] = lens
    lane = lax.broadcasted_iota(jnp.int32, (1, dim), 1)
    half_rot = dim // 4
    freq_lane = jnp.where(lane < half_rot, lane, lane - half_rot).astype(F32)
    inv_freq = jnp.where(lane < 2 * half_rot, jnp.exp(freq_lane * (-2.0 / (2 * half_rot) * math.log(ROPE_BASE))), 0.0)
    angle = lens * inv_freq
    cosine = jnp.cos(angle)
    sine = jnp.where(lane < half_rot, -1.0, 1.0) * jnp.sin(angle)
    for c in small[:3]:
        c.wait()
    total = jnp.zeros((rows, 128), F32)
    piece = width // 8
    for j in range(8):
        total = total + fold(x[:, j * piece:(j + 1) * piece].astype(F32))
    mean = jnp.sum(total, axis=-1, keepdims=True) / width
    total = jnp.zeros((rows, 128), F32)
    for j in range(8):
        total = total + fold(jnp.square(x[:, j * piece:(j + 1) * piece].astype(F32) - mean))
    scale = lax.rsqrt(jnp.sum(total, axis=-1, keepdims=True) / width + EPSILON)
    for j in range(8):
        cols = slice(j * piece, (j + 1) * piece)
        normed[:, cols] = ((x[:, cols].astype(F32) - mean) * scale * (1.0 + gb[0:1, cols]) + gb[1:2, cols]).astype(BF16)

    for i in range(PROJ):
        for c in w_in[i]:
            c.wait()
        part = slice(i * step_w, (i + 1) * step_w)
        product = dotf(normed[:, part], w_qkv[part])
        if i == 0:
            qkv[...] = product
        else:
            qkv[...] += product
    for h in range(heads + 1):
        cols = slice(h * dim, (h + 1) * dim)
        vec = qkv[:, cols]
        partner = jnp.where(lane < half_rot, pltpu.roll(vec, dim - half_rot, 1), pltpu.roll(vec, half_rot, 1))
        qkv[:, cols] = vec * cosine + partner * sine

    row_id = lax.broadcasted_iota(jnp.int32, (slots, dim), 0).astype(F32)
    group = 8
    span = group * slots
    offset = (lax.broadcasted_iota(jnp.int32, (group, span), 1) - slots * lax.broadcasted_iota(jnp.int32, (group, span), 0)).astype(F32)
    k_cols, v_cols = slice(q_cols, q_cols + dim), slice(q_cols + dim, q_cols + 2 * dim)
    for i in range(CHUNKS):
        for c in kv_in[i]:
            c.wait()

        def put(s, carry):
            base = pl.multiple_of(i * step_s + s * 8, 8)
            lens8 = len_col[pl.ds(base, 8), :]
            new_k = qkv[pl.ds(base, 8), k_cols]
            new_v = qkv[pl.ds(base, 8), v_cols]
            for t in range(8):
                here = row_id == lens8[t:t + 1]
                k_buf[base + t] = jnp.where(here, new_k[t:t + 1], k_buf[base + t].astype(F32)).astype(BF16)
                v_buf[base + t] = jnp.where(here, new_v[t:t + 1], v_buf[base + t].astype(F32)).astype(BF16)
            return carry

        lax.fori_loop(0, step_s // 8, put, 0)
        for c in kv_out[i]:
            c.start()
        groups = [i * step_s + g * group for g in range(step_s // group)]
        all_scores = []
        for b in groups:
            q = jnp.concatenate([qkv[b:b + group, h * dim:(h + 1) * dim] for h in range(heads)], axis=0).astype(BF16)
            keys = k_buf[b:b + group].reshape(span, dim)
            all_scores.append(lax.dot_general(q, keys, (((1,), (1,)), ((), ())), preferred_element_type=F32))
        probs = []
        for b, scores in zip(groups, all_scores):
            valid = (offset >= 0.0) & (offset <= len_col[b:b + group, 0:1])
            scores = jnp.where(valid[None], scores.reshape(heads, group, span) * (dim ** -0.5), -1e30)
            peak = jnp.max(scores, axis=-1, keepdims=True)
            weight = jnp.where(valid[None], jnp.exp(scores - peak), 0.0)
            prob = (weight / jnp.sum(weight, axis=-1, keepdims=True)).astype(BF16)
            probs.append(prob.reshape(heads * group, span))
        for b, prob in zip(groups, probs):
            mixed = dotf(prob, v_buf[b:b + group].reshape(span, dim)).astype(BF16)
            for h in range(heads):
                attended[b:b + group, h * dim:(h + 1) * dim] = mixed[h * group:(h + 1) * group]
    for pair in kv_out:
        for c in pair:
            c.wait()


def run_attend(hidden, cache_k, cache_v, lengths, gain, bias, w_q, w_k, w_v):
    rows, width = hidden.shape
    seqs, slots, dim = cache_k.shape
    q_cols = w_q.shape[1]
    hbm = pl.BlockSpec(memory_space=pltpu.HBM)
    vmem = pl.BlockSpec(memory_space=pltpu.VMEM)
    return pl.pallas_call(
        attend_kernel,
        out_shape=(pltpu.VMEM((rows, q_cols), BF16), jax.ShapeDtypeStruct(cache_k.shape, BF16), jax.ShapeDtypeStruct(cache_v.shape, BF16)),
        in_specs=[hbm] * 9,
        out_specs=(vmem, hbm, hbm),
        scratch_shapes=[
            pltpu.VMEM((rows, width), BF16),
            pltpu.VMEM((8, width), F32),
            pltpu.VMEM((1, rows), jnp.int32),
            pltpu.VMEM((rows, width), BF16),
            pltpu.VMEM((width, q_cols + 2 * dim), BF16),
            pltpu.VMEM((rows, q_cols + 2 * dim), F32),
            pltpu.VMEM((rows, rows), F32),
            pltpu.VMEM((seqs, slots, dim), BF16),
            pltpu.VMEM((seqs, slots, dim), BF16),
            pltpu.SemaphoreType.DMA((4,)),
            pltpu.SemaphoreType.DMA((3, PROJ)),
            pltpu.SemaphoreType.DMA((2, CHUNKS)),
            pltpu.SemaphoreType.DMA((2, CHUNKS)),
        ],
        compiler_params=pltpu.CompilerParams(vmem_limit_bytes=62 * 1024 * 1024),
        name='attend',
    )(hidden, lengths, gain, bias, w_q, w_k, w_v, cache_k, cache_v)


PARTS = 8


def finish_kernel(logits, norm, y, out, y_out, buf, sem, y_sem):
    copy = pltpu.make_async_copy(y, y_out, y_sem)
    copy.start()
    block = logits.shape[0] // PARTS // 8 * 8
    outs = []
    for i in range(PARTS):
        size = block if i < PARTS - 1 else logits.shape[0] - block * (PARTS - 1)
        part = pl.ds(i * block, size)
        buf[part] = logits[part] - norm[0:1]
        outs.append(pltpu.make_async_copy(buf.at[part], out.at[part], sem.at[i]))
        outs[-1].start()
    for c in outs:
        c.wait()
    copy.wait()


def run_finish(logits, norm, y):
    vocab, rows = logits.shape
    vmem = pl.BlockSpec(memory_space=pltpu.VMEM)
    hbm = pl.BlockSpec(memory_space=pltpu.HBM)
    return pl.pallas_call(
        finish_kernel,
        out_shape=(jax.ShapeDtypeStruct((vocab, rows), F32), jax.ShapeDtypeStruct(y.shape, BF16)),
        in_specs=[vmem, vmem, vmem],
        out_specs=(hbm, hbm),
        scratch_shapes=[pltpu.VMEM((vocab, rows), F32), pltpu.SemaphoreType.DMA((PARTS,)), pltpu.SemaphoreType.DMA],
        compiler_params=pltpu.CompilerParams(vmem_limit_bytes=16 * 1024 * 1024),
        name='finish',
    )(logits, norm, y)


def solution(mesh):
    ways = mesh.shape['tp']
    row_spec = P('bs', None)
    cache_spec = P('bs', None, 'tp', None)
    col_split = P(None, 'tp')
    row_split = P('tp', None)
    in_specs = (row_spec, cache_spec, cache_spec, P('bs'), P(), P(), col_split, col_split, col_split, row_split, P(), P(), col_split, row_split, P(), P(), col_split)
    out_specs = (P('bs', 'tp'), cache_spec, cache_spec, row_spec)

    def local_step(new_hidden, cache_k, cache_v, lengths, ln1_gain, ln1_bias, w_q, w_k, w_v, w_o, ln2_gain, ln2_bias, w_up, w_down, lnf_gain, lnf_bias, w_out):
        shape = cache_k.shape
        flat = (shape[0], shape[1], shape[3])
        attended, new_cache_k, new_cache_v = run_attend(new_hidden, cache_k.reshape(flat), cache_v.reshape(flat), lengths[None], ln1_gain[None], ln1_bias[None], w_q, w_k, w_v)
        logits, norm, y = run_tail(ways, attended, new_hidden, w_o, w_up, w_down, w_out.T,
                                   ln2_gain[None], ln2_bias[None], lnf_gain[None], lnf_bias[None])
        log_probs_t, out_hidden = run_finish(logits, norm, y)
        return log_probs_t.T, new_cache_k.reshape(shape), new_cache_v.reshape(shape), out_hidden

    return jax.shard_map(local_step, mesh=mesh, in_specs=in_specs, out_specs=out_specs, check_vma=False)
```

```python
import functools
import math

import jax
import jax.numpy as jnp
from jax import lax
from jax.experimental import pallas as pl
from jax.experimental.pallas import tpu as pltpu
from jax.sharding import PartitionSpec as P

EPSILON = 1e-5
ROPE_BASE = 10000.0
BF16 = jnp.bfloat16
F32 = jnp.float32
MESH = pl.DeviceIdType.MESH
RING = 13
FLIPS = 12
BLOCK = 256
FILL = (
    (((0, 1, 2), (0,)), (('up', 3), (1, 2)), (('down', 4, 5), (3,)), ((6, 7, 8), (4,))),
    (((9, 10, 11, 12), (5,)), (('last',), (6, 7, 8)), ((), (9, 10)), ((), (11, 12))),
)
ROWS = 512
NSEM = 26


def dotf(lhs, rhs):
    return jnp.dot(lhs, rhs, preferred_element_type=F32)


def fold(values):
    out = values[:, 0:128]
    for lane in range(128, values.shape[1], 128):
        out = out + values[:, lane:lane + 128]
    return out


def norm_chunks(chunks, gain, bias, out):
    count, rows, piece = chunks.shape
    width = count * piece
    total = jnp.zeros((rows, 128), F32)
    for j in range(count):
        total = total + fold(chunks[j].astype(F32))
    mean = jnp.sum(total, axis=-1, keepdims=True) / width
    total = jnp.zeros((rows, 128), F32)
    for j in range(count):
        total = total + fold(jnp.square(chunks[j].astype(F32) - mean))
    scale = lax.rsqrt(jnp.sum(total, axis=-1, keepdims=True) / width + EPSILON)
    for j in range(count):
        cols = slice(j * piece, (j + 1) * piece)
        normed = (chunks[j].astype(F32) - mean) * scale * (1.0 + gain[:, cols]) + bias[:, cols]
        out[:, cols] = normed.astype(BF16)


def tail_kernel(ways, attended, hidden, w_o, w_up, w_down, w_out, gain2, bias2, gainf, biasf,
                logits, norm_out, y_out,
                ring, turned, last, resid, act, normed, normed_t, parts, raw1, raw2, sib, sibh, send3, recv3, own, gath, stats,
                w_sem, small_sem, send_sem, recv_sem, stat_send, stat_recv):
    me = lax.axis_index('tp')
    core = lax.rem(me, 2)
    chip = me // 2
    chips = ways // 2
    right = lax.rem(chip + 1, chips)
    left = lax.rem(chip + chips - 1, chips)
    far = lax.rem(chip + 2, chips)
    other = 1 - core
    rows, piece = resid.shape
    half = rows // 2
    top, bot = pl.ds(0, half), pl.ds(half, half)
    vocab, width = w_out.shape
    n_full = vocab // ROWS
    rest = vocab - n_full * ROWS
    s_o, s_up, s_down = RING - 5, RING - 4, RING - 2

    def dev(c, k):
        return {'tp': 2 * c + k}

    ld_res = pltpu.make_async_copy(hidden.at[:, pl.ds(pl.multiple_of(me * piece, piece), piece)], resid, small_sem.at[0])
    ld_o = pltpu.make_async_copy(w_o, ring.at[s_o, pl.ds(0, w_o.shape[0])], w_sem.at[s_o])
    ld_up = []
    for i in range(width // ROWS):
        ld_up.append(pltpu.make_async_copy(w_up.at[pl.ds(i * ROWS, ROWS)], ring.at[s_up + i // 3, :, pl.ds((i % 3) * w_up.shape[1], w_up.shape[1])], small_sem.at[4 + i]))
    ld_down = [pltpu.make_async_copy(w_down.at[pl.ds(i * ROWS, ROWS)], ring.at[s_down + i], small_sem.at[1 + i]) for i in range(2)]
    ld_last = pltpu.make_async_copy(w_out.at[pl.ds(n_full * ROWS, rest)], last, small_sem.at[3])

    def ld_tile(tile):
        slot = lax.rem(tile, RING)
        return pltpu.make_async_copy(w_out.at[pl.ds(pl.multiple_of(tile * ROWS, ROWS), ROWS)], ring.at[slot], w_sem.at[slot])

    ld_o.start()
    ld_res.start()

    def start(item):
        if item == 'up':
            for c in ld_up:
                c.start()
        elif item == 'down':
            for c in ld_down:
                c.start()
        elif item == 'last':
            ld_last.start()
        else:
            ld_tile(item).start()

    def flip(tile):
        ld_tile(tile).wait()
        target = ring.at[tile] if tile < FLIPS else turned

        def turn(b, carry):
            for part in range(2):
                cols = pl.ds(pl.multiple_of((2 * b + part) * BLOCK, BLOCK), BLOCK)
                for a in range(0, ROWS, BLOCK):
                    target[a:a + BLOCK, cols] = ring[tile, a:a + BLOCK, cols].T
            return carry

        lax.fori_loop(0, width // BLOCK // 2, turn, 0)
        if tile == FLIPS:
            ld_tile(tile + RING).start()

    barrier = pltpu.get_barrier_semaphore()
    for d in range(1, ways):
        pl.semaphore_signal(barrier, inc=1, device_id={'tp': lax.rem(me + d, ways)}, device_id_type=MESH)

    def copy(phase, idx, src, dst, to, ridx=None):
        ridx = idx if ridx is None else ridx
        return pltpu.make_async_remote_copy(src_ref=src, dst_ref=dst, send_sem=send_sem.at[phase, idx], recv_sem=recv_sem.at[phase, ridx],
                                            device_id=to, device_id_type=MESH)

    def arrive(phase, idx, dst):
        copy(phase, idx, dst, dst, dev(chip, core)).wait_recv()

    def busy(work):
        for item in work[0]:
            start(item)
        for tile in work[1]:
            flip(tile)

    def all_sum(phase, product, residual, fill):
        pb = parts.at[phase]
        sent = []

        def go(c):
            c.start()
            sent.append(c)

        def term(c):
            value = product(c).astype(BF16)
            pb[2 * c] = value[:, :piece]
            pb[2 * c + 1] = value[:, piece:]

        g = gath.at[phase]
        term(far)
        if phase == 0:
            pl.semaphore_wait(barrier, ways - 1)
        for k in range(2):
            go(copy(phase, k, pb.at[2 * far + k, top], raw1.at[phase, 0, core], dev(right, k), core))
            go(copy(phase, 2 + k, pb.at[2 * far + k, bot], raw1.at[phase, 1, core], dev(left, k), 2 + core))
        term(right)
        for k in range(2):
            go(copy(phase, 6 + k, pb.at[2 * right + k, bot], raw2.at[phase, 1, core], dev(right, k), 6 + core))
        go(copy(phase, 9, pb.at[2 * right + other, top], sibh.at[phase, 0], dev(chip, other)))
        term(left)
        for k in range(2):
            go(copy(phase, 4 + k, pb.at[2 * left + k, top], raw2.at[phase, 0, core], dev(left, k), 4 + core))
        go(copy(phase, 10, pb.at[2 * left + other, bot], sibh.at[phase, 1], dev(chip, other)))
        term(chip)
        go(copy(phase, 8, pb.at[2 * chip + other], sib.at[phase], dev(chip, other)))
        busy(fill[0])
        for side, (to, rws) in enumerate(((right, top), (left, bot))):
            for k in range(2):
                arrive(phase, 2 * side + k, raw1.at[phase, side, k])
            arrive(phase, 9 + side, sibh.at[phase, side])
            send3[phase, side] = (raw1[phase, side, 0].astype(F32) + raw1[phase, side, 1].astype(F32)
                                  + pb[2 * to + core, rws].astype(F32) + sibh[phase, side].astype(F32))
            go(copy(phase, 11 + side, send3.at[phase, side], recv3.at[phase, side], dev(to, core)))
        busy(fill[1])
        arrive(phase, 8, sib.at[phase])
        for side, rws in enumerate((top, bot)):
            for k in range(2):
                arrive(phase, 4 + 2 * side + k, raw2.at[phase, side, k])
            base = (residual[rws].astype(F32) + pb[me, rws].astype(F32) + sib[phase, rws].astype(F32)
                    + raw2[phase, side, 0].astype(F32) + raw2[phase, side, 1].astype(F32))
            arrive(phase, 11 + side, recv3.at[phase, side])
            value = (base + recv3[phase, side]).astype(BF16)
            own[phase, rws] = value
            g[me, rws] = value
        ob = own.at[phase]
        go(copy(phase, 13, ob.at[top], g.at[me, top], dev(right, core)))
        go(copy(phase, 16, ob.at[bot], g.at[me, bot], dev(left, core)))
        go(copy(phase, 19, ob, g.at[me], dev(chip, other)))
        go(copy(phase, 14, ob.at[bot], g.at[me, bot], dev(right, core)))
        go(copy(phase, 15, ob.at[top], g.at[me, top], dev(left, core)))
        busy(fill[2])
        ml, mr, mf = 2 * left + core, 2 * right + core, 2 * far + core
        arrive(phase, 13, g.at[ml, top])
        go(copy(phase, 17, g.at[ml, top], g.at[ml, top], dev(right, core)))
        arrive(phase, 16, g.at[mr, bot])
        go(copy(phase, 18, g.at[mr, bot], g.at[mr, bot], dev(left, core)))
        go(copy(phase, 20, g.at[ml, top], g.at[ml, top], dev(chip, other)))
        go(copy(phase, 21, g.at[mr, bot], g.at[mr, bot], dev(chip, other)))
        busy(fill[3])
        arrive(phase, 14, g.at[ml, bot])
        go(copy(phase, 22, g.at[ml, bot], g.at[ml, bot], dev(chip, other)))
        arrive(phase, 15, g.at[mr, top])
        go(copy(phase, 23, g.at[mr, top], g.at[mr, top], dev(chip, other)))
        arrive(phase, 17, g.at[mf, top])
        go(copy(phase, 24, g.at[mf, top], g.at[mf, top], dev(chip, other)))
        arrive(phase, 18, g.at[mf, bot])
        go(copy(phase, 25, g.at[mf, bot], g.at[mf, bot], dev(chip, other)))
        ol, orr, of = 2 * left + other, 2 * right + other, 2 * far + other
        arrive(phase, 19, g.at[2 * chip + other])
        arrive(phase, 20, g.at[ol, top])
        arrive(phase, 21, g.at[orr, bot])
        arrive(phase, 22, g.at[ol, bot])
        arrive(phase, 23, g.at[orr, top])
        arrive(phase, 24, g.at[of, top])
        arrive(phase, 25, g.at[of, bot])
        return sent

    ld_o.wait()
    ld_res.wait()
    depth_o = w_o.shape[0]

    def product_o(c):
        return dotf(attended[...], ring[s_o, 0:depth_o, pl.ds(pl.multiple_of(2 * piece * c, 2 * piece), 2 * piece)])

    sent = all_sum(0, product_o, resid, FILL[0])
    norm_chunks(gath.at[0], gain2, bias2, normed)

    for c in ld_up:
        c.wait()
    ff = w_up.shape[1]
    for n in range(0, ff, 256):
        total = jnp.zeros((rows, 256), F32)
        for i in range(width // ROWS):
            total = total + dotf(normed[:, i * ROWS:(i + 1) * ROWS], ring[s_up + i // 3, :, (i % 3) * ff + n:(i % 3) * ff + n + 256])
        act[:, n:n + 256] = jnp.square(jnp.maximum(total, 0.0)).astype(BF16)
    for c in ld_down:
        c.wait()

    def product_down(c):
        cols = pl.ds(pl.multiple_of(2 * piece * c, 2 * piece), 2 * piece)
        return dotf(act[:, :ROWS], ring[s_down, :, cols]) + dotf(act[:, ROWS:], ring[s_down + 1, :, cols])

    sent += all_sum(1, product_down, gath.at[0, me], FILL[1])
    norm_chunks(gath.at[1], gainf, biasf, normed)
    for j in range(ways):
        y_out[:, j * piece:(j + 1) * piece] = gath[1, j]
        normed_t[j * piece:(j + 1) * piece] = normed[:, j * piece:(j + 1) * piece].T

    def reduce_tile(z, carry):
        peak, total = carry
        z3 = z.reshape(z.shape[0] // 8, 8, z.shape[1])
        new_peak = jnp.maximum(peak, jnp.max(z3, axis=0))
        total = total * jnp.exp(peak - new_peak) + jnp.sum(jnp.exp(z3 - new_peak[None]), axis=0)
        return new_peak, total

    def rows_of(tile):
        return pl.ds(pl.multiple_of(tile * ROWS, ROWS), ROWS)

    def refill(tile):
        @pl.when(tile + RING < n_full)
        def _():
            ld_tile(tile + RING).start()

    def step_turned(pair, carry):
        for t in range(2):
            before = jnp.maximum(2 * pair - 2 + t, 0)
            carry = reduce_tile(logits[rows_of(before)], carry)
        for t in range(2):
            tile = 2 * pair + t
            for a in range(0, ROWS, BLOCK):
                z = jnp.zeros((rows, BLOCK), F32)
                for b in range(0, width, BLOCK):
                    z = z + dotf(normed[:, b:b + BLOCK], ring[tile, a:a + BLOCK, b:b + BLOCK])
                logits[pl.ds(pl.multiple_of(tile * ROWS + a, BLOCK), BLOCK)] = z.T
        for t in range(2):
            refill(2 * pair + t)
        return carry

    def turned_product(tile):
        for a in range(0, ROWS, BLOCK):
            z = jnp.zeros((rows, BLOCK), F32)
            for b in range(0, width, BLOCK):
                z = z + dotf(normed[:, b:b + BLOCK], turned[a:a + BLOCK, b:b + BLOCK])
            logits[pl.ds(pl.multiple_of(tile * ROWS + a, BLOCK), BLOCK)] = z.T

    def step_pair(pair, carry):
        tile = FLIPS + 2 * pair
        plain, coming = lax.rem(tile + 1, RING), lax.rem(tile + 2, RING)
        ld_tile(tile + 1).wait()
        ld_tile(tile + 2).wait()
        for t in range(2):
            carry = reduce_tile(logits[rows_of(tile - 2 + t)], carry)
        turned_product(tile)
        for a in range(0, ROWS, BLOCK):
            logits[pl.ds(pl.multiple_of((tile + 1) * ROWS + a, BLOCK), BLOCK)] = dotf(ring[plain, a:a + BLOCK], normed_t[...])
            for b in range(width // ROWS * a, width // ROWS * (a + BLOCK), BLOCK):
                for r in range(0, ROWS, BLOCK):
                    turned[r:r + BLOCK, b:b + BLOCK] = ring[coming, r:r + BLOCK, b:b + BLOCK].T
        refill(tile + 1)
        refill(tile + 2)
        return carry

    logits[pl.ds(0, 2 * ROWS)] = jnp.full((2 * ROWS, rows), -1e30, F32)
    carry = (jnp.full((8, rows), -1e30, F32), jnp.zeros((8, rows), F32))
    carry = lax.fori_loop(0, FLIPS // 2, step_turned, carry)
    carry = lax.fori_loop(0, (n_full - FLIPS - 1) // 2, step_pair, carry)
    for t in range(n_full - 3, n_full - 1):
        carry = reduce_tile(logits[rows_of(t)], carry)
    ld_last.wait()
    turned_product(n_full - 1)
    logits[pl.ds(n_full * ROWS, rest)] = dotf(last[...], normed_t[...])
    peak8, total8 = reduce_tile(logits[pl.ds((n_full - 1) * ROWS, ROWS + rest)], carry)
    peak = jnp.max(peak8, axis=0, keepdims=True)
    total = jnp.sum(total8 * jnp.exp(peak8 - peak), axis=0, keepdims=True)
    row = lax.broadcasted_iota(jnp.int32, (8, rows), 0)
    stats[me] = jnp.where(row == 0, peak, total)
    stat_out = []
    for d in range(1, ways):
        c = pltpu.make_async_remote_copy(src_ref=stats.at[me], dst_ref=stats.at[me], send_sem=stat_send.at[d], recv_sem=stat_recv.at[d],
                                         device_id={'tp': lax.rem(me + d, ways)}, device_id_type=MESH)
        c.start()
        stat_out.append(c)
    for d in range(1, ways):
        src = lax.rem(me + ways - d, ways)
        pltpu.make_async_remote_copy(src_ref=stats.at[src], dst_ref=stats.at[src], send_sem=stat_send.at[d], recv_sem=stat_recv.at[d],
                                     device_id={'tp': me}, device_id_type=MESH).wait_recv()
    all_stats = stats[...]
    peaks = all_stats[:, 0, :]
    totals = all_stats[:, 1, :]
    top_peak = jnp.max(peaks, axis=0, keepdims=True)
    whole = jnp.sum(totals * jnp.exp(peaks - top_peak), axis=0, keepdims=True)
    norm_out[...] = jnp.broadcast_to(top_peak + jnp.log(whole), norm_out.shape)
    for c in sent + stat_out:
        c.wait_send()


def run_tail(ways, attended, hidden, w_o, w_up, w_down, w_out_t, gain2, bias2, gainf, biasf):
    rows, width = hidden.shape
    piece = width // ways
    half = rows // 2
    vocab = w_out_t.shape[0]
    rest = vocab % ROWS
    ff = w_up.shape[1]
    any_ = pl.BlockSpec(memory_space=pl.ANY)
    vmem = pl.BlockSpec(memory_space=pltpu.VMEM)
    hbm = pl.BlockSpec(memory_space=pltpu.HBM)
    return pl.pallas_call(
        functools.partial(tail_kernel, ways),
        out_shape=(pltpu.VMEM((vocab, rows), F32), pltpu.VMEM((8, rows), F32), pltpu.VMEM((rows, width), BF16)),
        in_specs=[vmem, hbm, hbm, hbm, hbm, hbm, vmem, vmem, vmem, vmem],
        out_specs=(vmem, vmem, vmem),
        scratch_shapes=[
            pltpu.VMEM((RING, ROWS, width), BF16),
            pltpu.VMEM((ROWS, width), BF16),
            pltpu.VMEM((rest, width), BF16),
            pltpu.VMEM((rows, piece), BF16),
            pltpu.VMEM((rows, ff), BF16),
            pltpu.VMEM((rows, width), BF16),
            pltpu.VMEM((width, rows), BF16),
            pltpu.VMEM((2, ways, rows, piece), BF16),
            pltpu.VMEM((2, 2, 2, half, piece), BF16),
            pltpu.VMEM((2, 2, 2, half, piece), BF16),
            pltpu.VMEM((2, rows, piece), BF16),
            pltpu.VMEM((2, 2, half, piece), BF16),
            pltpu.VMEM((2, 2, half, piece), F32),
            pltpu.VMEM((2, 2, half, piece), F32),
            pltpu.VMEM((2, rows, piece), BF16),
            pltpu.VMEM((2, ways, rows, piece), BF16),
            pltpu.VMEM((ways, 8, rows), F32),
            pltpu.SemaphoreType.DMA((RING,)),
            pltpu.SemaphoreType.DMA((10,)),
            pltpu.SemaphoreType.DMA((2, NSEM)),
            pltpu.SemaphoreType.DMA((2, NSEM)),
            pltpu.SemaphoreType.DMA((ways,)),
            pltpu.SemaphoreType.DMA((ways,)),
        ],
        compiler_params=pltpu.CompilerParams(collective_id=0, has_side_effects=True, vmem_limit_bytes=LIMIT),
        name='tail',
    )(pltpu.with_memory_space_constraint(attended, pltpu.VMEM), hidden, w_o, w_up, w_down, w_out_t, gain2, bias2, gainf, biasf)


LIMIT = 53 * 1024 * 1024


CHUNKS = 4
PROJ = 2


def attend_kernel(hidden, lengths, gain, bias, w_q, w_k, w_v, cache_k, cache_v,
                  attended, out_k, out_v,
                  x, gb, len_row, normed, w_qkv, qkv, len_col, k_buf, v_buf, misc_sem, w_sem, in_sem, out_sem):
    rows, width = hidden.shape
    seqs, slots, dim = cache_k.shape
    q_cols = w_q.shape[1]
    heads = q_cols // dim
    step_w = width // PROJ
    step_s = seqs // CHUNKS

    small = [pltpu.make_async_copy(hidden, x, misc_sem.at[0]),
             pltpu.make_async_copy(gain, gb.at[pl.ds(0, 1)], misc_sem.at[1]),
             pltpu.make_async_copy(bias, gb.at[pl.ds(1, 1)], misc_sem.at[2]),
             pltpu.make_async_copy(lengths, len_row, misc_sem.at[3])]
    for c in small:
        c.start()
    w_in = []
    for i in range(PROJ):
        part = pl.ds(i * step_w, step_w)
        w_in.append([pltpu.make_async_copy(w_q.at[part], w_qkv.at[part, pl.ds(0, q_cols)], w_sem.at[0, i]),
                     pltpu.make_async_copy(w_k.at[part], w_qkv.at[part, pl.ds(q_cols, dim)], w_sem.at[1, i]),
                     pltpu.make_async_copy(w_v.at[part], w_qkv.at[part, pl.ds(q_cols + dim, dim)], w_sem.at[2, i])])
        for c in w_in[-1]:
            c.start()
    kv_in, kv_out = [], []
    for i in range(CHUNKS):
        part = pl.ds(i * step_s, step_s)
        kv_in.append([pltpu.make_async_copy(cache_k.at[part], k_buf.at[part], in_sem.at[0, i]),
                      pltpu.make_async_copy(cache_v.at[part], v_buf.at[part], in_sem.at[1, i])])
        kv_out.append([pltpu.make_async_copy(k_buf.at[part], out_k.at[part], out_sem.at[0, i]),
                       pltpu.make_async_copy(v_buf.at[part], out_v.at[part], out_sem.at[1, i])])
        for c in kv_in[-1]:
            c.start()

    small[3].wait()
    lens = jnp.broadcast_to(len_row[...].astype(F32), (rows, rows)).T
    len_col[...] = lens
    lane = lax.broadcasted_iota(jnp.int32, (1, dim), 1)
    half_rot = dim // 4
    freq_lane = jnp.where(lane < half_rot, lane, lane - half_rot).astype(F32)
    inv_freq = jnp.where(lane < 2 * half_rot, jnp.exp(freq_lane * (-2.0 / (2 * half_rot) * math.log(ROPE_BASE))), 0.0)
    angle = lens * inv_freq
    cosine = jnp.cos(angle)
    sine = jnp.where(lane < half_rot, -1.0, 1.0) * jnp.sin(angle)
    for c in small[:3]:
        c.wait()
    total = jnp.zeros((rows, 128), F32)
    piece = width // 8
    for j in range(8):
        total = total + fold(x[:, j * piece:(j + 1) * piece].astype(F32))
    mean = jnp.sum(total, axis=-1, keepdims=True) / width
    total = jnp.zeros((rows, 128), F32)
    for j in range(8):
        total = total + fold(jnp.square(x[:, j * piece:(j + 1) * piece].astype(F32) - mean))
    scale = lax.rsqrt(jnp.sum(total, axis=-1, keepdims=True) / width + EPSILON)
    for j in range(8):
        cols = slice(j * piece, (j + 1) * piece)
        normed[:, cols] = ((x[:, cols].astype(F32) - mean) * scale * (1.0 + gb[0:1, cols]) + gb[1:2, cols]).astype(BF16)

    for i in range(PROJ):
        for c in w_in[i]:
            c.wait()
        part = slice(i * step_w, (i + 1) * step_w)
        product = dotf(normed[:, part], w_qkv[part])
        if i == 0:
            qkv[...] = product
        else:
            qkv[...] += product
    for h in range(heads + 1):
        cols = slice(h * dim, (h + 1) * dim)
        vec = qkv[:, cols]
        partner = jnp.where(lane < half_rot, pltpu.roll(vec, dim - half_rot, 1), pltpu.roll(vec, half_rot, 1))
        qkv[:, cols] = vec * cosine + partner * sine

    row_id = lax.broadcasted_iota(jnp.int32, (slots, dim), 0).astype(F32)
    group = 8
    span = group * slots
    offset = (lax.broadcasted_iota(jnp.int32, (group, span), 1) - slots * lax.broadcasted_iota(jnp.int32, (group, span), 0)).astype(F32)
    k_cols, v_cols = slice(q_cols, q_cols + dim), slice(q_cols + dim, q_cols + 2 * dim)
    for i in range(CHUNKS):
        for c in kv_in[i]:
            c.wait()

        def put(s, carry):
            base = pl.multiple_of(i * step_s + s * 8, 8)
            lens8 = len_col[pl.ds(base, 8), :]
            new_k = qkv[pl.ds(base, 8), k_cols]
            new_v = qkv[pl.ds(base, 8), v_cols]
            for t in range(8):
                here = row_id == lens8[t:t + 1]
                k_buf[base + t] = jnp.where(here, new_k[t:t + 1], k_buf[base + t].astype(F32)).astype(BF16)
                v_buf[base + t] = jnp.where(here, new_v[t:t + 1], v_buf[base + t].astype(F32)).astype(BF16)
            return carry

        lax.fori_loop(0, step_s // 8, put, 0)
        for c in kv_out[i]:
            c.start()
        groups = [i * step_s + g * group for g in range(step_s // group)]
        all_scores = []
        for b in groups:
            q = jnp.concatenate([qkv[b:b + group, h * dim:(h + 1) * dim] for h in range(heads)], axis=0).astype(BF16)
            keys = k_buf[b:b + group].reshape(span, dim)
            all_scores.append(lax.dot_general(q, keys, (((1,), (1,)), ((), ())), preferred_element_type=F32))
        probs = []
        for b, scores in zip(groups, all_scores):
            valid = (offset >= 0.0) & (offset <= len_col[b:b + group, 0:1])
            scores = jnp.where(valid[None], scores.reshape(heads, group, span) * (dim ** -0.5), -1e30)
            peak = jnp.max(scores, axis=-1, keepdims=True)
            weight = jnp.where(valid[None], jnp.exp(scores - peak), 0.0)
            prob = (weight / jnp.sum(weight, axis=-1, keepdims=True)).astype(BF16)
            probs.append(prob.reshape(heads * group, span))
        for b, prob in zip(groups, probs):
            mixed = dotf(prob, v_buf[b:b + group].reshape(span, dim)).astype(BF16)
            for h in range(heads):
                attended[b:b + group, h * dim:(h + 1) * dim] = mixed[h * group:(h + 1) * group]
    for pair in kv_out:
        for c in pair:
            c.wait()


def run_attend(hidden, cache_k, cache_v, lengths, gain, bias, w_q, w_k, w_v):
    rows, width = hidden.shape
    seqs, slots, dim = cache_k.shape
    q_cols = w_q.shape[1]
    hbm = pl.BlockSpec(memory_space=pltpu.HBM)
    vmem = pl.BlockSpec(memory_space=pltpu.VMEM)
    return pl.pallas_call(
        attend_kernel,
        out_shape=(pltpu.VMEM((rows, q_cols), BF16), jax.ShapeDtypeStruct(cache_k.shape, BF16), jax.ShapeDtypeStruct(cache_v.shape, BF16)),
        in_specs=[hbm] * 9,
        out_specs=(vmem, hbm, hbm),
        scratch_shapes=[
            pltpu.VMEM((rows, width), BF16),
            pltpu.VMEM((8, width), F32),
            pltpu.VMEM((1, rows), jnp.int32),
            pltpu.VMEM((rows, width), BF16),
            pltpu.VMEM((width, q_cols + 2 * dim), BF16),
            pltpu.VMEM((rows, q_cols + 2 * dim), F32),
            pltpu.VMEM((rows, rows), F32),
            pltpu.VMEM((seqs, slots, dim), BF16),
            pltpu.VMEM((seqs, slots, dim), BF16),
            pltpu.SemaphoreType.DMA((4,)),
            pltpu.SemaphoreType.DMA((3, PROJ)),
            pltpu.SemaphoreType.DMA((2, CHUNKS)),
            pltpu.SemaphoreType.DMA((2, CHUNKS)),
        ],
        compiler_params=pltpu.CompilerParams(vmem_limit_bytes=62 * 1024 * 1024),
        name='attend',
    )(hidden, lengths, gain, bias, w_q, w_k, w_v, cache_k, cache_v)


PARTS = 8


def finish_kernel(logits, norm, y, out, y_out, buf, sem, y_sem):
    copy = pltpu.make_async_copy(y, y_out, y_sem)
    copy.start()
    block = logits.shape[0] // PARTS // 8 * 8
    outs = []
    for i in range(PARTS):
        size = block if i < PARTS - 1 else logits.shape[0] - block * (PARTS - 1)
        part = pl.ds(i * block, size)
        buf[part] = logits[part] - norm[0:1]
        outs.append(pltpu.make_async_copy(buf.at[part], out.at[part], sem.at[i]))
        outs[-1].start()
    for c in outs:
        c.wait()
    copy.wait()


def run_finish(logits, norm, y):
    vocab, rows = logits.shape
    vmem = pl.BlockSpec(memory_space=pltpu.VMEM)
    hbm = pl.BlockSpec(memory_space=pltpu.HBM)
    return pl.pallas_call(
        finish_kernel,
        out_shape=(jax.ShapeDtypeStruct((vocab, rows), F32), jax.ShapeDtypeStruct(y.shape, BF16)),
        in_specs=[vmem, vmem, vmem],
        out_specs=(hbm, hbm),
        scratch_shapes=[pltpu.VMEM((vocab, rows), F32), pltpu.SemaphoreType.DMA((PARTS,)), pltpu.SemaphoreType.DMA],
        compiler_params=pltpu.CompilerParams(vmem_limit_bytes=16 * 1024 * 1024),
        name='finish',
    )(logits, norm, y)


def solution(mesh):
    ways = mesh.shape['tp']
    row_spec = P('bs', None)
    cache_spec = P('bs', None, 'tp', None)
    col_split = P(None, 'tp')
    row_split = P('tp', None)
    in_specs = (row_spec, cache_spec, cache_spec, P('bs'), P(), P(), col_split, col_split, col_split, row_split, P(), P(), col_split, row_split, P(), P(), col_split)
    out_specs = (P('bs', 'tp'), cache_spec, cache_spec, row_spec)

    def local_step(new_hidden, cache_k, cache_v, lengths, ln1_gain, ln1_bias, w_q, w_k, w_v, w_o, ln2_gain, ln2_bias, w_up, w_down, lnf_gain, lnf_bias, w_out):
        shape = cache_k.shape
        flat = (shape[0], shape[1], shape[3])
        attended, new_cache_k, new_cache_v = run_attend(new_hidden, cache_k.reshape(flat), cache_v.reshape(flat), lengths[None], ln1_gain[None], ln1_bias[None], w_q, w_k, w_v)
        logits, norm, y = run_tail(ways, attended, new_hidden, w_o, w_up, w_down, w_out.T,
                                   ln2_gain[None], ln2_bias[None], lnf_gain[None], lnf_bias[None])
        log_probs_t, out_hidden = run_finish(logits, norm, y)
        return log_probs_t.T, new_cache_k.reshape(shape), new_cache_v.reshape(shape), out_hidden

    return jax.shard_map(local_step, mesh=mesh, in_specs=in_specs, out_specs=out_specs, check_vma=False)
```

```python
import functools
import math

import jax
import jax.numpy as jnp
from jax import lax
from jax.experimental import pallas as pl
from jax.experimental.pallas import tpu as pltpu
from jax.sharding import PartitionSpec as P

EPSILON = 1e-5
ROPE_BASE = 10000.0
BF16 = jnp.bfloat16
F32 = jnp.float32
MESH = pl.DeviceIdType.MESH
RING = 13
FLIPS = 12
BLOCK = 256
QUAD = 4
FILL = (
    (((0, 1, 2, 3), (0,)), (('up',), (1, 2)), (('down', 4, 5), (3,)), ((6, 7, 8), (4,))),
    (((9, 10, 11, 12), (5,)), (('last',), (6, 7, 8)), ((), (9, 10)), ((), (11, 12))),
)
ROWS = 512
NSEM = 26


def dotf(lhs, rhs):
    return jnp.dot(lhs, rhs, preferred_element_type=F32)


def fold(values):
    out = values[:, 0:128]
    for lane in range(128, values.shape[1], 128):
        out = out + values[:, lane:lane + 128]
    return out


def norm_chunks(chunks, gain, bias, out):
    count, rows, piece = chunks.shape
    width = count * piece
    total = jnp.zeros((rows, 128), F32)
    for j in range(count):
        total = total + fold(chunks[j].astype(F32))
    mean = jnp.sum(total, axis=-1, keepdims=True) / width
    total = jnp.zeros((rows, 128), F32)
    for j in range(count):
        total = total + fold(jnp.square(chunks[j].astype(F32) - mean))
    scale = lax.rsqrt(jnp.sum(total, axis=-1, keepdims=True) / width + EPSILON)
    for j in range(count):
        cols = slice(j * piece, (j + 1) * piece)
        normed = (chunks[j].astype(F32) - mean) * scale * (1.0 + gain[:, cols]) + bias[:, cols]
        out[:, cols] = normed.astype(BF16)


def tail_kernel(ways, attended, hidden, w_o, w_up, w_down, w_out, gain2, bias2, gainf, biasf,
                logits, norm_out, y_out,
                ring, turned, last, resid, act, normed, normed_t, parts, raw1, raw2, sib, sibh, send3, recv3, own, gath, stats,
                w_sem, small_sem, send_sem, recv_sem, stat_send, stat_recv):
    me = lax.axis_index('tp')
    core = lax.rem(me, 2)
    chip = me // 2
    chips = ways // 2
    right = lax.rem(chip + 1, chips)
    left = lax.rem(chip + chips - 1, chips)
    far = lax.rem(chip + 2, chips)
    other = 1 - core
    rows, piece = resid.shape
    half = rows // 2
    top, bot = pl.ds(0, half), pl.ds(half, half)
    vocab, width = w_out.shape
    n_full = vocab // ROWS
    rest = vocab - n_full * ROWS
    s_up, s_down = RING - 4, RING - 2

    def dev(c, k):
        return {'tp': 2 * c + k}

    ld_res = pltpu.make_async_copy(hidden.at[:, pl.ds(pl.multiple_of(me * piece, piece), piece)], resid, small_sem.at[0])
    ld_up = []
    for i in range(width // ROWS):
        ld_up.append(pltpu.make_async_copy(w_up.at[pl.ds(i * ROWS, ROWS)], ring.at[s_up + i // 3, :, pl.ds((i % 3) * w_up.shape[1], w_up.shape[1])], small_sem.at[4 + i]))
    ld_down = [pltpu.make_async_copy(w_down.at[pl.ds(i * ROWS, ROWS)], ring.at[s_down + i], small_sem.at[1 + i]) for i in range(2)]
    ld_last = pltpu.make_async_copy(w_out.at[pl.ds(n_full * ROWS, rest)], last, small_sem.at[3])

    def ld_tile(tile):
        slot = lax.rem(tile, RING)
        return pltpu.make_async_copy(w_out.at[pl.ds(pl.multiple_of(tile * ROWS, ROWS), ROWS)], ring.at[slot], w_sem.at[slot])

    ld_res.start()

    def start(item):
        if item == 'up':
            for c in ld_up:
                c.start()
        elif item == 'down':
            for c in ld_down:
                c.start()
        elif item == 'last':
            ld_last.start()
        else:
            ld_tile(item).start()

    def flip(tile):
        ld_tile(tile).wait()
        target = ring.at[tile] if tile < FLIPS else turned

        def turn(b, carry):
            for part in range(2):
                cols = pl.ds(pl.multiple_of((2 * b + part) * BLOCK, BLOCK), BLOCK)
                for a in range(0, ROWS, BLOCK):
                    target[a:a + BLOCK, cols] = ring[tile, a:a + BLOCK, cols].T
            return carry

        lax.fori_loop(0, width // BLOCK // 2, turn, 0)
        if tile == FLIPS:
            ld_tile(tile + RING).start()

    barrier = pltpu.get_barrier_semaphore()
    for d in range(1, ways):
        pl.semaphore_signal(barrier, inc=1, device_id={'tp': lax.rem(me + d, ways)}, device_id_type=MESH)

    def copy(phase, idx, src, dst, to, ridx=None):
        ridx = idx if ridx is None else ridx
        return pltpu.make_async_remote_copy(src_ref=src, dst_ref=dst, send_sem=send_sem.at[phase, idx], recv_sem=recv_sem.at[phase, ridx],
                                            device_id=to, device_id_type=MESH)

    def arrive(phase, idx, dst):
        copy(phase, idx, dst, dst, dev(chip, core)).wait_recv()

    def busy(work):
        for item in work[0]:
            start(item)
        for tile in work[1]:
            flip(tile)

    def all_sum(phase, product, residual, fill):
        pb = parts
        sent = []

        def go(c):
            c.start()
            sent.append(c)

        def term(c):
            value = product(c).astype(BF16)
            pb[2 * c] = value[:, :piece]
            pb[2 * c + 1] = value[:, piece:]

        g = gath.at[phase]
        term(far)
        if phase == 0:
            pl.semaphore_wait(barrier, ways - 1)
        for k in range(2):
            go(copy(phase, k, pb.at[2 * far + k, top], raw1.at[phase, 0, core], dev(right, k), core))
            go(copy(phase, 2 + k, pb.at[2 * far + k, bot], raw1.at[phase, 1, core], dev(left, k), 2 + core))
        term(right)
        for k in range(2):
            go(copy(phase, 6 + k, pb.at[2 * right + k, bot], raw2.at[phase, 1, core], dev(right, k), 6 + core))
        go(copy(phase, 9, pb.at[2 * right + other, top], sibh.at[phase, 0], dev(chip, other)))
        term(left)
        for k in range(2):
            go(copy(phase, 4 + k, pb.at[2 * left + k, top], raw2.at[phase, 0, core], dev(left, k), 4 + core))
        go(copy(phase, 10, pb.at[2 * left + other, bot], sibh.at[phase, 1], dev(chip, other)))
        term(chip)
        go(copy(phase, 8, pb.at[2 * chip + other], sib.at[phase], dev(chip, other)))
        busy(fill[0])
        for side, (to, rws) in enumerate(((right, top), (left, bot))):
            for k in range(2):
                arrive(phase, 2 * side + k, raw1.at[phase, side, k])
            arrive(phase, 9 + side, sibh.at[phase, side])
            send3[phase, side] = (raw1[phase, side, 0].astype(F32) + raw1[phase, side, 1].astype(F32)
                                  + pb[2 * to + core, rws].astype(F32) + sibh[phase, side].astype(F32))
            go(copy(phase, 11 + side, send3.at[phase, side], recv3.at[phase, side], dev(to, core)))
        busy(fill[1])
        arrive(phase, 8, sib.at[phase])
        for side, rws in enumerate((top, bot)):
            for k in range(2):
                arrive(phase, 4 + 2 * side + k, raw2.at[phase, side, k])
            base = (residual[rws].astype(F32) + pb[me, rws].astype(F32) + sib[phase, rws].astype(F32)
                    + raw2[phase, side, 0].astype(F32) + raw2[phase, side, 1].astype(F32))
            arrive(phase, 11 + side, recv3.at[phase, side])
            value = (base + recv3[phase, side]).astype(BF16)
            own[phase, rws] = value
            g[me, rws] = value
        ob = own.at[phase]
        go(copy(phase, 13, ob.at[top], g.at[me, top], dev(right, core)))
        go(copy(phase, 16, ob.at[bot], g.at[me, bot], dev(left, core)))
        go(copy(phase, 19, ob, g.at[me], dev(chip, other)))
        go(copy(phase, 14, ob.at[bot], g.at[me, bot], dev(right, core)))
        go(copy(phase, 15, ob.at[top], g.at[me, top], dev(left, core)))
        busy(fill[2])
        ml, mr, mf = 2 * left + core, 2 * right + core, 2 * far + core
        arrive(phase, 13, g.at[ml, top])
        go(copy(phase, 17, g.at[ml, top], g.at[ml, top], dev(right, core)))
        arrive(phase, 16, g.at[mr, bot])
        go(copy(phase, 18, g.at[mr, bot], g.at[mr, bot], dev(left, core)))
        go(copy(phase, 20, g.at[ml, top], g.at[ml, top], dev(chip, other)))
        go(copy(phase, 21, g.at[mr, bot], g.at[mr, bot], dev(chip, other)))
        busy(fill[3])
        arrive(phase, 14, g.at[ml, bot])
        go(copy(phase, 22, g.at[ml, bot], g.at[ml, bot], dev(chip, other)))
        arrive(phase, 15, g.at[mr, top])
        go(copy(phase, 23, g.at[mr, top], g.at[mr, top], dev(chip, other)))
        arrive(phase, 17, g.at[mf, top])
        go(copy(phase, 24, g.at[mf, top], g.at[mf, top], dev(chip, other)))
        arrive(phase, 18, g.at[mf, bot])
        go(copy(phase, 25, g.at[mf, bot], g.at[mf, bot], dev(chip, other)))
        ol, orr, of = 2 * left + other, 2 * right + other, 2 * far + other
        arrive(phase, 19, g.at[2 * chip + other])
        arrive(phase, 20, g.at[ol, top])
        arrive(phase, 21, g.at[orr, bot])
        arrive(phase, 22, g.at[ol, bot])
        arrive(phase, 23, g.at[orr, top])
        arrive(phase, 24, g.at[of, top])
        arrive(phase, 25, g.at[of, bot])
        return sent

    ld_res.wait()

    def product_o(c):
        return dotf(attended[...], w_o[:, pl.ds(pl.multiple_of(2 * piece * c, 2 * piece), 2 * piece)])

    sent = all_sum(0, product_o, resid, FILL[0])
    norm_chunks(gath.at[0], gain2, bias2, normed)

    for c in ld_up:
        c.wait()
    ff = w_up.shape[1]
    for n in range(0, ff, 256):
        total = jnp.zeros((rows, 256), F32)
        for i in range(width // ROWS):
            total = total + dotf(normed[:, i * ROWS:(i + 1) * ROWS], ring[s_up + i // 3, :, (i % 3) * ff + n:(i % 3) * ff + n + 256])
        act[:, n:n + 256] = jnp.square(jnp.maximum(total, 0.0)).astype(BF16)
    for c in ld_down:
        c.wait()

    def product_down(c):
        cols = pl.ds(pl.multiple_of(2 * piece * c, 2 * piece), 2 * piece)
        return dotf(act[:, :ROWS], ring[s_down, :, cols]) + dotf(act[:, ROWS:], ring[s_down + 1, :, cols])

    for c in sent:
        c.wait_send()
    sent = all_sum(1, product_down, gath.at[0, me], FILL[1])
    norm_chunks(gath.at[1], gainf, biasf, normed)
    for j in range(ways):
        y_out[:, j * piece:(j + 1) * piece] = gath[1, j]
        normed_t[j * piece:(j + 1) * piece] = normed[:, j * piece:(j + 1) * piece].T

    def reduce_tile(z, carry):
        peak, total = carry
        z3 = z.reshape(z.shape[0] // 8, 8, z.shape[1])
        new_peak = jnp.maximum(peak, jnp.max(z3, axis=0))
        total = total * jnp.exp(peak - new_peak) + jnp.sum(jnp.exp(z3 - new_peak[None]), axis=0)
        return new_peak, total

    def rows_of(tile):
        return pl.ds(pl.multiple_of(tile * ROWS, ROWS), ROWS)

    def refill(tile):
        @pl.when(tile + RING < n_full)
        def _():
            ld_tile(tile + RING).start()

    def step_turned(quad, carry):
        for t in range(QUAD):
            tile = QUAD * quad + t
            carry = reduce_tile(logits[rows_of(jnp.maximum(tile - QUAD, 0))], carry)
        for t in range(QUAD):
            tile = QUAD * quad + t
            for a in range(0, ROWS, BLOCK):
                z = jnp.zeros((rows, BLOCK), F32)
                for b in range(0, width, BLOCK):
                    z = z + dotf(normed[:, b:b + BLOCK], ring[tile, a:a + BLOCK, b:b + BLOCK])
                logits[pl.ds(pl.multiple_of(tile * ROWS + a, BLOCK), BLOCK)] = z.T
            refill(tile)
        return carry

    def turned_product(tile):
        for a in range(0, ROWS, BLOCK):
            z = jnp.zeros((rows, BLOCK), F32)
            for b in range(0, width, BLOCK):
                z = z + dotf(normed[:, b:b + BLOCK], turned[a:a + BLOCK, b:b + BLOCK])
            logits[pl.ds(pl.multiple_of(tile * ROWS + a, BLOCK), BLOCK)] = z.T

    def step_pair(pair, carry):
        tile = FLIPS + 2 * pair
        plain, coming = lax.rem(tile + 1, RING), lax.rem(tile + 2, RING)
        ld_tile(tile + 1).wait()
        ld_tile(tile + 2).wait()
        for t in range(2):
            carry = reduce_tile(logits[rows_of(tile - 2 + t)], carry)
        turned_product(tile)
        for a in range(0, ROWS, BLOCK):
            logits[pl.ds(pl.multiple_of((tile + 1) * ROWS + a, BLOCK), BLOCK)] = dotf(ring[plain, a:a + BLOCK], normed_t[...])
            for b in range(width // ROWS * a, width // ROWS * (a + BLOCK), BLOCK):
                for r in range(0, ROWS, BLOCK):
                    turned[r:r + BLOCK, b:b + BLOCK] = ring[coming, r:r + BLOCK, b:b + BLOCK].T
        refill(tile + 1)
        refill(tile + 2)
        return carry

    logits[pl.ds(0, ROWS)] = jnp.full((ROWS, rows), -1e30, F32)
    carry = (jnp.full((8, rows), -1e30, F32), jnp.zeros((8, rows), F32))
    carry = lax.fori_loop(0, FLIPS // QUAD, step_turned, carry)
    for t in range(FLIPS - QUAD, FLIPS - 2):
        carry = reduce_tile(logits[rows_of(t)], carry)
    carry = lax.fori_loop(0, (n_full - FLIPS - 1) // 2, step_pair, carry)
    for t in range(n_full - 3, n_full - 1):
        carry = reduce_tile(logits[rows_of(t)], carry)
    ld_last.wait()
    turned_product(n_full - 1)
    logits[pl.ds(n_full * ROWS, rest)] = dotf(last[...], normed_t[...])
    peak8, total8 = reduce_tile(logits[pl.ds((n_full - 1) * ROWS, ROWS + rest)], carry)
    peak = jnp.max(peak8, axis=0, keepdims=True)
    total = jnp.sum(total8 * jnp.exp(peak8 - peak), axis=0, keepdims=True)
    row = lax.broadcasted_iota(jnp.int32, (8, rows), 0)
    stats[me] = jnp.where(row == 0, peak, total)
    stat_out = []
    for d in range(1, ways):
        c = pltpu.make_async_remote_copy(src_ref=stats.at[me], dst_ref=stats.at[me], send_sem=stat_send.at[d], recv_sem=stat_recv.at[d],
                                         device_id={'tp': lax.rem(me + d, ways)}, device_id_type=MESH)
        c.start()
        stat_out.append(c)
    for d in range(1, ways):
        src = lax.rem(me + ways - d, ways)
        pltpu.make_async_remote_copy(src_ref=stats.at[src], dst_ref=stats.at[src], send_sem=stat_send.at[d], recv_sem=stat_recv.at[d],
                                     device_id={'tp': me}, device_id_type=MESH).wait_recv()
    all_stats = stats[...]
    peaks = all_stats[:, 0, :]
    totals = all_stats[:, 1, :]
    top_peak = jnp.max(peaks, axis=0, keepdims=True)
    whole = jnp.sum(totals * jnp.exp(peaks - top_peak), axis=0, keepdims=True)
    norm_out[...] = jnp.broadcast_to(top_peak + jnp.log(whole), norm_out.shape)
    for c in sent + stat_out:
        c.wait_send()


def run_tail(ways, attended, hidden, w_o, w_up, w_down, w_out_t, gain2, bias2, gainf, biasf):
    rows, width = hidden.shape
    piece = width // ways
    half = rows // 2
    vocab = w_out_t.shape[0]
    rest = vocab % ROWS
    ff = w_up.shape[1]
    any_ = pl.BlockSpec(memory_space=pl.ANY)
    vmem = pl.BlockSpec(memory_space=pltpu.VMEM)
    hbm = pl.BlockSpec(memory_space=pltpu.HBM)
    return pl.pallas_call(
        functools.partial(tail_kernel, ways),
        out_shape=(pltpu.VMEM((vocab, rows), F32), pltpu.VMEM((8, rows), F32), pltpu.VMEM((rows, width), BF16)),
        in_specs=[vmem, hbm, vmem, hbm, hbm, hbm, vmem, vmem, vmem, vmem],
        out_specs=(vmem, vmem, vmem),
        scratch_shapes=[
            pltpu.VMEM((RING, ROWS, width), BF16),
            pltpu.VMEM((ROWS, width), BF16),
            pltpu.VMEM((rest, width), BF16),
            pltpu.VMEM((rows, piece), BF16),
            pltpu.VMEM((rows, ff), BF16),
            pltpu.VMEM((rows, width), BF16),
            pltpu.VMEM((width, rows), BF16),
            pltpu.VMEM((ways, rows, piece), BF16),
            pltpu.VMEM((2, 2, 2, half, piece), BF16),
            pltpu.VMEM((2, 2, 2, half, piece), BF16),
            pltpu.VMEM((2, rows, piece), BF16),
            pltpu.VMEM((2, 2, half, piece), BF16),
            pltpu.VMEM((2, 2, half, piece), F32),
            pltpu.VMEM((2, 2, half, piece), F32),
            pltpu.VMEM((2, rows, piece), BF16),
            pltpu.VMEM((2, ways, rows, piece), BF16),
            pltpu.VMEM((ways, 8, rows), F32),
            pltpu.SemaphoreType.DMA((RING,)),
            pltpu.SemaphoreType.DMA((10,)),
            pltpu.SemaphoreType.DMA((2, NSEM)),
            pltpu.SemaphoreType.DMA((2, NSEM)),
            pltpu.SemaphoreType.DMA((ways,)),
            pltpu.SemaphoreType.DMA((ways,)),
        ],
        compiler_params=pltpu.CompilerParams(collective_id=0, has_side_effects=True, vmem_limit_bytes=LIMIT),
        name='tail',
    )(pltpu.with_memory_space_constraint(attended, pltpu.VMEM), hidden, pltpu.with_memory_space_constraint(w_o, pltpu.VMEM), w_up, w_down, w_out_t, gain2, bias2, gainf, biasf)


LIMIT = int(51.6 * 1024 * 1024)


CHUNKS = 4
PROJ = 2


def attend_kernel(hidden, lengths, gain, bias, w_q, w_k, w_v, w_o, cache_k, cache_v,
                  attended, o_out, out_k, out_v,
                  x, gb, len_row, normed, w_qkv, qkv, len_col, k_buf, v_buf, misc_sem, w_sem, in_sem, out_sem):
    rows, width = hidden.shape
    seqs, slots, dim = cache_k.shape
    q_cols = w_q.shape[1]
    heads = q_cols // dim
    step_w = width // PROJ
    step_s = seqs // CHUNKS

    small = [pltpu.make_async_copy(hidden, x, misc_sem.at[0]),
             pltpu.make_async_copy(gain, gb.at[pl.ds(0, 1)], misc_sem.at[1]),
             pltpu.make_async_copy(bias, gb.at[pl.ds(1, 1)], misc_sem.at[2]),
             pltpu.make_async_copy(lengths, len_row, misc_sem.at[3])]
    for c in small:
        c.start()
    w_in = []
    for i in range(PROJ):
        part = pl.ds(i * step_w, step_w)
        w_in.append([pltpu.make_async_copy(w_q.at[part], w_qkv.at[part, pl.ds(0, q_cols)], w_sem.at[0, i]),
                     pltpu.make_async_copy(w_k.at[part], w_qkv.at[part, pl.ds(q_cols, dim)], w_sem.at[1, i]),
                     pltpu.make_async_copy(w_v.at[part], w_qkv.at[part, pl.ds(q_cols + dim, dim)], w_sem.at[2, i])])
        for c in w_in[-1]:
            c.start()
    kv_in, kv_out = [], []
    for i in range(CHUNKS):
        part = pl.ds(i * step_s, step_s)
        kv_in.append([pltpu.make_async_copy(cache_k.at[part], k_buf.at[part], in_sem.at[0, i]),
                      pltpu.make_async_copy(cache_v.at[part], v_buf.at[part], in_sem.at[1, i])])
        kv_out.append([pltpu.make_async_copy(k_buf.at[part], out_k.at[part], out_sem.at[0, i]),
                       pltpu.make_async_copy(v_buf.at[part], out_v.at[part], out_sem.at[1, i])])
        for c in kv_in[-1]:
            c.start()

    ld_o = pltpu.make_async_copy(w_o, o_out, misc_sem.at[4])
    ld_o.start()
    small[3].wait()
    lens = jnp.broadcast_to(len_row[...].astype(F32), (rows, rows)).T
    len_col[...] = lens
    lane = lax.broadcasted_iota(jnp.int32, (1, dim), 1)
    half_rot = dim // 4
    freq_lane = jnp.where(lane < half_rot, lane, lane - half_rot).astype(F32)
    inv_freq = jnp.where(lane < 2 * half_rot, jnp.exp(freq_lane * (-2.0 / (2 * half_rot) * math.log(ROPE_BASE))), 0.0)
    angle = lens * inv_freq
    cosine = jnp.cos(angle)
    sine = jnp.where(lane < half_rot, -1.0, 1.0) * jnp.sin(angle)
    for c in small[:3]:
        c.wait()
    total = jnp.zeros((rows, 128), F32)
    piece = width // 8
    for j in range(8):
        total = total + fold(x[:, j * piece:(j + 1) * piece].astype(F32))
    mean = jnp.sum(total, axis=-1, keepdims=True) / width
    total = jnp.zeros((rows, 128), F32)
    for j in range(8):
        total = total + fold(jnp.square(x[:, j * piece:(j + 1) * piece].astype(F32) - mean))
    scale = lax.rsqrt(jnp.sum(total, axis=-1, keepdims=True) / width + EPSILON)
    for j in range(8):
        cols = slice(j * piece, (j + 1) * piece)
        normed[:, cols] = ((x[:, cols].astype(F32) - mean) * scale * (1.0 + gb[0:1, cols]) + gb[1:2, cols]).astype(BF16)

    for i in range(PROJ):
        for c in w_in[i]:
            c.wait()
        part = slice(i * step_w, (i + 1) * step_w)
        product = dotf(normed[:, part], w_qkv[part])
        if i == 0:
            qkv[...] = product
        else:
            qkv[...] += product
    for h in range(heads + 1):
        cols = slice(h * dim, (h + 1) * dim)
        vec = qkv[:, cols]
        partner = jnp.where(lane < half_rot, pltpu.roll(vec, dim - half_rot, 1), pltpu.roll(vec, half_rot, 1))
        qkv[:, cols] = vec * cosine + partner * sine

    row_id = lax.broadcasted_iota(jnp.int32, (slots, dim), 0).astype(F32)
    group = 8
    span = group * slots
    offset = (lax.broadcasted_iota(jnp.int32, (group, span), 1) - slots * lax.broadcasted_iota(jnp.int32, (group, span), 0)).astype(F32)
    k_cols, v_cols = slice(q_cols, q_cols + dim), slice(q_cols + dim, q_cols + 2 * dim)
    for i in range(CHUNKS):
        for c in kv_in[i]:
            c.wait()

        def put(s, carry):
            base = pl.multiple_of(i * step_s + s * 8, 8)
            lens8 = len_col[pl.ds(base, 8), :]
            new_k = qkv[pl.ds(base, 8), k_cols]
            new_v = qkv[pl.ds(base, 8), v_cols]
            for t in range(8):
                here = row_id == lens8[t:t + 1]
                k_buf[base + t] = jnp.where(here, new_k[t:t + 1], k_buf[base + t].astype(F32)).astype(BF16)
                v_buf[base + t] = jnp.where(here, new_v[t:t + 1], v_buf[base + t].astype(F32)).astype(BF16)
            return carry

        lax.fori_loop(0, step_s // 8, put, 0)
        for c in kv_out[i]:
            c.start()
    for i in range(CHUNKS):
        groups = [i * step_s + g * group for g in range(step_s // group)]
        all_scores = []
        for b in groups:
            q = jnp.concatenate([qkv[b:b + group, h * dim:(h + 1) * dim] for h in range(heads)], axis=0).astype(BF16)
            keys = k_buf[b:b + group].reshape(span, dim)
            all_scores.append(lax.dot_general(q, keys, (((1,), (1,)), ((), ())), preferred_element_type=F32))
        probs = []
        for b, scores in zip(groups, all_scores):
            valid = (offset >= 0.0) & (offset <= len_col[b:b + group, 0:1])
            scores = jnp.where(valid[None], scores.reshape(heads, group, span) * (dim ** -0.5), -1e30)
            peak = jnp.max(scores, axis=-1, keepdims=True)
            weight = jnp.where(valid[None], jnp.exp(scores - peak), 0.0)
            prob = (weight / jnp.sum(weight, axis=-1, keepdims=True)).astype(BF16)
            probs.append(prob.reshape(heads * group, span))
        for b, prob in zip(groups, probs):
            mixed = dotf(prob, v_buf[b:b + group].reshape(span, dim)).astype(BF16)
            for h in range(heads):
                attended[b:b + group, h * dim:(h + 1) * dim] = mixed[h * group:(h + 1) * group]
    for pair in kv_out:
        for c in pair:
            c.wait()
    ld_o.wait()


def run_attend(hidden, cache_k, cache_v, lengths, gain, bias, w_q, w_k, w_v, w_o):
    rows, width = hidden.shape
    seqs, slots, dim = cache_k.shape
    q_cols = w_q.shape[1]
    hbm = pl.BlockSpec(memory_space=pltpu.HBM)
    vmem = pl.BlockSpec(memory_space=pltpu.VMEM)
    return pl.pallas_call(
        attend_kernel,
        out_shape=(pltpu.VMEM((rows, q_cols), BF16), pltpu.VMEM(w_o.shape, BF16), jax.ShapeDtypeStruct(cache_k.shape, BF16), jax.ShapeDtypeStruct(cache_v.shape, BF16)),
        in_specs=[hbm] * 10,
        out_specs=(vmem, vmem, hbm, hbm),
        scratch_shapes=[
            pltpu.VMEM((rows, width), BF16),
            pltpu.VMEM((8, width), F32),
            pltpu.VMEM((1, rows), jnp.int32),
            pltpu.VMEM((rows, width), BF16),
            pltpu.VMEM((width, q_cols + 2 * dim), BF16),
            pltpu.VMEM((rows, q_cols + 2 * dim), F32),
            pltpu.VMEM((rows, rows), F32),
            pltpu.VMEM((seqs, slots, dim), BF16),
            pltpu.VMEM((seqs, slots, dim), BF16),
            pltpu.SemaphoreType.DMA((5,)),
            pltpu.SemaphoreType.DMA((3, PROJ)),
            pltpu.SemaphoreType.DMA((2, CHUNKS)),
            pltpu.SemaphoreType.DMA((2, CHUNKS)),
        ],
        compiler_params=pltpu.CompilerParams(vmem_limit_bytes=40 * 1024 * 1024),
        name='attend',
    )(*(pltpu.with_memory_space_constraint(v, pltpu.HBM) for v in (hidden, lengths, gain, bias, w_q, w_k, w_v, w_o, cache_k, cache_v)))


PARTS = 8


def finish_kernel(logits, norm, y, out, y_out, buf, sem, y_sem):
    copy = pltpu.make_async_copy(y, y_out, y_sem)
    copy.start()
    block = logits.shape[0] // PARTS // 8 * 8
    outs = []
    for i in range(PARTS):
        size = block if i < PARTS - 1 else logits.shape[0] - block * (PARTS - 1)
        part = pl.ds(i * block, size)
        buf[part] = logits[part] - norm[0:1]
        outs.append(pltpu.make_async_copy(buf.at[part], out.at[part], sem.at[i]))
        outs[-1].start()
    for c in outs:
        c.wait()
    copy.wait()


def run_finish(logits, norm, y):
    vocab, rows = logits.shape
    vmem = pl.BlockSpec(memory_space=pltpu.VMEM)
    hbm = pl.BlockSpec(memory_space=pltpu.HBM)
    return pl.pallas_call(
        finish_kernel,
        out_shape=(jax.ShapeDtypeStruct((vocab, rows), F32), jax.ShapeDtypeStruct(y.shape, BF16)),
        in_specs=[vmem, vmem, vmem],
        out_specs=(hbm, hbm),
        scratch_shapes=[pltpu.VMEM((vocab, rows), F32), pltpu.SemaphoreType.DMA((PARTS,)), pltpu.SemaphoreType.DMA],
        compiler_params=pltpu.CompilerParams(vmem_limit_bytes=16 * 1024 * 1024),
        name='finish',
    )(logits, norm, y)


def solution(mesh):
    ways = mesh.shape['tp']
    row_spec = P('bs', None)
    cache_spec = P('bs', None, 'tp', None)
    col_split = P(None, 'tp')
    row_split = P('tp', None)
    in_specs = (row_spec, cache_spec, cache_spec, P('bs'), P(), P(), col_split, col_split, col_split, row_split, P(), P(), col_split, row_split, P(), P(), col_split)
    out_specs = (P('bs', 'tp'), cache_spec, cache_spec, row_spec)

    def local_step(new_hidden, cache_k, cache_v, lengths, ln1_gain, ln1_bias, w_q, w_k, w_v, w_o, ln2_gain, ln2_bias, w_up, w_down, lnf_gain, lnf_bias, w_out):
        shape = cache_k.shape
        flat = (shape[0], shape[1], shape[3])
        attended, w_o, new_cache_k, new_cache_v = run_attend(new_hidden, cache_k.reshape(flat), cache_v.reshape(flat), lengths[None], ln1_gain[None], ln1_bias[None], w_q, w_k, w_v, w_o)
        logits, norm, y = run_tail(ways, attended, new_hidden, w_o, w_up, w_down, w_out.T,
                                   ln2_gain[None], ln2_bias[None], lnf_gain[None], lnf_bias[None])
        log_probs_t, out_hidden = run_finish(logits, norm, y)
        return log_probs_t.T, new_cache_k.reshape(shape), new_cache_v.reshape(shape), out_hidden

    return jax.shard_map(local_step, mesh=mesh, in_specs=in_specs, out_specs=out_specs, check_vma=False)
```

```python
import functools
import math

import jax
import jax.numpy as jnp
from jax import lax
from jax.experimental import pallas as pl
from jax.experimental.pallas import tpu as pltpu
from jax.sharding import PartitionSpec as P

EPSILON = 1e-5
ROPE_BASE = 10000.0
BF16 = jnp.bfloat16
F32 = jnp.float32
MESH = pl.DeviceIdType.MESH
RING = 13
FLIPS = 12
BLOCK = 256
QUAD = 4
FILL = (
    (((2, 3), (0,)), ((4, 'up'), (1, 2)), ((5, 'down'), (3,)), ((6, 7, 8), (4,))),
    (((9, 10), (5,)), ((11, 12), (6, 7, 8)), (('last',), (9, 10)), ((), (11, 12))),
)
ROWS = 512
NSEM = 26


def dotf(lhs, rhs):
    return jnp.dot(lhs, rhs, preferred_element_type=F32)


def fold(values):
    out = values[:, 0:128]
    for lane in range(128, values.shape[1], 128):
        out = out + values[:, lane:lane + 128]
    return out


def norm_chunks(chunks, gain, bias, out):
    count, rows, piece = chunks.shape
    width = count * piece
    total = jnp.zeros((rows, 128), F32)
    for j in range(count):
        total = total + fold(chunks[j].astype(F32))
    mean = jnp.sum(total, axis=-1, keepdims=True) / width
    total = jnp.zeros((rows, 128), F32)
    for j in range(count):
        total = total + fold(jnp.square(chunks[j].astype(F32) - mean))
    scale = lax.rsqrt(jnp.sum(total, axis=-1, keepdims=True) / width + EPSILON)
    for j in range(count):
        cols = slice(j * piece, (j + 1) * piece)
        normed = (chunks[j].astype(F32) - mean) * scale * (1.0 + gain[:, cols]) + bias[:, cols]
        out[:, cols] = normed.astype(BF16)


def tail_kernel(ways, attended, hidden, w_o, w_up, w_down, w_out, gain2, bias2, gainf, biasf,
                logits, norm_out, y_out,
                ring, turned, last, resid, act, normed, normed_t, parts, raw1, raw2, sib, sibh, send3, recv3, own, gath, stats,
                w_sem, small_sem, send_sem, recv_sem, stat_send, stat_recv):
    me = lax.axis_index('tp')
    core = lax.rem(me, 2)
    chip = me // 2
    chips = ways // 2
    right = lax.rem(chip + 1, chips)
    left = lax.rem(chip + chips - 1, chips)
    far = lax.rem(chip + 2, chips)
    other = 1 - core
    rows, piece = resid.shape
    half = rows // 2
    top, bot = pl.ds(0, half), pl.ds(half, half)
    vocab, width = w_out.shape
    n_full = vocab // ROWS
    rest = vocab - n_full * ROWS
    s_up, s_down = RING - 4, RING - 2

    def dev(c, k):
        return {'tp': 2 * c + k}

    ld_res = pltpu.make_async_copy(hidden.at[:, pl.ds(pl.multiple_of(me * piece, piece), piece)], resid, small_sem.at[0])
    ld_up = []
    for i in range(width // ROWS):
        ld_up.append(pltpu.make_async_copy(w_up.at[pl.ds(i * ROWS, ROWS)], ring.at[s_up + i // 3, :, pl.ds((i % 3) * w_up.shape[1], w_up.shape[1])], small_sem.at[4 + i]))
    ld_down = [pltpu.make_async_copy(w_down.at[pl.ds(i * ROWS, ROWS)], ring.at[s_down + i], small_sem.at[1 + i]) for i in range(2)]
    ld_last = pltpu.make_async_copy(w_out.at[pl.ds(n_full * ROWS, rest)], last, small_sem.at[3])

    def ld_tile(tile):
        slot = lax.rem(tile, RING)
        return pltpu.make_async_copy(w_out.at[pl.ds(pl.multiple_of(tile * ROWS, ROWS), ROWS)], ring.at[slot], w_sem.at[slot])

    ld_res.start()

    def start(item):
        if item == 'up':
            for c in ld_up:
                c.start()
        elif item == 'down':
            for c in ld_down:
                c.start()
        elif item == 'last':
            ld_last.start()
        else:
            ld_tile(item).start()

    def flip(tile):
        ld_tile(tile).wait()
        target = ring.at[tile] if tile < FLIPS else turned

        def turn(b, carry):
            for part in range(2):
                cols = pl.ds(pl.multiple_of((2 * b + part) * BLOCK, BLOCK), BLOCK)
                for a in range(0, ROWS, BLOCK):
                    target[a:a + BLOCK, cols] = ring[tile, a:a + BLOCK, cols].T
            return carry

        lax.fori_loop(0, width // BLOCK // 2, turn, 0)
        if tile == FLIPS:
            ld_tile(tile + RING).start()

    start(0)
    start(1)
    barrier = pltpu.get_barrier_semaphore()
    for d in range(1, ways):
        pl.semaphore_signal(barrier, inc=1, device_id={'tp': lax.rem(me + d, ways)}, device_id_type=MESH)

    def copy(phase, idx, src, dst, to, ridx=None):
        ridx = idx if ridx is None else ridx
        return pltpu.make_async_remote_copy(src_ref=src, dst_ref=dst, send_sem=send_sem.at[phase, idx], recv_sem=recv_sem.at[phase, ridx],
                                            device_id=to, device_id_type=MESH)

    def arrive(phase, idx, dst):
        copy(phase, idx, dst, dst, dev(chip, core)).wait_recv()

    def busy(work):
        for item in work[0]:
            start(item)
        for tile in work[1]:
            flip(tile)

    def all_sum(phase, product, residual, fill):
        pb = parts
        sent = []

        def go(c):
            c.start()
            sent.append(c)

        def term(c):
            value = product(c).astype(BF16)
            pb[2 * c] = value[:, :piece]
            pb[2 * c + 1] = value[:, piece:]

        g = gath.at[phase]
        term(far)
        if phase == 0:
            pl.semaphore_wait(barrier, ways - 1)
        for k in range(2):
            go(copy(phase, k, pb.at[2 * far + k, top], raw1.at[phase, 0, core], dev(right, k), core))
            go(copy(phase, 2 + k, pb.at[2 * far + k, bot], raw1.at[phase, 1, core], dev(left, k), 2 + core))
        term(right)
        for k in range(2):
            go(copy(phase, 6 + k, pb.at[2 * right + k, bot], raw2.at[phase, 1, core], dev(right, k), 6 + core))
        go(copy(phase, 9, pb.at[2 * right + other, top], sibh.at[phase, 0], dev(chip, other)))
        term(left)
        for k in range(2):
            go(copy(phase, 4 + k, pb.at[2 * left + k, top], raw2.at[phase, 0, core], dev(left, k), 4 + core))
        go(copy(phase, 10, pb.at[2 * left + other, bot], sibh.at[phase, 1], dev(chip, other)))
        term(chip)
        go(copy(phase, 8, pb.at[2 * chip + other], sib.at[phase], dev(chip, other)))
        busy(fill[0])
        for side, (to, rws) in enumerate(((right, top), (left, bot))):
            for k in range(2):
                arrive(phase, 2 * side + k, raw1.at[phase, side, k])
            arrive(phase, 9 + side, sibh.at[phase, side])
            send3[phase, side] = (raw1[phase, side, 0].astype(F32) + raw1[phase, side, 1].astype(F32)
                                  + pb[2 * to + core, rws].astype(F32) + sibh[phase, side].astype(F32))
            go(copy(phase, 11 + side, send3.at[phase, side], recv3.at[phase, side], dev(to, core)))
        busy(fill[1])
        arrive(phase, 8, sib.at[phase])
        for side, rws in enumerate((top, bot)):
            for k in range(2):
                arrive(phase, 4 + 2 * side + k, raw2.at[phase, side, k])
            base = (residual[rws].astype(F32) + pb[me, rws].astype(F32) + sib[phase, rws].astype(F32)
                    + raw2[phase, side, 0].astype(F32) + raw2[phase, side, 1].astype(F32))
            arrive(phase, 11 + side, recv3.at[phase, side])
            value = (base + recv3[phase, side]).astype(BF16)
            own[phase, rws] = value
            g[me, rws] = value
        ob = own.at[phase]
        go(copy(phase, 13, ob.at[top], g.at[me, top], dev(right, core)))
        go(copy(phase, 16, ob.at[bot], g.at[me, bot], dev(left, core)))
        go(copy(phase, 19, ob, g.at[me], dev(chip, other)))
        go(copy(phase, 14, ob.at[bot], g.at[me, bot], dev(right, core)))
        go(copy(phase, 15, ob.at[top], g.at[me, top], dev(left, core)))
        busy(fill[2])
        ml, mr, mf = 2 * left + core, 2 * right + core, 2 * far + core
        arrive(phase, 13, g.at[ml, top])
        go(copy(phase, 17, g.at[ml, top], g.at[ml, top], dev(right, core)))
        arrive(phase, 16, g.at[mr, bot])
        go(copy(phase, 18, g.at[mr, bot], g.at[mr, bot], dev(left, core)))
        go(copy(phase, 20, g.at[ml, top], g.at[ml, top], dev(chip, other)))
        go(copy(phase, 21, g.at[mr, bot], g.at[mr, bot], dev(chip, other)))
        busy(fill[3])
        arrive(phase, 14, g.at[ml, bot])
        go(copy(phase, 22, g.at[ml, bot], g.at[ml, bot], dev(chip, other)))
        arrive(phase, 15, g.at[mr, top])
        go(copy(phase, 23, g.at[mr, top], g.at[mr, top], dev(chip, other)))
        arrive(phase, 17, g.at[mf, top])
        go(copy(phase, 24, g.at[mf, top], g.at[mf, top], dev(chip, other)))
        arrive(phase, 18, g.at[mf, bot])
        go(copy(phase, 25, g.at[mf, bot], g.at[mf, bot], dev(chip, other)))
        ol, orr, of = 2 * left + other, 2 * right + other, 2 * far + other
        arrive(phase, 19, g.at[2 * chip + other])
        arrive(phase, 20, g.at[ol, top])
        arrive(phase, 21, g.at[orr, bot])
        arrive(phase, 22, g.at[ol, bot])
        arrive(phase, 23, g.at[orr, top])
        arrive(phase, 24, g.at[of, top])
        arrive(phase, 25, g.at[of, bot])
        return sent

    ld_res.wait()

    def product_o(c):
        return dotf(attended[...], w_o[:, pl.ds(pl.multiple_of(2 * piece * c, 2 * piece), 2 * piece)])

    sent = all_sum(0, product_o, resid, FILL[0])
    norm_chunks(gath.at[0], gain2, bias2, normed)

    for c in ld_up:
        c.wait()
    ff = w_up.shape[1]
    for n in range(0, ff, 256):
        total = jnp.zeros((rows, 256), F32)
        for i in range(width // ROWS):
            total = total + dotf(normed[:, i * ROWS:(i + 1) * ROWS], ring[s_up + i // 3, :, (i % 3) * ff + n:(i % 3) * ff + n + 256])
        act[:, n:n + 256] = jnp.square(jnp.maximum(total, 0.0)).astype(BF16)
    for c in ld_down:
        c.wait()

    def product_down(c):
        cols = pl.ds(pl.multiple_of(2 * piece * c, 2 * piece), 2 * piece)
        return dotf(act[:, :ROWS], ring[s_down, :, cols]) + dotf(act[:, ROWS:], ring[s_down + 1, :, cols])

    for c in sent:
        c.wait_send()
    sent = all_sum(1, product_down, gath.at[0, me], FILL[1])
    norm_chunks(gath.at[1], gainf, biasf, normed)
    for j in range(ways):
        y_out[:, j * piece:(j + 1) * piece] = gath[1, j]
        normed_t[j * piece:(j + 1) * piece] = normed[:, j * piece:(j + 1) * piece].T

    def reduce_tile(z, carry):
        peak, total = carry
        z3 = z.reshape(z.shape[0] // 8, 8, z.shape[1])
        new_peak = jnp.maximum(peak, jnp.max(z3, axis=0))
        total = total * jnp.exp(peak - new_peak) + jnp.sum(jnp.exp(z3 - new_peak[None]), axis=0)
        return new_peak, total

    def rows_of(tile):
        return pl.ds(pl.multiple_of(tile * ROWS, ROWS), ROWS)

    def refill(tile):
        @pl.when(tile + RING < n_full)
        def _():
            ld_tile(tile + RING).start()

    def step_turned(quad, carry):
        for t in range(QUAD):
            tile = QUAD * quad + t
            carry = reduce_tile(logits[rows_of(jnp.maximum(tile - QUAD, 0))], carry)
        for t in range(QUAD):
            tile = QUAD * quad + t
            for a in range(0, ROWS, BLOCK):
                z = jnp.zeros((rows, BLOCK), F32)
                for b in range(0, width, BLOCK):
                    z = z + dotf(normed[:, b:b + BLOCK], ring[tile, a:a + BLOCK, b:b + BLOCK])
                logits[pl.ds(pl.multiple_of(tile * ROWS + a, BLOCK), BLOCK)] = z.T
            ld_tile(tile + RING).start()
        return carry

    def turned_product(tile):
        for a in range(0, ROWS, BLOCK):
            z = jnp.zeros((rows, BLOCK), F32)
            for b in range(0, width, BLOCK):
                z = z + dotf(normed[:, b:b + BLOCK], turned[a:a + BLOCK, b:b + BLOCK])
            logits[pl.ds(pl.multiple_of(tile * ROWS + a, BLOCK), BLOCK)] = z.T

    def step_pair(pair, carry):
        tile = FLIPS + 2 * pair
        plain, coming = lax.rem(tile + 1, RING), lax.rem(tile + 2, RING)
        ld_tile(tile + 1).wait()
        ld_tile(tile + 2).wait()
        for t in range(2):
            carry = reduce_tile(logits[rows_of(tile - 2 + t)], carry)
        turned_product(tile)
        for a in range(0, ROWS, BLOCK):
            logits[pl.ds(pl.multiple_of((tile + 1) * ROWS + a, BLOCK), BLOCK)] = dotf(ring[plain, a:a + BLOCK], normed_t[...])
            for b in range(width // ROWS * a, width // ROWS * (a + BLOCK), BLOCK):
                for r in range(0, ROWS, BLOCK):
                    turned[r:r + BLOCK, b:b + BLOCK] = ring[coming, r:r + BLOCK, b:b + BLOCK].T
        refill(tile + 1)
        refill(tile + 2)
        return carry

    logits[pl.ds(0, ROWS)] = jnp.full((ROWS, rows), -1e30, F32)
    carry = (jnp.full((8, rows), -1e30, F32), jnp.zeros((8, rows), F32))
    carry = lax.fori_loop(0, FLIPS // QUAD, step_turned, carry)
    for t in range(FLIPS - QUAD, FLIPS - 2):
        carry = reduce_tile(logits[rows_of(t)], carry)
    carry = lax.fori_loop(0, (n_full - FLIPS - 1) // 2, step_pair, carry)
    for t in range(n_full - 3, n_full - 1):
        carry = reduce_tile(logits[rows_of(t)], carry)
    ld_last.wait()
    turned_product(n_full - 1)
    logits[pl.ds(n_full * ROWS, rest)] = dotf(last[...], normed_t[...])
    peak8, total8 = reduce_tile(logits[pl.ds((n_full - 1) * ROWS, ROWS + rest)], carry)
    peak = jnp.max(peak8, axis=0, keepdims=True)
    total = jnp.sum(total8 * jnp.exp(peak8 - peak), axis=0, keepdims=True)
    row = lax.broadcasted_iota(jnp.int32, (8, rows), 0)
    stats[me] = jnp.where(row == 0, peak, total)
    stat_out = []
    for d in range(1, ways):
        c = pltpu.make_async_remote_copy(src_ref=stats.at[me], dst_ref=stats.at[me], send_sem=stat_send.at[d], recv_sem=stat_recv.at[d],
                                         device_id={'tp': lax.rem(me + d, ways)}, device_id_type=MESH)
        c.start()
        stat_out.append(c)
    for d in range(1, ways):
        src = lax.rem(me + ways - d, ways)
        pltpu.make_async_remote_copy(src_ref=stats.at[src], dst_ref=stats.at[src], send_sem=stat_send.at[d], recv_sem=stat_recv.at[d],
                                     device_id={'tp': me}, device_id_type=MESH).wait_recv()
    all_stats = stats[...]
    peaks = all_stats[:, 0, :]
    totals = all_stats[:, 1, :]
    top_peak = jnp.max(peaks, axis=0, keepdims=True)
    whole = jnp.sum(totals * jnp.exp(peaks - top_peak), axis=0, keepdims=True)
    norm_out[...] = jnp.broadcast_to(top_peak + jnp.log(whole), norm_out.shape)
    for c in sent + stat_out:
        c.wait_send()


def run_tail(ways, attended, hidden, w_o, w_up, w_down, w_out_t, gain2, bias2, gainf, biasf):
    rows, width = hidden.shape
    piece = width // ways
    half = rows // 2
    vocab = w_out_t.shape[0]
    rest = vocab % ROWS
    ff = w_up.shape[1]
    any_ = pl.BlockSpec(memory_space=pl.ANY)
    vmem = pl.BlockSpec(memory_space=pltpu.VMEM)
    hbm = pl.BlockSpec(memory_space=pltpu.HBM)
    return pl.pallas_call(
        functools.partial(tail_kernel, ways),
        out_shape=(pltpu.VMEM((vocab, rows), F32), pltpu.VMEM((8, rows), F32), pltpu.VMEM((rows, width), BF16)),
        in_specs=[vmem, hbm, vmem, hbm, hbm, hbm, vmem, vmem, vmem, vmem],
        out_specs=(vmem, vmem, vmem),
        scratch_shapes=[
            pltpu.VMEM((RING, ROWS, width), BF16),
            pltpu.VMEM((ROWS, width), BF16),
            pltpu.VMEM((rest, width), BF16),
            pltpu.VMEM((rows, piece), BF16),
            pltpu.VMEM((rows, ff), BF16),
            pltpu.VMEM((rows, width), BF16),
            pltpu.VMEM((width, rows), BF16),
            pltpu.VMEM((ways, rows, piece), BF16),
            pltpu.VMEM((2, 2, 2, half, piece), BF16),
            pltpu.VMEM((2, 2, 2, half, piece), BF16),
            pltpu.VMEM((2, rows, piece), BF16),
            pltpu.VMEM((2, 2, half, piece), BF16),
            pltpu.VMEM((2, 2, half, piece), F32),
            pltpu.VMEM((2, 2, half, piece), F32),
            pltpu.VMEM((2, rows, piece), BF16),
            pltpu.VMEM((2, ways, rows, piece), BF16),
            pltpu.VMEM((ways, 8, rows), F32),
            pltpu.SemaphoreType.DMA((RING,)),
            pltpu.SemaphoreType.DMA((10,)),
            pltpu.SemaphoreType.DMA((2, NSEM)),
            pltpu.SemaphoreType.DMA((2, NSEM)),
            pltpu.SemaphoreType.DMA((ways,)),
            pltpu.SemaphoreType.DMA((ways,)),
        ],
        compiler_params=pltpu.CompilerParams(collective_id=0, has_side_effects=True, vmem_limit_bytes=LIMIT),
        name='tail',
    )(pltpu.with_memory_space_constraint(attended, pltpu.VMEM), hidden, pltpu.with_memory_space_constraint(w_o, pltpu.VMEM), w_up, w_down, w_out_t, gain2, bias2, gainf, biasf)


LIMIT = int(51.6 * 1024 * 1024)


CHUNKS = 4
PROJ = 2


def attend_kernel(hidden, lengths, gain, bias, w_q, w_k, w_v, w_o, cache_k, cache_v,
                  attended, o_out, out_k, out_v,
                  x, gb, len_row, normed, w_qkv, qkv, len_col, k_buf, v_buf, misc_sem, w_sem, in_sem, out_sem):
    rows, width = hidden.shape
    seqs, slots, dim = cache_k.shape
    q_cols = w_q.shape[1]
    heads = q_cols // dim
    step_w = width // PROJ
    step_s = seqs // CHUNKS

    small = [pltpu.make_async_copy(hidden, x, misc_sem.at[0]),
             pltpu.make_async_copy(gain, gb.at[pl.ds(0, 1)], misc_sem.at[1]),
             pltpu.make_async_copy(bias, gb.at[pl.ds(1, 1)], misc_sem.at[2]),
             pltpu.make_async_copy(lengths, len_row, misc_sem.at[3])]
    for c in small:
        c.start()
    w_in = []
    for i in range(PROJ):
        part = pl.ds(i * step_w, step_w)
        w_in.append([pltpu.make_async_copy(w_q.at[part], w_qkv.at[part, pl.ds(0, q_cols)], w_sem.at[0, i]),
                     pltpu.make_async_copy(w_k.at[part], w_qkv.at[part, pl.ds(q_cols, dim)], w_sem.at[1, i]),
                     pltpu.make_async_copy(w_v.at[part], w_qkv.at[part, pl.ds(q_cols + dim, dim)], w_sem.at[2, i])])
        for c in w_in[-1]:
            c.start()
    kv_in, kv_out = [], []
    for i in range(CHUNKS):
        part = pl.ds(i * step_s, step_s)
        kv_in.append([pltpu.make_async_copy(cache_k.at[part], k_buf.at[part], in_sem.at[0, i]),
                      pltpu.make_async_copy(cache_v.at[part], v_buf.at[part], in_sem.at[1, i])])
        kv_out.append([pltpu.make_async_copy(k_buf.at[part], out_k.at[part], out_sem.at[0, i]),
                       pltpu.make_async_copy(v_buf.at[part], out_v.at[part], out_sem.at[1, i])])
        for c in kv_in[-1]:
            c.start()

    ld_o = pltpu.make_async_copy(w_o, o_out, misc_sem.at[4])
    ld_o.start()
    small[3].wait()
    lens = jnp.broadcast_to(len_row[...].astype(F32), (rows, rows)).T
    len_col[...] = lens
    lane = lax.broadcasted_iota(jnp.int32, (1, dim), 1)
    half_rot = dim // 4
    freq_lane = jnp.where(lane < half_rot, lane, lane - half_rot).astype(F32)
    inv_freq = jnp.where(lane < 2 * half_rot, jnp.exp(freq_lane * (-2.0 / (2 * half_rot) * math.log(ROPE_BASE))), 0.0)
    angle = lens * inv_freq
    cosine = jnp.cos(angle)
    sine = jnp.where(lane < half_rot, -1.0, 1.0) * jnp.sin(angle)
    for c in small[:3]:
        c.wait()
    total = jnp.zeros((rows, 128), F32)
    piece = width // 8
    for j in range(8):
        total = total + fold(x[:, j * piece:(j + 1) * piece].astype(F32))
    mean = jnp.sum(total, axis=-1, keepdims=True) / width
    total = jnp.zeros((rows, 128), F32)
    for j in range(8):
        total = total + fold(jnp.square(x[:, j * piece:(j + 1) * piece].astype(F32) - mean))
    scale = lax.rsqrt(jnp.sum(total, axis=-1, keepdims=True) / width + EPSILON)
    for j in range(8):
        cols = slice(j * piece, (j + 1) * piece)
        normed[:, cols] = ((x[:, cols].astype(F32) - mean) * scale * (1.0 + gb[0:1, cols]) + gb[1:2, cols]).astype(BF16)

    for i in range(PROJ):
        for c in w_in[i]:
            c.wait()
        part = slice(i * step_w, (i + 1) * step_w)
        product = dotf(normed[:, part], w_qkv[part])
        if i == 0:
            qkv[...] = product
        else:
            qkv[...] += product
    for h in range(heads + 1):
        cols = slice(h * dim, (h + 1) * dim)
        vec = qkv[:, cols]
        partner = jnp.where(lane < half_rot, pltpu.roll(vec, dim - half_rot, 1), pltpu.roll(vec, half_rot, 1))
        qkv[:, cols] = vec * cosine + partner * sine

    row_id = lax.broadcasted_iota(jnp.int32, (slots, dim), 0).astype(F32)
    group = 8
    span = group * slots
    offset = (lax.broadcasted_iota(jnp.int32, (group, span), 1) - slots * lax.broadcasted_iota(jnp.int32, (group, span), 0)).astype(F32)
    k_cols, v_cols = slice(q_cols, q_cols + dim), slice(q_cols + dim, q_cols + 2 * dim)
    for i in range(CHUNKS):
        for c in kv_in[i]:
            c.wait()

        def put(s, carry):
            base = pl.multiple_of(i * step_s + s * 8, 8)
            lens8 = len_col[pl.ds(base, 8), :]
            new_k = qkv[pl.ds(base, 8), k_cols]
            new_v = qkv[pl.ds(base, 8), v_cols]
            for t in range(8):
                here = row_id == lens8[t:t + 1]
                k_buf[base + t] = jnp.where(here, new_k[t:t + 1], k_buf[base + t].astype(F32)).astype(BF16)
                v_buf[base + t] = jnp.where(here, new_v[t:t + 1], v_buf[base + t].astype(F32)).astype(BF16)
            return carry

        lax.fori_loop(0, step_s // 8, put, 0)
        for c in kv_out[i]:
            c.start()
    for i in range(CHUNKS):
        groups = [i * step_s + g * group for g in range(step_s // group)]
        all_scores = []
        for b in groups:
            q = jnp.concatenate([qkv[b:b + group, h * dim:(h + 1) * dim] for h in range(heads)], axis=0).astype(BF16)
            keys = k_buf[b:b + group].reshape(span, dim)
            all_scores.append(lax.dot_general(q, keys, (((1,), (1,)), ((), ())), preferred_element_type=F32))
        probs = []
        for b, scores in zip(groups, all_scores):
            valid = (offset >= 0.0) & (offset <= len_col[b:b + group, 0:1])
            scores = jnp.where(valid[None], scores.reshape(heads, group, span) * (dim ** -0.5), -1e30)
            peak = jnp.max(scores, axis=-1, keepdims=True)
            weight = jnp.where(valid[None], jnp.exp(scores - peak), 0.0)
            prob = (weight / jnp.sum(weight, axis=-1, keepdims=True)).astype(BF16)
            probs.append(prob.reshape(heads * group, span))
        for b, prob in zip(groups, probs):
            mixed = dotf(prob, v_buf[b:b + group].reshape(span, dim)).astype(BF16)
            for h in range(heads):
                attended[b:b + group, h * dim:(h + 1) * dim] = mixed[h * group:(h + 1) * group]
    for pair in kv_out:
        for c in pair:
            c.wait()
    ld_o.wait()


def run_attend(hidden, cache_k, cache_v, lengths, gain, bias, w_q, w_k, w_v, w_o):
    rows, width = hidden.shape
    seqs, slots, dim = cache_k.shape
    q_cols = w_q.shape[1]
    hbm = pl.BlockSpec(memory_space=pltpu.HBM)
    vmem = pl.BlockSpec(memory_space=pltpu.VMEM)
    return pl.pallas_call(
        attend_kernel,
        out_shape=(pltpu.VMEM((rows, q_cols), BF16), pltpu.VMEM(w_o.shape, BF16), jax.ShapeDtypeStruct(cache_k.shape, BF16), jax.ShapeDtypeStruct(cache_v.shape, BF16)),
        in_specs=[hbm] * 10,
        out_specs=(vmem, vmem, hbm, hbm),
        scratch_shapes=[
            pltpu.VMEM((rows, width), BF16),
            pltpu.VMEM((8, width), F32),
            pltpu.VMEM((1, rows), jnp.int32),
            pltpu.VMEM((rows, width), BF16),
            pltpu.VMEM((width, q_cols + 2 * dim), BF16),
            pltpu.VMEM((rows, q_cols + 2 * dim), F32),
            pltpu.VMEM((rows, rows), F32),
            pltpu.VMEM((seqs, slots, dim), BF16),
            pltpu.VMEM((seqs, slots, dim), BF16),
            pltpu.SemaphoreType.DMA((5,)),
            pltpu.SemaphoreType.DMA((3, PROJ)),
            pltpu.SemaphoreType.DMA((2, CHUNKS)),
            pltpu.SemaphoreType.DMA((2, CHUNKS)),
        ],
        compiler_params=pltpu.CompilerParams(vmem_limit_bytes=40 * 1024 * 1024),
        name='attend',
    )(*(pltpu.with_memory_space_constraint(v, pltpu.HBM) for v in (hidden, lengths, gain, bias, w_q, w_k, w_v, w_o, cache_k, cache_v)))


PARTS = 8


def finish_kernel(logits, norm, y, out, y_out, buf, sem, y_sem):
    copy = pltpu.make_async_copy(y, y_out, y_sem)
    copy.start()
    block = logits.shape[0] // PARTS // 8 * 8
    outs = []
    for i in range(PARTS):
        size = block if i < PARTS - 1 else logits.shape[0] - block * (PARTS - 1)
        part = pl.ds(i * block, size)
        buf[part] = logits[part] - norm[0:1]
        outs.append(pltpu.make_async_copy(buf.at[part], out.at[part], sem.at[i]))
        outs[-1].start()
    for c in outs:
        c.wait()
    copy.wait()


def run_finish(logits, norm, y):
    vocab, rows = logits.shape
    vmem = pl.BlockSpec(memory_space=pltpu.VMEM)
    hbm = pl.BlockSpec(memory_space=pltpu.HBM)
    return pl.pallas_call(
        finish_kernel,
        out_shape=(jax.ShapeDtypeStruct((vocab, rows), F32), jax.ShapeDtypeStruct(y.shape, BF16)),
        in_specs=[vmem, vmem, vmem],
        out_specs=(hbm, hbm),
        scratch_shapes=[pltpu.VMEM((vocab, rows), F32), pltpu.SemaphoreType.DMA((PARTS,)), pltpu.SemaphoreType.DMA],
        compiler_params=pltpu.CompilerParams(vmem_limit_bytes=16 * 1024 * 1024),
        name='finish',
    )(logits, norm, y)


def solution(mesh):
    ways = mesh.shape['tp']
    row_spec = P('bs', None)
    cache_spec = P('bs', None, 'tp', None)
    col_split = P(None, 'tp')
    row_split = P('tp', None)
    in_specs = (row_spec, cache_spec, cache_spec, P('bs'), P(), P(), col_split, col_split, col_split, row_split, P(), P(), col_split, row_split, P(), P(), col_split)
    out_specs = (P('bs', 'tp'), cache_spec, cache_spec, row_spec)

    def local_step(new_hidden, cache_k, cache_v, lengths, ln1_gain, ln1_bias, w_q, w_k, w_v, w_o, ln2_gain, ln2_bias, w_up, w_down, lnf_gain, lnf_bias, w_out):
        shape = cache_k.shape
        flat = (shape[0], shape[1], shape[3])
        attended, w_o, new_cache_k, new_cache_v = run_attend(new_hidden, cache_k.reshape(flat), cache_v.reshape(flat), lengths[None], ln1_gain[None], ln1_bias[None], w_q, w_k, w_v, w_o)
        logits, norm, y = run_tail(ways, attended, new_hidden, w_o, w_up, w_down, w_out.T,
                                   ln2_gain[None], ln2_bias[None], lnf_gain[None], lnf_bias[None])
        log_probs_t, out_hidden = run_finish(logits, norm, y)
        return log_probs_t.T, new_cache_k.reshape(shape), new_cache_v.reshape(shape), out_hidden

    return jax.shard_map(local_step, mesh=mesh, in_specs=in_specs, out_specs=out_specs, check_vma=False)
```

```python
import functools
import math

import jax
import jax.numpy as jnp
from jax import lax
from jax.experimental import pallas as pl
from jax.experimental.pallas import tpu as pltpu
from jax.sharding import PartitionSpec as P

EPSILON = 1e-5
ROPE_BASE = 10000.0
BF16 = jnp.bfloat16
F32 = jnp.float32
MESH = pl.DeviceIdType.MESH
RING = 13
FLIPS = 12
BLOCK = 256
QUAD = 4
FILL = (
    (((0, 1), ()), (('up', 2, 3), (0, 1)), ((4, 5, 6), (2, 3)), ((), (4,)), (('down',), ())),
    (((7, 8), (5, 6)), ((9, 10, 11, 12), (7, 8)), ((), (9, 10)), ((), (11, 12)), ((FLIPS + RING, 'last'), ())),
)
ROWS = 512
NSEM = 26


def dotf(lhs, rhs):
    return jnp.dot(lhs, rhs, preferred_element_type=F32)


def fold(values):
    out = values[:, 0:128]
    for lane in range(128, values.shape[1], 128):
        out = out + values[:, lane:lane + 128]
    return out


def norm_chunks(chunks, gain, bias, out):
    count, rows, piece = chunks.shape
    width = count * piece
    total = jnp.zeros((rows, 128), F32)
    for j in range(count):
        total = total + fold(chunks[j].astype(F32))
    mean = jnp.sum(total, axis=-1, keepdims=True) / width
    total = jnp.zeros((rows, 128), F32)
    for j in range(count):
        total = total + fold(jnp.square(chunks[j].astype(F32) - mean))
    scale = lax.rsqrt(jnp.sum(total, axis=-1, keepdims=True) / width + EPSILON)
    for j in range(count):
        cols = slice(j * piece, (j + 1) * piece)
        normed = (chunks[j].astype(F32) - mean) * scale * (1.0 + gain[:, cols]) + bias[:, cols]
        out[:, cols] = normed.astype(BF16)


def tail_kernel(ways, attended, hidden, w_o, w_up, w_down, w_out, gain2, bias2, gainf, biasf,
                logits, norm_out, y_out,
                ring, turned, last, resid, act, normed, normed_t, parts, raw1, raw2, sib, sibh, send3, recv3, own, gath, stats,
                w_sem, small_sem, send_sem, recv_sem, stat_send, stat_recv):
    me = lax.axis_index('tp')
    core = lax.rem(me, 2)
    chip = me // 2
    chips = ways // 2
    right = lax.rem(chip + 1, chips)
    left = lax.rem(chip + chips - 1, chips)
    far = lax.rem(chip + 2, chips)
    other = 1 - core
    rows, piece = resid.shape
    half = rows // 2
    top, bot = pl.ds(0, half), pl.ds(half, half)
    vocab, width = w_out.shape
    n_full = vocab // ROWS
    rest = vocab - n_full * ROWS
    s_up, s_down = RING - 4, RING - 2

    def dev(c, k):
        return {'tp': 2 * c + k}

    ld_res = pltpu.make_async_copy(hidden.at[:, pl.ds(pl.multiple_of(me * piece, piece), piece)], resid, small_sem.at[0])
    ld_up = []
    for i in range(width // ROWS):
        ld_up.append(pltpu.make_async_copy(w_up.at[pl.ds(i * ROWS, ROWS)], ring.at[s_up + i // 3, :, pl.ds((i % 3) * w_up.shape[1], w_up.shape[1])], small_sem.at[4 + i]))
    ld_down = [pltpu.make_async_copy(w_down.at[pl.ds(i * ROWS, ROWS)], ring.at[s_down + i], small_sem.at[1 + i]) for i in range(2)]
    ld_last = pltpu.make_async_copy(w_out.at[pl.ds(n_full * ROWS, rest)], last, small_sem.at[3])

    def ld_tile(tile):
        slot = lax.rem(tile, RING)
        return pltpu.make_async_copy(w_out.at[pl.ds(pl.multiple_of(tile * ROWS, ROWS), ROWS)], ring.at[slot], w_sem.at[slot])

    ld_res.start()

    def start(item):
        if item == 'up':
            for c in ld_up:
                c.start()
        elif item == 'down':
            for c in ld_down:
                c.start()
        elif item == 'last':
            ld_last.start()
        else:
            ld_tile(item).start()

    def flip(tile):
        ld_tile(tile).wait()
        target = ring.at[tile] if tile < FLIPS else turned

        def turn(b, carry):
            for part in range(2):
                cols = pl.ds(pl.multiple_of((2 * b + part) * BLOCK, BLOCK), BLOCK)
                for a in range(0, ROWS, BLOCK):
                    target[a:a + BLOCK, cols] = ring[tile, a:a + BLOCK, cols].T
            return carry

        lax.fori_loop(0, width // BLOCK // 2, turn, 0)

    barrier = pltpu.get_barrier_semaphore()
    for d in range(1, ways):
        pl.semaphore_signal(barrier, inc=1, device_id={'tp': lax.rem(me + d, ways)}, device_id_type=MESH)

    def copy(phase, idx, src, dst, to, ridx=None):
        ridx = idx if ridx is None else ridx
        return pltpu.make_async_remote_copy(src_ref=src, dst_ref=dst, send_sem=send_sem.at[phase, idx], recv_sem=recv_sem.at[phase, ridx],
                                            device_id=to, device_id_type=MESH)

    def arrive(phase, idx, dst):
        copy(phase, idx, dst, dst, dev(chip, core)).wait_recv()

    def busy(work):
        for item in work[0]:
            start(item)
        for tile in work[1]:
            flip(tile)

    def all_sum(phase, product, residual, fill):
        pb = parts
        sent = []

        def go(c):
            c.start()
            sent.append(c)

        def term(c):
            value = product(c).astype(BF16)
            pb[2 * c] = value[:, :piece]
            pb[2 * c + 1] = value[:, piece:]

        g = gath.at[phase]
        term(far)
        if phase == 0:
            pl.semaphore_wait(barrier, ways - 1)
        for k in range(2):
            go(copy(phase, k, pb.at[2 * far + k, top], raw1.at[phase, 0, core], dev(right, k), core))
            go(copy(phase, 2 + k, pb.at[2 * far + k, bot], raw1.at[phase, 1, core], dev(left, k), 2 + core))
        term(right)
        for k in range(2):
            go(copy(phase, 6 + k, pb.at[2 * right + k, bot], raw2.at[phase, 1, core], dev(right, k), 6 + core))
        go(copy(phase, 9, pb.at[2 * right + other, top], sibh.at[phase, 0], dev(chip, other)))
        term(left)
        for k in range(2):
            go(copy(phase, 4 + k, pb.at[2 * left + k, top], raw2.at[phase, 0, core], dev(left, k), 4 + core))
        go(copy(phase, 10, pb.at[2 * left + other, bot], sibh.at[phase, 1], dev(chip, other)))
        term(chip)
        go(copy(phase, 8, pb.at[2 * chip + other], sib.at[phase], dev(chip, other)))
        busy(fill[0])
        for side, (to, rws) in enumerate(((right, top), (left, bot))):
            for k in range(2):
                arrive(phase, 2 * side + k, raw1.at[phase, side, k])
            arrive(phase, 9 + side, sibh.at[phase, side])
            send3[phase, side] = (raw1[phase, side, 0].astype(F32) + raw1[phase, side, 1].astype(F32)
                                  + pb[2 * to + core, rws].astype(F32) + sibh[phase, side].astype(F32))
            go(copy(phase, 11 + side, send3.at[phase, side], recv3.at[phase, side], dev(to, core)))
        busy(fill[1])
        arrive(phase, 8, sib.at[phase])
        for side, rws in enumerate((top, bot)):
            for k in range(2):
                arrive(phase, 4 + 2 * side + k, raw2.at[phase, side, k])
            base = (residual[rws].astype(F32) + pb[me, rws].astype(F32) + sib[phase, rws].astype(F32)
                    + raw2[phase, side, 0].astype(F32) + raw2[phase, side, 1].astype(F32))
            arrive(phase, 11 + side, recv3.at[phase, side])
            value = (base + recv3[phase, side]).astype(BF16)
            own[phase, rws] = value
            g[me, rws] = value
        ob = own.at[phase]
        go(copy(phase, 13, ob.at[top], g.at[me, top], dev(right, core)))
        go(copy(phase, 16, ob.at[bot], g.at[me, bot], dev(left, core)))
        go(copy(phase, 19, ob, g.at[me], dev(chip, other)))
        go(copy(phase, 14, ob.at[bot], g.at[me, bot], dev(right, core)))
        go(copy(phase, 15, ob.at[top], g.at[me, top], dev(left, core)))
        busy(fill[2])
        ml, mr, mf = 2 * left + core, 2 * right + core, 2 * far + core
        arrive(phase, 13, g.at[ml, top])
        go(copy(phase, 17, g.at[ml, top], g.at[ml, top], dev(right, core)))
        arrive(phase, 16, g.at[mr, bot])
        go(copy(phase, 18, g.at[mr, bot], g.at[mr, bot], dev(left, core)))
        go(copy(phase, 20, g.at[ml, top], g.at[ml, top], dev(chip, other)))
        go(copy(phase, 21, g.at[mr, bot], g.at[mr, bot], dev(chip, other)))
        busy(fill[3])
        arrive(phase, 14, g.at[ml, bot])
        go(copy(phase, 22, g.at[ml, bot], g.at[ml, bot], dev(chip, other)))
        arrive(phase, 15, g.at[mr, top])
        go(copy(phase, 23, g.at[mr, top], g.at[mr, top], dev(chip, other)))
        arrive(phase, 17, g.at[mf, top])
        go(copy(phase, 24, g.at[mf, top], g.at[mf, top], dev(chip, other)))
        arrive(phase, 18, g.at[mf, bot])
        go(copy(phase, 25, g.at[mf, bot], g.at[mf, bot], dev(chip, other)))
        busy(fill[4])
        ol, orr, of = 2 * left + other, 2 * right + other, 2 * far + other
        arrive(phase, 19, g.at[2 * chip + other])
        arrive(phase, 20, g.at[ol, top])
        arrive(phase, 21, g.at[orr, bot])
        arrive(phase, 22, g.at[ol, bot])
        arrive(phase, 23, g.at[orr, top])
        arrive(phase, 24, g.at[of, top])
        arrive(phase, 25, g.at[of, bot])
        return sent

    ld_res.wait()

    def product_o(c):
        return dotf(attended[...], w_o[:, pl.ds(pl.multiple_of(2 * piece * c, 2 * piece), 2 * piece)])

    sent = all_sum(0, product_o, resid, FILL[0])
    norm_chunks(gath.at[0], gain2, bias2, normed)

    for c in ld_up:
        c.wait()
    ff = w_up.shape[1]
    for n in range(0, ff, 256):
        total = jnp.zeros((rows, 256), F32)
        for i in range(width // ROWS):
            total = total + dotf(normed[:, i * ROWS:(i + 1) * ROWS], ring[s_up + i // 3, :, (i % 3) * ff + n:(i % 3) * ff + n + 256])
        act[:, n:n + 256] = jnp.square(jnp.maximum(total, 0.0)).astype(BF16)
    for c in ld_down:
        c.wait()

    def product_down(c):
        cols = pl.ds(pl.multiple_of(2 * piece * c, 2 * piece), 2 * piece)
        return dotf(act[:, :ROWS], ring[s_down, :, cols]) + dotf(act[:, ROWS:], ring[s_down + 1, :, cols])

    for c in sent:
        c.wait_send()
    sent = all_sum(1, product_down, gath.at[0, me], FILL[1])
    norm_chunks(gath.at[1], gainf, biasf, normed)
    for j in range(ways):
        y_out[:, j * piece:(j + 1) * piece] = gath[1, j]
        normed_t[j * piece:(j + 1) * piece] = normed[:, j * piece:(j + 1) * piece].T

    def reduce_tile(z, carry):
        peak, total = carry
        z3 = z.reshape(z.shape[0] // 8, 8, z.shape[1])
        new_peak = jnp.maximum(peak, jnp.max(z3, axis=0))
        total = total * jnp.exp(peak - new_peak) + jnp.sum(jnp.exp(z3 - new_peak[None]), axis=0)
        return new_peak, total

    def rows_of(tile):
        return pl.ds(pl.multiple_of(tile * ROWS, ROWS), ROWS)

    def refill(tile):
        @pl.when(tile + RING < n_full)
        def _():
            ld_tile(tile + RING).start()

    def step_turned(quad, carry):
        for t in range(QUAD):
            tile = QUAD * quad + t
            carry = reduce_tile(logits[rows_of(jnp.maximum(tile - QUAD, 0))], carry)
        for t in range(QUAD):
            tile = QUAD * quad + t
            for a in range(0, ROWS, BLOCK):
                z = jnp.zeros((rows, BLOCK), F32)
                for b in range(0, width, BLOCK):
                    z = z + dotf(normed[:, b:b + BLOCK], ring[tile, a:a + BLOCK, b:b + BLOCK])
                logits[pl.ds(pl.multiple_of(tile * ROWS + a, BLOCK), BLOCK)] = z.T
            ld_tile(tile + RING).start()
        return carry

    def turned_product(tile):
        for a in range(0, ROWS, BLOCK):
            z = jnp.zeros((rows, BLOCK), F32)
            for b in range(0, width, BLOCK):
                z = z + dotf(normed[:, b:b + BLOCK], turned[a:a + BLOCK, b:b + BLOCK])
            logits[pl.ds(pl.multiple_of(tile * ROWS + a, BLOCK), BLOCK)] = z.T

    def step_pair(pair, carry):
        tile = FLIPS + 2 * pair
        plain, coming = lax.rem(tile + 1, RING), lax.rem(tile + 2, RING)
        ld_tile(tile + 1).wait()
        ld_tile(tile + 2).wait()
        for t in range(2):
            carry = reduce_tile(logits[rows_of(tile - 2 + t)], carry)
        turned_product(tile)
        for a in range(0, ROWS, BLOCK):
            logits[pl.ds(pl.multiple_of((tile + 1) * ROWS + a, BLOCK), BLOCK)] = dotf(ring[plain, a:a + BLOCK], normed_t[...])
            for b in range(width // ROWS * a, width // ROWS * (a + BLOCK), BLOCK):
                for r in range(0, ROWS, BLOCK):
                    turned[r:r + BLOCK, b:b + BLOCK] = ring[coming, r:r + BLOCK, b:b + BLOCK].T
        refill(tile + 1)
        refill(tile + 2)
        return carry

    logits[pl.ds(0, ROWS)] = jnp.full((ROWS, rows), -1e30, F32)
    carry = (jnp.full((8, rows), -1e30, F32), jnp.zeros((8, rows), F32))
    carry = lax.fori_loop(0, FLIPS // QUAD, step_turned, carry)
    for t in range(FLIPS - QUAD, FLIPS - 2):
        carry = reduce_tile(logits[rows_of(t)], carry)
    carry = lax.fori_loop(0, (n_full - FLIPS - 1) // 2, step_pair, carry)
    for t in range(n_full - 3, n_full - 1):
        carry = reduce_tile(logits[rows_of(t)], carry)
    ld_last.wait()
    turned_product(n_full - 1)
    logits[pl.ds(n_full * ROWS, rest)] = dotf(last[...], normed_t[...])
    peak8, total8 = reduce_tile(logits[pl.ds((n_full - 1) * ROWS, ROWS + rest)], carry)
    peak = jnp.max(peak8, axis=0, keepdims=True)
    total = jnp.sum(total8 * jnp.exp(peak8 - peak), axis=0, keepdims=True)
    row = lax.broadcasted_iota(jnp.int32, (8, rows), 0)
    stats[me] = jnp.where(row == 0, peak, total)
    stat_out = []
    for d in range(1, ways):
        c = pltpu.make_async_remote_copy(src_ref=stats.at[me], dst_ref=stats.at[me], send_sem=stat_send.at[d], recv_sem=stat_recv.at[d],
                                         device_id={'tp': lax.rem(me + d, ways)}, device_id_type=MESH)
        c.start()
        stat_out.append(c)
    for d in range(1, ways):
        src = lax.rem(me + ways - d, ways)
        pltpu.make_async_remote_copy(src_ref=stats.at[src], dst_ref=stats.at[src], send_sem=stat_send.at[d], recv_sem=stat_recv.at[d],
                                     device_id={'tp': me}, device_id_type=MESH).wait_recv()
    all_stats = stats[...]
    peaks = all_stats[:, 0, :]
    totals = all_stats[:, 1, :]
    top_peak = jnp.max(peaks, axis=0, keepdims=True)
    whole = jnp.sum(totals * jnp.exp(peaks - top_peak), axis=0, keepdims=True)
    norm_out[...] = jnp.broadcast_to(top_peak + jnp.log(whole), norm_out.shape)
    for c in sent + stat_out:
        c.wait_send()


def run_tail(ways, attended, hidden, w_o, w_up, w_down, w_out_t, gain2, bias2, gainf, biasf):
    rows, width = hidden.shape
    piece = width // ways
    half = rows // 2
    vocab = w_out_t.shape[0]
    rest = vocab % ROWS
    ff = w_up.shape[1]
    any_ = pl.BlockSpec(memory_space=pl.ANY)
    vmem = pl.BlockSpec(memory_space=pltpu.VMEM)
    hbm = pl.BlockSpec(memory_space=pltpu.HBM)
    return pl.pallas_call(
        functools.partial(tail_kernel, ways),
        out_shape=(pltpu.VMEM((vocab, rows), F32), pltpu.VMEM((8, rows), F32), pltpu.VMEM((rows, width), BF16)),
        in_specs=[vmem, hbm, vmem, hbm, hbm, hbm, vmem, vmem, vmem, vmem],
        out_specs=(vmem, vmem, vmem),
        scratch_shapes=[
            pltpu.VMEM((RING, ROWS, width), BF16),
            pltpu.VMEM((ROWS, width), BF16),
            pltpu.VMEM((rest, width), BF16),
            pltpu.VMEM((rows, piece), BF16),
            pltpu.VMEM((rows, ff), BF16),
            pltpu.VMEM((rows, width), BF16),
            pltpu.VMEM((width, rows), BF16),
            pltpu.VMEM((ways, rows, piece), BF16),
            pltpu.VMEM((2, 2, 2, half, piece), BF16),
            pltpu.VMEM((2, 2, 2, half, piece), BF16),
            pltpu.VMEM((2, rows, piece), BF16),
            pltpu.VMEM((2, 2, half, piece), BF16),
            pltpu.VMEM((2, 2, half, piece), F32),
            pltpu.VMEM((2, 2, half, piece), F32),
            pltpu.VMEM((2, rows, piece), BF16),
            pltpu.VMEM((2, ways, rows, piece), BF16),
            pltpu.VMEM((ways, 8, rows), F32),
            pltpu.SemaphoreType.DMA((RING,)),
            pltpu.SemaphoreType.DMA((10,)),
            pltpu.SemaphoreType.DMA((2, NSEM)),
            pltpu.SemaphoreType.DMA((2, NSEM)),
            pltpu.SemaphoreType.DMA((ways,)),
            pltpu.SemaphoreType.DMA((ways,)),
        ],
        compiler_params=pltpu.CompilerParams(collective_id=0, has_side_effects=True, vmem_limit_bytes=LIMIT),
        name='tail',
    )(pltpu.with_memory_space_constraint(attended, pltpu.VMEM), hidden, pltpu.with_memory_space_constraint(w_o, pltpu.VMEM), w_up, w_down, w_out_t, gain2, bias2, gainf, biasf)


LIMIT = int(51.6 * 1024 * 1024)


CHUNKS = 4
PROJ = 2


def attend_kernel(hidden, lengths, gain, bias, w_q, w_k, w_v, w_o, cache_k, cache_v,
                  attended, o_out, out_k, out_v,
                  x, gb, len_row, normed, w_qkv, qkv, len_col, k_buf, v_buf, misc_sem, w_sem, in_sem, out_sem):
    rows, width = hidden.shape
    seqs, slots, dim = cache_k.shape
    q_cols = w_q.shape[1]
    heads = q_cols // dim
    step_w = width // PROJ
    step_s = seqs // CHUNKS

    small = [pltpu.make_async_copy(hidden, x, misc_sem.at[0]),
             pltpu.make_async_copy(gain, gb.at[pl.ds(0, 1)], misc_sem.at[1]),
             pltpu.make_async_copy(bias, gb.at[pl.ds(1, 1)], misc_sem.at[2]),
             pltpu.make_async_copy(lengths, len_row, misc_sem.at[3])]
    for c in small:
        c.start()
    w_in = []
    for i in range(PROJ):
        part = pl.ds(i * step_w, step_w)
        w_in.append([pltpu.make_async_copy(w_q.at[part], w_qkv.at[part, pl.ds(0, q_cols)], w_sem.at[0, i]),
                     pltpu.make_async_copy(w_k.at[part], w_qkv.at[part, pl.ds(q_cols, dim)], w_sem.at[1, i]),
                     pltpu.make_async_copy(w_v.at[part], w_qkv.at[part, pl.ds(q_cols + dim, dim)], w_sem.at[2, i])])
        for c in w_in[-1]:
            c.start()
    kv_in, kv_out = [], []
    for i in range(CHUNKS):
        part = pl.ds(i * step_s, step_s)
        kv_in.append([pltpu.make_async_copy(cache_k.at[part], k_buf.at[part], in_sem.at[0, i]),
                      pltpu.make_async_copy(cache_v.at[part], v_buf.at[part], in_sem.at[1, i])])
        kv_out.append([pltpu.make_async_copy(k_buf.at[part], out_k.at[part], out_sem.at[0, i]),
                       pltpu.make_async_copy(v_buf.at[part], out_v.at[part], out_sem.at[1, i])])
        for c in kv_in[-1]:
            c.start()

    ld_o = pltpu.make_async_copy(w_o, o_out, misc_sem.at[4])
    ld_o.start()
    small[3].wait()
    lens = jnp.broadcast_to(len_row[...].astype(F32), (rows, rows)).T
    len_col[...] = lens
    lane = lax.broadcasted_iota(jnp.int32, (1, dim), 1)
    half_rot = dim // 4
    freq_lane = jnp.where(lane < half_rot, lane, lane - half_rot).astype(F32)
    inv_freq = jnp.where(lane < 2 * half_rot, jnp.exp(freq_lane * (-2.0 / (2 * half_rot) * math.log(ROPE_BASE))), 0.0)
    angle = lens * inv_freq
    cosine = jnp.cos(angle)
    sine = jnp.where(lane < half_rot, -1.0, 1.0) * jnp.sin(angle)
    for c in small[:3]:
        c.wait()
    total = jnp.zeros((rows, 128), F32)
    piece = width // 8
    for j in range(8):
        total = total + fold(x[:, j * piece:(j + 1) * piece].astype(F32))
    mean = jnp.sum(total, axis=-1, keepdims=True) / width
    total = jnp.zeros((rows, 128), F32)
    for j in range(8):
        total = total + fold(jnp.square(x[:, j * piece:(j + 1) * piece].astype(F32) - mean))
    scale = lax.rsqrt(jnp.sum(total, axis=-1, keepdims=True) / width + EPSILON)
    for j in range(8):
        cols = slice(j * piece, (j + 1) * piece)
        normed[:, cols] = ((x[:, cols].astype(F32) - mean) * scale * (1.0 + gb[0:1, cols]) + gb[1:2, cols]).astype(BF16)

    for i in range(PROJ):
        for c in w_in[i]:
            c.wait()
        part = slice(i * step_w, (i + 1) * step_w)
        product = dotf(normed[:, part], w_qkv[part])
        if i == 0:
            qkv[...] = product
        else:
            qkv[...] += product
    for h in range(heads + 1):
        cols = slice(h * dim, (h + 1) * dim)
        vec = qkv[:, cols]
        partner = jnp.where(lane < half_rot, pltpu.roll(vec, dim - half_rot, 1), pltpu.roll(vec, half_rot, 1))
        qkv[:, cols] = vec * cosine + partner * sine

    row_id = lax.broadcasted_iota(jnp.int32, (slots, dim), 0).astype(F32)
    group = 8
    span = group * slots
    offset = (lax.broadcasted_iota(jnp.int32, (group, span), 1) - slots * lax.broadcasted_iota(jnp.int32, (group, span), 0)).astype(F32)
    k_cols, v_cols = slice(q_cols, q_cols + dim), slice(q_cols + dim, q_cols + 2 * dim)
    for i in range(CHUNKS):
        for c in kv_in[i]:
            c.wait()

        def put(s, carry):
            base = pl.multiple_of(i * step_s + s * 8, 8)
            lens8 = len_col[pl.ds(base, 8), :]
            new_k = qkv[pl.ds(base, 8), k_cols]
            new_v = qkv[pl.ds(base, 8), v_cols]
            for t in range(8):
                here = row_id == lens8[t:t + 1]
                k_buf[base + t] = jnp.where(here, new_k[t:t + 1], k_buf[base + t].astype(F32)).astype(BF16)
                v_buf[base + t] = jnp.where(here, new_v[t:t + 1], v_buf[base + t].astype(F32)).astype(BF16)
            return carry

        lax.fori_loop(0, step_s // 8, put, 0)
        for c in kv_out[i]:
            c.start()
    for i in range(CHUNKS):
        groups = [i * step_s + g * group for g in range(step_s // group)]
        all_scores = []
        for b in groups:
            q = jnp.concatenate([qkv[b:b + group, h * dim:(h + 1) * dim] for h in range(heads)], axis=0).astype(BF16)
            keys = k_buf[b:b + group].reshape(span, dim)
            all_scores.append(lax.dot_general(q, keys, (((1,), (1,)), ((), ())), preferred_element_type=F32))
        probs = []
        for b, scores in zip(groups, all_scores):
            valid = (offset >= 0.0) & (offset <= len_col[b:b + group, 0:1])
            scores = jnp.where(valid[None], scores.reshape(heads, group, span) * (dim ** -0.5), -1e30)
            peak = jnp.max(scores, axis=-1, keepdims=True)
            weight = jnp.where(valid[None], jnp.exp(scores - peak), 0.0)
            prob = (weight / jnp.sum(weight, axis=-1, keepdims=True)).astype(BF16)
            probs.append(prob.reshape(heads * group, span))
        for b, prob in zip(groups, probs):
            mixed = dotf(prob, v_buf[b:b + group].reshape(span, dim)).astype(BF16)
            for h in range(heads):
                attended[b:b + group, h * dim:(h + 1) * dim] = mixed[h * group:(h + 1) * group]
    for pair in kv_out:
        for c in pair:
            c.wait()
    ld_o.wait()


def run_attend(hidden, cache_k, cache_v, lengths, gain, bias, w_q, w_k, w_v, w_o):
    rows, width = hidden.shape
    seqs, slots, dim = cache_k.shape
    q_cols = w_q.shape[1]
    hbm = pl.BlockSpec(memory_space=pltpu.HBM)
    vmem = pl.BlockSpec(memory_space=pltpu.VMEM)
    return pl.pallas_call(
        attend_kernel,
        out_shape=(pltpu.VMEM((rows, q_cols), BF16), pltpu.VMEM(w_o.shape, BF16), jax.ShapeDtypeStruct(cache_k.shape, BF16), jax.ShapeDtypeStruct(cache_v.shape, BF16)),
        in_specs=[hbm] * 10,
        out_specs=(vmem, vmem, hbm, hbm),
        scratch_shapes=[
            pltpu.VMEM((rows, width), BF16),
            pltpu.VMEM((8, width), F32),
            pltpu.VMEM((1, rows), jnp.int32),
            pltpu.VMEM((rows, width), BF16),
            pltpu.VMEM((width, q_cols + 2 * dim), BF16),
            pltpu.VMEM((rows, q_cols + 2 * dim), F32),
            pltpu.VMEM((rows, rows), F32),
            pltpu.VMEM((seqs, slots, dim), BF16),
            pltpu.VMEM((seqs, slots, dim), BF16),
            pltpu.SemaphoreType.DMA((5,)),
            pltpu.SemaphoreType.DMA((3, PROJ)),
            pltpu.SemaphoreType.DMA((2, CHUNKS)),
            pltpu.SemaphoreType.DMA((2, CHUNKS)),
        ],
        compiler_params=pltpu.CompilerParams(vmem_limit_bytes=40 * 1024 * 1024),
        name='attend',
    )(*(pltpu.with_memory_space_constraint(v, pltpu.HBM) for v in (hidden, lengths, gain, bias, w_q, w_k, w_v, w_o, cache_k, cache_v)))


PARTS = 8


def finish_kernel(logits, norm, y, out, y_out, buf, sem, y_sem):
    copy = pltpu.make_async_copy(y, y_out, y_sem)
    copy.start()
    block = logits.shape[0] // PARTS // 8 * 8
    outs = []
    for i in range(PARTS):
        size = block if i < PARTS - 1 else logits.shape[0] - block * (PARTS - 1)
        part = pl.ds(i * block, size)
        buf[part] = logits[part] - norm[0:1]
        outs.append(pltpu.make_async_copy(buf.at[part], out.at[part], sem.at[i]))
        outs[-1].start()
    for c in outs:
        c.wait()
    copy.wait()


def run_finish(logits, norm, y):
    vocab, rows = logits.shape
    vmem = pl.BlockSpec(memory_space=pltpu.VMEM)
    hbm = pl.BlockSpec(memory_space=pltpu.HBM)
    return pl.pallas_call(
        finish_kernel,
        out_shape=(jax.ShapeDtypeStruct((vocab, rows), F32), jax.ShapeDtypeStruct(y.shape, BF16)),
        in_specs=[vmem, vmem, vmem],
        out_specs=(hbm, hbm),
        scratch_shapes=[pltpu.VMEM((vocab, rows), F32), pltpu.SemaphoreType.DMA((PARTS,)), pltpu.SemaphoreType.DMA],
        compiler_params=pltpu.CompilerParams(vmem_limit_bytes=16 * 1024 * 1024),
        name='finish',
    )(logits, norm, y)


def solution(mesh):
    ways = mesh.shape['tp']
    row_spec = P('bs', None)
    cache_spec = P('bs', None, 'tp', None)
    col_split = P(None, 'tp')
    row_split = P('tp', None)
    in_specs = (row_spec, cache_spec, cache_spec, P('bs'), P(), P(), col_split, col_split, col_split, row_split, P(), P(), col_split, row_split, P(), P(), col_split)
    out_specs = (P('bs', 'tp'), cache_spec, cache_spec, row_spec)

    def local_step(new_hidden, cache_k, cache_v, lengths, ln1_gain, ln1_bias, w_q, w_k, w_v, w_o, ln2_gain, ln2_bias, w_up, w_down, lnf_gain, lnf_bias, w_out):
        shape = cache_k.shape
        flat = (shape[0], shape[1], shape[3])
        attended, w_o, new_cache_k, new_cache_v = run_attend(new_hidden, cache_k.reshape(flat), cache_v.reshape(flat), lengths[None], ln1_gain[None], ln1_bias[None], w_q, w_k, w_v, w_o)
        logits, norm, y = run_tail(ways, attended, new_hidden, w_o, w_up, w_down, w_out.T,
                                   ln2_gain[None], ln2_bias[None], lnf_gain[None], lnf_bias[None])
        log_probs_t, out_hidden = run_finish(logits, norm, y)
        return log_probs_t.T, new_cache_k.reshape(shape), new_cache_v.reshape(shape), out_hidden

    return jax.shard_map(local_step, mesh=mesh, in_specs=in_specs, out_specs=out_specs, check_vma=False)
```
